512 devices in a mesh: scan: 2 (over y), ang: 32 (over z, core), row: 8 (over x).
Axes of the slice: x: 8, y: 2, z: 16, core: 2. Of those that a mesh axis runs over, the one named last changes fastest.
The devices are a block of a 8x16x16 slice.
Arguments:
- projections: bfloat16 [64, 64, 2560], P(('scan', 'ang'), 'row'), parts along dimension 0, may hold values from 0 to 2
- flats: float32 [128, 2560], P(('scan', 'row')), parts along dimension 0, may hold values from 1 to 3
- block_start: int32 [32, 32], replicated, may hold values from 0 to 2528
- bp_weights: bfloat16 [32, 32, 8192], P(None, None, 'ang'), may hold values from -0.1875 to 0.1875
Outputs:
- recon: float32 [128, 8192], P(('scan', 'row'), 'ang'), parts along dimension 0
The draws below stay inside these ranges and needn't reach their ends.
There are 2 independent parts, one for each index of `scan`. The reference program is written for one: setup_inputs(seed, part) draws one part's arguments, and reference() takes and returns one part's arrays. A program takes and returns all parts, laid end to end along the dimension named above; an argument that names none is the same for every part. Nothing has to cross between parts.
Inputs may be any that keep to these rules, and one draw needn't show every extreme that they name: block_start[a, r] is the first of the 32 detector columns that pixel region r reads at angle a.
All inputs are finite; a program needn't handle non-finite values.
Results may differ from the reference program's by a relative error of at most 0.009.
Values may be sent and summed in bfloat16 or wider, within the bound.
No kernel may reach another device: no remote copies, remote signals or barrier semaphores. Data moves between devices by JAX's collectives and lax.ppermute only.
A program may use at most 64 MiB of HBM per device.

```python
import math
import jax
import jax.numpy as jnp
from jax import lax

W = 2560
RD = 8
HALO = 4
CB = 32
PIX_DEV = 256
TILE = 16
ANGLES = 32
SLICES = 64
REGIONS = 32
PIX = 8192


def set_ends(entries, stream_key, smallest, largest):
    shape = entries.shape
    spot = [jax.random.randint(jax.random.fold_in(stream_key, axis), (), 0, shape[axis]) for axis in range(len(shape))]
    entries = entries.at[tuple(spot)].set(smallest)
    longest = shape.index(max(shape))
    spot[longest] = (spot[longest] + 1) % shape[longest]
    return entries.at[tuple(spot)].set(largest)


def levels(rng, extent, shards, least, largest):
    factor_of = 1.0
    for position, shards_of in shards:
        steps = jax.random.uniform(jax.random.fold_in(jax.random.fold_in(rng, 6), position), (shards_of,), jnp.float32, least / len(shards), largest / len(shards))
        factor_of = factor_of * jnp.repeat(jnp.exp(steps), extent[position] // shards_of).reshape((-1,) + (1,) * (len(extent) - 1 - position))
    return factor_of


def gaussian(own_key, dims, scale, bound, shards=(), kind=jnp.bfloat16):
    array = jax.random.normal(own_key, dims, jnp.float32) * scale
    if len(shards) > 0:
        array = levels(own_key, dims, shards, -0.22, 0.18) * array
    return jnp.clip(array, min=-bound, max=bound).astype(kind)


def setup_inputs(seed: int = 0, part: int = 0) -> dict:
    keys = jax.random.split(jax.random.key(seed), 5)
    part_splits = jax.random.split(jax.random.fold_in(keys[4], part), 5)
    projections = jnp.clip(2.0 * jax.random.uniform(part_splits[0], (ANGLES, SLICES, W), jnp.float32) ** levels(part_splits[0], (ANGLES, SLICES, W), ((0, 32), (1, 8)), -0.2, 0.2), 0.0, 2.0).astype(jnp.bfloat16)
    flats = jnp.clip(jnp.exp(math.log(3.0) - 1.0986123 * jax.random.uniform(part_splits[1], (SLICES, W), jnp.float32) ** levels(part_splits[1], (SLICES, W), ((0, 8),), -0.2, 0.2)), 1.0, 3.0)
    block_start = set_ends(jax.random.randint(keys[2], (ANGLES, REGIONS), 0, W - CB + 1), jax.random.fold_in(keys[2], 1), 0, W - CB).astype(jnp.int32)
    bp_weights = gaussian(keys[3], (ANGLES, CB, PIX), (ANGLES * CB) ** -0.5, 0.1875, ((2, 32),))
    return dict(projections=projections, flats=flats, block_start=block_start, bp_weights=bp_weights)


paganin_beta = 8.0
ramp_gain = 320.0


def reference(projections, flats, block_start, bp_weights):
    contrast = 1.0 - projections.astype(jnp.float32) / flats[None, :, :]
    padded = jnp.pad(contrast, ((0, 0), (HALO, HALO), (0, 0)))
    tile_count = SLICES // RD
    row_index = (jnp.arange(tile_count, dtype=jnp.int32)[:, None] * RD
                 + jnp.arange(TILE, dtype=jnp.int32)[None, :]).astype(jnp.int32)
    row_freq = jnp.arange(TILE, dtype=jnp.float32)
    col_freq = jnp.arange(W, dtype=jnp.float32)
    lam = (4.0 * jnp.sin(jnp.pi * row_freq / TILE) ** 2)[:, None] + (4.0 * jnp.sin(jnp.pi * col_freq / W) ** 2)[None, :]
    filt = 1.0 / (1.0 + paganin_beta * lam)
    folded = jnp.minimum(col_freq, W - col_freq)
    ramp = ramp_gain * (folded / W) * (0.5 + 0.5 * jnp.cos(2.0 * jnp.pi * folded / W))

    def one_angle(angle_rows):
        tiles = angle_rows[row_index]
        spectrum = jnp.fft.fft2(tiles, axes=(1, 2)) * filt
        back = jnp.real(jnp.fft.ifft2(spectrum, axes=(1, 2)))
        paganin = back[:, HALO:HALO + RD, :].reshape(SLICES, W)
        filtered = jnp.real(jnp.fft.ifft(jnp.fft.fft(paganin, axis=-1) * ramp, axis=-1))
        return filtered.astype(jnp.bfloat16)

    sinogram = lax.map(one_angle, padded)
    offsets = jnp.arange(CB, dtype=jnp.int32)

    def one_region(region):
        starts = lax.dynamic_index_in_dim(block_start, region, 1, keepdims=False)
        index = (starts[:, None] + offsets[None, :]).astype(jnp.int32)
        index = jnp.broadcast_to(index[:, None, :], (ANGLES, SLICES, CB))
        blocks = jnp.take_along_axis(sinogram, index, axis=2)
        weights = lax.dynamic_slice_in_dim(bp_weights, region * PIX_DEV, PIX_DEV, 2)
        return jnp.einsum('asc,acp->sp', blocks.astype(jnp.float32), weights.astype(jnp.float32))

    parts = lax.map(one_region, jnp.arange(REGIONS, dtype=jnp.int32))
    return jnp.transpose(parts, (1, 0, 2)).reshape(SLICES, PIX)
```

```python
from functools import partial

import jax
import jax.numpy as jnp
import numpy as np
from jax import lax
from jax.experimental import pallas as pl
from jax.experimental.pallas import tpu as pltpu
from jax.sharding import PartitionSpec as P

HALO = 4
LANES = 128
SUB = 8

paganin_beta = 8.0
ramp_gain = 320.0
halo_type = jnp.float32
VMEM = pl.BlockSpec(memory_space=pltpu.VMEM)
ANY = pl.BlockSpec(memory_space=pl.ANY)


def tables(width, tile_rows):
    blocks = width // LANES
    half = blocks // 2
    lane = np.arange(LANES)
    ks = np.arange(half + 1)
    turn = 2.0 * np.pi / width * (ks[:, None] * lane[None, :])
    turns = np.stack((np.cos(turn), np.sin(turn))).astype(np.float32)
    angle = 2.0 * np.pi / LANES * (lane[:, None] * lane[None, :] % LANES)
    cos, sin = np.cos(angle), np.sin(angle)
    forward = np.block([[cos, -sin], [sin, cos]])

    def split(matrix):
        high = matrix.astype(jnp.bfloat16)
        low = (matrix - high.astype(np.float64)).astype(jnp.bfloat16)
        return np.stack((high, low))

    freq = (ks[:, None] + blocks * lane[None, :]).astype(np.float64)
    row = np.arange(tile_rows, dtype=np.float64)
    lam = 4.0 * np.sin(np.pi * row / tile_rows)[:, None, None] ** 2 + 4.0 * np.sin(np.pi * freq / width) ** 2
    filt = 1.0 / (1.0 + paganin_beta * lam)
    dist = np.arange(tile_rows // 2 + 1)
    gains = np.einsum("du,ukm->dkm", np.cos(2.0 * np.pi / tile_rows * dist[:, None] * row), filt) / tile_rows
    folded = np.minimum(freq, width - freq)
    ramp = ramp_gain * (folded / width) * (0.5 + 0.5 * np.cos(2.0 * np.pi * folded / width))
    twice = np.where((ks == 0) | (ks == half), 1.0, 2.0)
    gains = gains * (ramp * twice[:, None] / width)
    return turns, split(forward), split(forward.T), gains.astype(np.float32)


def plus(terms):
    return sum(terms[1:], terms[0])


def scaled(terms, weights):
    out = None
    for term, weight in zip(terms, weights):
        weight = float(weight)
        if abs(weight) < 1e-12:
            continue
        piece = term if weight == 1.0 else -term if weight == -1.0 else term * weight
        out = piece if out is None else out + piece
    return out


def cosine_sums(terms, blocks):
    half = blocks // 2
    out = [None] * (half + 1)
    for k in range(half // 2 + 1):
        wave = [np.round(np.cos(2.0 * np.pi * a * k / blocks), 15) for a in range(half + 1)]
        even = scaled(terms[0::2], wave[0::2])
        odd = scaled(terms[1::2], wave[1::2])
        out[k] = even if odd is None else even + odd
        if half - k != k:
            out[half - k] = even if odd is None else even - odd
    return out


def sine_sums(terms, blocks):
    half = blocks // 2
    out = [None] * (half + 1)
    for k in range(1, half // 2 + 1):
        wave = [np.round(np.sin(2.0 * np.pi * a * k / blocks), 15) for a in range(half)]
        even = scaled(terms[2:half:2], wave[2::2])
        odd = scaled(terms[1:half:2], wave[1::2])
        if half - k != k:
            out[k] = plus([x for x in (even, odd) if x is not None])
            out[half - k] = odd - even if even is not None else odd
        else:
            out[k] = plus([x for x in (even, odd) if x is not None])
    return out


def accurate_dot(values, matrix_ref):
    high = values.astype(jnp.bfloat16)
    low = (values - high.astype(jnp.float32)).astype(jnp.bfloat16)
    dot = partial(jnp.dot, preferred_element_type=jnp.float32)
    return dot(high, matrix_ref[0]) + dot(low, matrix_ref[0]) + dot(high, matrix_ref[1])


def spectrum(chunks, turns_ref, forward_ref):
    blocks = len(chunks)
    half = blocks // 2
    folds = [chunks[0]] + [chunks[a] + chunks[blocks - a] for a in range(1, half)] + [chunks[half]]
    skews = [None] + [chunks[a] - chunks[blocks - a] for a in range(1, half)] + [None]
    reals = cosine_sums(folds, blocks)
    imags = sine_sums(skews, blocks)
    parts = []
    for k in range(half + 1):
        cos, sin = turns_ref[0, k : k + 1, :], turns_ref[1, k : k + 1, :]
        if k == 0:
            re, im = reals[0], jnp.zeros_like(reals[0])
        elif imags[k] is None:
            re, im = reals[k] * cos, -(reals[k] * sin)
        else:
            re, im = reals[k] * cos - imags[k] * sin, -(imags[k] * cos) - reals[k] * sin
        parts.append(jnp.concatenate((re, im), axis=1))
    return accurate_dot(jnp.concatenate(parts, axis=0), forward_ref)


def columns(spec, turns_ref, inverse_ref, blocks):
    half = blocks // 2
    back = accurate_dot(spec, inverse_ref)
    reals, imags = [], []
    for k in range(half + 1):
        rows = slice(k * SUB, (k + 1) * SUB)
        re, im = back[rows, :LANES], back[rows, LANES:]
        cos, sin = turns_ref[0, k : k + 1, :], turns_ref[1, k : k + 1, :]
        if k == 0:
            reals.append(re)
            imags.append(None)
        else:
            reals.append(re * cos - im * sin)
            imags.append(im * cos + re * sin if k < half else None)
    even = cosine_sums(reals, blocks)
    odd = sine_sums(imags, blocks)
    out = [None] * blocks
    out[0], out[half] = even[0], even[half]
    for a in range(1, half):
        out[a] = even[a] - odd[a]
        out[blocks - a] = even[a] + odd[a]
    return out


def contrast_kernel(proj_ref, flat_ref, own_ref, first_ref, last_ref):
    own = 1.0 - proj_ref[0].astype(jnp.float32) / flat_ref[...]
    own_ref[...] = own
    first_ref[...] = own[:HALO].astype(first_ref.dtype)
    last_ref[...] = own[SUB - HALO :].astype(last_ref.dtype)


def lanes_of(ref, block):
    return ref[:, block * LANES : (block + 1) * LANES]


def own_kernel(own_ref, turns_ref, forward_ref, gains_ref, out_ref):
    blocks = own_ref.shape[1] // LANES
    spec = spectrum([lanes_of(own_ref, a) for a in range(blocks)], turns_ref, forward_ref)
    row = lax.broadcasted_iota(jnp.int32, (SUB, LANES), 0)
    for k in range(blocks // 2 + 1):
        rows = slice(k * SUB, (k + 1) * SUB)
        for side in (slice(0, LANES), slice(LANES, 2 * LANES)):
            here = spec[rows, side]
            moved = [here] + [pltpu.roll(here, s, axis=0) for s in range(1, SUB)]
            total = here * gains_ref[0, k : k + 1, :]
            for d in range(1, SUB):
                pair = jnp.where(row >= d, moved[d], 0.0) + jnp.where(row < SUB - d, moved[SUB - d], 0.0)
                total += pair * gains_ref[d, k : k + 1, :]
            out_ref[rows, side] = total


def halo_terms(here, row):
    moved = [here] + [pltpu.roll(here, s, axis=0) for s in range(1, SUB)]
    terms = {HALO: moved[0], 2 * HALO: moved[HALO]}
    for d in range(1, HALO):
        s, w = HALO - d, HALO + d
        near_s, near_w = row >= s + HALO, row < w - HALO
        terms[d] = jnp.where(near_s, moved[s], jnp.where(near_w, moved[w], 0.0))
        terms[HALO + s] = jnp.where(near_s, 0.0, moved[s]) + jnp.where(near_w, 0.0, moved[w])
    return terms


def tile_kernel(
    own_ref, above_ref, below_ref, starts_hbm, turns_ref, forward_ref, inverse_ref, gains_ref, out_ref,
    sheet, starts, sem
):
    copy = pltpu.make_async_copy(starts_hbm, starts, sem)
    copy.start()
    blocks = above_ref.shape[1] // LANES
    halo = [
        jnp.concatenate((lanes_of(above_ref, a), lanes_of(below_ref, a)), axis=0).astype(jnp.float32)
        for a in range(blocks)
    ]
    spec = spectrum(halo, turns_ref, forward_ref)
    row = lax.broadcasted_iota(jnp.int32, (SUB, LANES), 0)
    lane = lax.broadcasted_iota(jnp.int32, (SUB, LANES), 1)
    parts = []
    for k in range(blocks // 2 + 1):
        rows = slice(k * SUB, (k + 1) * SUB)
        both = []
        for side in (slice(0, LANES), slice(LANES, 2 * LANES)):
            total = own_ref[rows, side]
            for d, term in halo_terms(spec[rows, side], row).items():
                total += term * gains_ref[d, k : k + 1, :]
            both.append(total)
        parts.append(jnp.concatenate(both, axis=1))
    filtered = columns(jnp.concatenate(parts, axis=0), turns_ref, inverse_ref, blocks)
    for a in range(blocks):
        sheet[:, a * LANES : (a + 1) * LANES] = filtered[a]
    copy.wait()
    regions = starts.shape[1]
    cut = out_ref.shape[0] * LANES // (regions * SUB)
    per = LANES // cut
    keep = lane // cut == row % per
    packed = []
    for group in range(regions // per):
        gathered = None
        for q in range(per):
            start = starts[0, group * per + q]
            block = start // LANES
            offset = start - block * LANES
            after = jnp.minimum(block + 1, blocks - 1)
            here = sheet[:, pl.ds(pl.multiple_of(block * LANES, LANES), LANES)]
            then = sheet[:, pl.ds(pl.multiple_of(after * LANES, LANES), LANES)]
            window = jnp.where(lane >= offset, here, then)
            window = pltpu.roll(window, lax.rem(LANES + q * cut - offset, LANES), axis=1)
            gathered = window if q == 0 else jnp.where(lane // cut == q, window, gathered)
        for shift in range(per):
            moved = gathered if shift == 0 else pltpu.roll(gathered, shift * cut, axis=1)
            packed.append(jnp.where(keep, moved, 0.0).astype(jnp.bfloat16))
    lines = out_ref.shape[0]
    want = lax.broadcasted_iota(jnp.int32, (lines, regions * SUB), 0)
    have = lax.broadcasted_iota(jnp.int32, (lines, regions * SUB), 1)
    have_row, have_shift, have_group = have % SUB, have // SUB % per, have // (SUB * per)
    have_region = have_group * per + (have_row % per + per - have_shift) % per
    pick = jnp.where(have_region * (SUB // per) + have_row // per == want, 1.0, 0.0).astype(jnp.bfloat16)
    out = jnp.dot(pick, jnp.concatenate(packed, axis=0), preferred_element_type=jnp.float32)
    out_ref[...] = out.astype(jnp.bfloat16)


def make_contrast(projections, flats):
    shape = flats.shape
    edge = jax.ShapeDtypeStruct((HALO, shape[1]), halo_type)
    return pl.pallas_call(
        contrast_kernel,
        out_shape=(jax.ShapeDtypeStruct(shape, jnp.float32), edge, edge),
        in_specs=[VMEM] * 2,
        out_specs=(VMEM,) * 3,
        name="contrast",
    )(projections, flats)


def make_own(own, turns, forward, gains):
    lines = turns.shape[1] * SUB
    return pl.pallas_call(
        own_kernel,
        out_shape=jax.ShapeDtypeStruct((lines, 2 * LANES), jnp.float32),
        in_specs=[VMEM] * 4,
        out_specs=VMEM,
        name="own_rows",
    )(own, turns, forward, gains)


def make_tile(own_spec, above, below, starts, turns, forward, inverse, gains, cut):
    regions = starts.shape[1]
    return pl.pallas_call(
        tile_kernel,
        out_shape=jax.ShapeDtypeStruct((regions * SUB * cut // LANES, LANES), jnp.bfloat16),
        in_specs=[VMEM] * 3 + [ANY] + [VMEM] * 4,
        out_specs=VMEM,
        scratch_shapes=[
            pltpu.VMEM((SUB, above.shape[1]), jnp.float32),
            pltpu.SMEM(starts.shape, jnp.int32),
            pltpu.SemaphoreType.DMA,
        ],
        name="tile",
    )(own_spec, above, below, starts, turns, forward, inverse, gains)


def body(projections, flats, block_start, bp_weights):
    angles_dev, rows_dev, width = projections.shape
    assert angles_dev == 1 and rows_dev == SUB and width % (2 * LANES) == 0
    cut = bp_weights.shape[1]
    rows = lax.axis_size("row")
    up = [(i, i + 1) for i in range(rows - 1)]
    down = [(j, i) for i, j in up]
    turns, forward, inverse, gains = (jnp.asarray(t) for t in tables(width, rows_dev + 2 * HALO))
    my_starts = lax.dynamic_slice_in_dim(block_start, lax.axis_index("ang"), 1, 0)
    own, first, last = make_contrast(projections, flats)
    above = lax.ppermute(last, "row", up)
    below = lax.ppermute(first, "row", down)
    own_spec = make_own(own, turns, forward, gains)
    outgoing = make_tile(own_spec, above, below, my_starts, turns, forward, inverse, gains, cut)
    incoming = lax.all_to_all(outgoing, "ang", split_axis=0, concat_axis=0, tiled=True)
    blocks = incoming.reshape(bp_weights.shape[0], rows_dev, cut)
    return lax.dot_general(
        blocks, bp_weights, (((0, 2), (0, 1)), ((), ())), preferred_element_type=jnp.float32
    )


def solution(mesh):
    placed = (P(("scan", "ang"), "row", None), P(("scan", "row"), None), P(), P(None, None, "ang"))
    return jax.shard_map(
        body, mesh=mesh, in_specs=placed, out_specs=P(("scan", "row"), "ang"), check_vma=False
    )
```

```python
from functools import partial

import jax
import jax.numpy as jnp
import numpy as np
from jax import lax
from jax.experimental import pallas as pl
from jax.experimental.pallas import tpu as pltpu
from jax.sharding import PartitionSpec as P

HALO = 4
LANES = 128
SUB = 8

paganin_beta = 8.0
ramp_gain = 320.0
halo_type = jnp.float32
VMEM = pl.BlockSpec(memory_space=pltpu.VMEM)
ANY = pl.BlockSpec(memory_space=pl.ANY)
HBM = pl.BlockSpec(memory_space=pltpu.HBM)
PARAMS = pltpu.CompilerParams(vmem_limit_bytes=8 * 2**20)


def tables(width, tile_rows):
    blocks = width // LANES
    half = blocks // 2
    lane = np.arange(LANES)
    ks = np.arange(half + 1)
    turn = 2.0 * np.pi / width * (ks[:, None] * lane[None, :])
    turns = np.stack((np.cos(turn), np.sin(turn))).astype(np.float32)
    angle = 2.0 * np.pi / LANES * (lane[:, None] * lane[None, :] % LANES)
    cos, sin = np.cos(angle), np.sin(angle)
    forward = np.block([[cos, -sin], [sin, cos]])

    def split(matrix):
        high = matrix.astype(jnp.bfloat16)
        low = (matrix - high.astype(np.float64)).astype(jnp.bfloat16)
        return np.stack((high, low))

    freq = (ks[:, None] + blocks * lane[None, :]).astype(np.float64)
    row = np.arange(tile_rows, dtype=np.float64)
    lam = 4.0 * np.sin(np.pi * row / tile_rows)[:, None, None] ** 2 + 4.0 * np.sin(np.pi * freq / width) ** 2
    filt = 1.0 / (1.0 + paganin_beta * lam)
    dist = np.arange(tile_rows // 2 + 1)
    gains = np.einsum("du,ukm->dkm", np.cos(2.0 * np.pi / tile_rows * dist[:, None] * row), filt) / tile_rows
    folded = np.minimum(freq, width - freq)
    ramp = ramp_gain * (folded / width) * (0.5 + 0.5 * np.cos(2.0 * np.pi * folded / width))
    twice = np.where((ks == 0) | (ks == half), 1.0, 2.0)
    gains = gains * (ramp * twice[:, None] / width)
    return turns, split(forward), split(forward.T), gains.astype(np.float32)


def plus(terms):
    return sum(terms[1:], terms[0])


def scaled(terms, weights):
    out = None
    for term, weight in zip(terms, weights):
        weight = float(weight)
        if abs(weight) < 1e-12:
            continue
        piece = term if weight == 1.0 else -term if weight == -1.0 else term * weight
        out = piece if out is None else out + piece
    return out


def cosine_sums(terms, blocks):
    half = blocks // 2
    out = [None] * (half + 1)
    for k in range(half // 2 + 1):
        wave = [np.round(np.cos(2.0 * np.pi * a * k / blocks), 15) for a in range(half + 1)]
        even = scaled(terms[0::2], wave[0::2])
        odd = scaled(terms[1::2], wave[1::2])
        out[k] = even if odd is None else even + odd
        if half - k != k:
            out[half - k] = even if odd is None else even - odd
    return out


def sine_sums(terms, blocks):
    half = blocks // 2
    out = [None] * (half + 1)
    for k in range(1, half // 2 + 1):
        wave = [np.round(np.sin(2.0 * np.pi * a * k / blocks), 15) for a in range(half)]
        even = scaled(terms[2:half:2], wave[2::2])
        odd = scaled(terms[1:half:2], wave[1::2])
        if half - k != k:
            out[k] = plus([x for x in (even, odd) if x is not None])
            out[half - k] = odd - even if even is not None else odd
        else:
            out[k] = plus([x for x in (even, odd) if x is not None])
    return out


def accurate_dot(values, matrix_ref):
    high = values.astype(jnp.bfloat16)
    low = (values - high.astype(jnp.float32)).astype(jnp.bfloat16)
    dot = partial(jnp.dot, preferred_element_type=jnp.float32)
    return dot(high, matrix_ref[0]) + dot(low, matrix_ref[0]) + dot(high, matrix_ref[1])


def spectrum(chunks, turns_ref, forward_ref):
    blocks = len(chunks)
    half = blocks // 2
    folds = [chunks[0]] + [chunks[a] + chunks[blocks - a] for a in range(1, half)] + [chunks[half]]
    skews = [None] + [chunks[a] - chunks[blocks - a] for a in range(1, half)] + [None]
    reals = cosine_sums(folds, blocks)
    imags = sine_sums(skews, blocks)
    parts = []
    for k in range(half + 1):
        cos, sin = turns_ref[0, k : k + 1, :], turns_ref[1, k : k + 1, :]
        if k == 0:
            re, im = reals[0], jnp.zeros_like(reals[0])
        elif imags[k] is None:
            re, im = reals[k] * cos, -(reals[k] * sin)
        else:
            re, im = reals[k] * cos - imags[k] * sin, -(imags[k] * cos) - reals[k] * sin
        parts.append(jnp.concatenate((re, im), axis=1))
    return accurate_dot(jnp.concatenate(parts, axis=0), forward_ref)


def columns(spec, turns_ref, inverse_ref, blocks):
    half = blocks // 2
    back = accurate_dot(spec, inverse_ref)
    reals, imags = [], []
    for k in range(half + 1):
        rows = slice(k * SUB, (k + 1) * SUB)
        re, im = back[rows, :LANES], back[rows, LANES:]
        cos, sin = turns_ref[0, k : k + 1, :], turns_ref[1, k : k + 1, :]
        if k == 0:
            reals.append(re)
            imags.append(None)
        else:
            reals.append(re * cos - im * sin)
            imags.append(im * cos + re * sin if k < half else None)
    even = cosine_sums(reals, blocks)
    odd = sine_sums(imags, blocks)
    out = [None] * blocks
    out[0], out[half] = even[0], even[half]
    for a in range(1, half):
        out[a] = even[a] - odd[a]
        out[blocks - a] = even[a] + odd[a]
    return out


def contrast_kernel(proj_hbm, flat_hbm, own_ref, first_ref, last_ref, proj, flat, sems):
    copies = [
        pltpu.make_async_copy(proj_hbm, proj, sems.at[0]),
        pltpu.make_async_copy(flat_hbm, flat, sems.at[1]),
    ]
    for copy in copies:
        copy.start()
    for copy in copies:
        copy.wait()
    own = 1.0 - proj[0].astype(jnp.float32) / flat[...]
    own_ref[...] = own
    first_ref[...] = own[:HALO].astype(first_ref.dtype)
    last_ref[...] = own[SUB - HALO :].astype(last_ref.dtype)


def lanes_of(ref, block):
    return ref[:, block * LANES : (block + 1) * LANES]


def own_kernel(own_ref, turns_ref, forward_ref, gains_ref, out_ref):
    blocks = own_ref.shape[1] // LANES
    spec = spectrum([lanes_of(own_ref, a) for a in range(blocks)], turns_ref, forward_ref)
    row = lax.broadcasted_iota(jnp.int32, (SUB, LANES), 0)
    for k in range(blocks // 2 + 1):
        rows = slice(k * SUB, (k + 1) * SUB)
        for side in (slice(0, LANES), slice(LANES, 2 * LANES)):
            here = spec[rows, side]
            moved = [here] + [pltpu.roll(here, s, axis=0) for s in range(1, SUB)]
            total = here * gains_ref[0, k : k + 1, :]
            for d in range(1, SUB):
                pair = jnp.where(row >= d, moved[d], 0.0) + jnp.where(row < SUB - d, moved[SUB - d], 0.0)
                total += pair * gains_ref[d, k : k + 1, :]
            out_ref[rows, side] = total


def halo_terms(here, row):
    moved = [here] + [pltpu.roll(here, s, axis=0) for s in range(1, SUB)]
    terms = {HALO: moved[0], 2 * HALO: moved[HALO]}
    for d in range(1, HALO):
        s, w = HALO - d, HALO + d
        near_s, near_w = row >= s + HALO, row < w - HALO
        terms[d] = jnp.where(near_s, moved[s], jnp.where(near_w, moved[w], 0.0))
        terms[HALO + s] = jnp.where(near_s, 0.0, moved[s]) + jnp.where(near_w, 0.0, moved[w])
    return terms


def tile_kernel(
    own_ref, above_ref, below_ref, starts_hbm, turns_ref, forward_ref, inverse_ref, gains_ref, out_ref,
    sheet, starts, sem
):
    copy = pltpu.make_async_copy(starts_hbm, starts, sem)
    copy.start()
    blocks = above_ref.shape[1] // LANES
    halo = [
        jnp.concatenate((lanes_of(above_ref, a), lanes_of(below_ref, a)), axis=0).astype(jnp.float32)
        for a in range(blocks)
    ]
    spec = spectrum(halo, turns_ref, forward_ref)
    row = lax.broadcasted_iota(jnp.int32, (SUB, LANES), 0)
    lane = lax.broadcasted_iota(jnp.int32, (SUB, LANES), 1)
    parts = []
    for k in range(blocks // 2 + 1):
        rows = slice(k * SUB, (k + 1) * SUB)
        both = []
        for side in (slice(0, LANES), slice(LANES, 2 * LANES)):
            total = own_ref[rows, side]
            for d, term in halo_terms(spec[rows, side], row).items():
                total += term * gains_ref[d, k : k + 1, :]
            both.append(total)
        parts.append(jnp.concatenate(both, axis=1))
    filtered = columns(jnp.concatenate(parts, axis=0), turns_ref, inverse_ref, blocks)
    for a in range(blocks):
        sheet[:, a * LANES : (a + 1) * LANES] = filtered[a]
    copy.wait()
    mine = lax.axis_index("ang")
    regions = starts.shape[1]
    cut = out_ref.shape[0] * LANES // (regions * SUB)
    per = LANES // cut
    keep = lane // cut == row % per
    packed = []
    for group in range(regions // per):
        gathered = None
        for q in range(per):
            start = starts[mine, group * per + q]
            block = start // LANES
            offset = start - block * LANES
            after = jnp.minimum(block + 1, blocks - 1)
            here = sheet[:, pl.ds(pl.multiple_of(block * LANES, LANES), LANES)]
            then = sheet[:, pl.ds(pl.multiple_of(after * LANES, LANES), LANES)]
            window = jnp.where(lane >= offset, here, then)
            window = pltpu.roll(window, lax.rem(LANES + q * cut - offset, LANES), axis=1)
            gathered = window if q == 0 else jnp.where(lane // cut == q, window, gathered)
        for shift in range(per):
            moved = gathered if shift == 0 else pltpu.roll(gathered, shift * cut, axis=1)
            packed.append(jnp.where(keep, moved, 0.0).astype(jnp.bfloat16))
    lines = out_ref.shape[0]
    want = lax.broadcasted_iota(jnp.int32, (lines, regions * SUB), 0)
    have = lax.broadcasted_iota(jnp.int32, (lines, regions * SUB), 1)
    have_row, have_shift, have_group = have % SUB, have // SUB % per, have // (SUB * per)
    have_region = have_group * per + (have_row % per + per - have_shift) % per
    pick = jnp.where(have_region * (SUB // per) + have_row // per == want, 1.0, 0.0).astype(jnp.bfloat16)
    out = jnp.dot(pick, jnp.concatenate(packed, axis=0), preferred_element_type=jnp.float32)
    out_ref[...] = out.astype(jnp.bfloat16)


def make_contrast(projections, flats):
    shape = flats.shape
    edge = jax.ShapeDtypeStruct((HALO, shape[1]), halo_type)
    return pl.pallas_call(
        contrast_kernel,
        out_shape=(jax.ShapeDtypeStruct(shape, jnp.float32), edge, edge),
        in_specs=[HBM] * 2,
        out_specs=(VMEM,) * 3,
        scratch_shapes=[
            pltpu.VMEM(projections.shape, projections.dtype),
            pltpu.VMEM(flats.shape, flats.dtype),
            pltpu.SemaphoreType.DMA((2,)),
        ],
        compiler_params=PARAMS,
        name="contrast",
    )(projections, flats)


def make_own(own, turns, forward, gains):
    lines = turns.shape[1] * SUB
    return pl.pallas_call(
        own_kernel,
        out_shape=jax.ShapeDtypeStruct((lines, 2 * LANES), jnp.float32),
        in_specs=[VMEM] * 4,
        out_specs=VMEM,
        compiler_params=PARAMS,
        name="own_rows",
    )(own, turns, forward, gains)


def make_tile(own_spec, above, below, starts, turns, forward, inverse, gains, cut):
    regions = starts.shape[1]
    return pl.pallas_call(
        tile_kernel,
        out_shape=jax.ShapeDtypeStruct((regions * SUB * cut // LANES, LANES), jnp.bfloat16),
        in_specs=[VMEM] * 3 + [ANY] + [VMEM] * 4,
        out_specs=VMEM,
        scratch_shapes=[
            pltpu.VMEM((SUB, above.shape[1]), jnp.float32),
            pltpu.SMEM(starts.shape, jnp.int32),
            pltpu.SemaphoreType.DMA,
        ],
        compiler_params=PARAMS,
        name="tile",
    )(own_spec, above, below, starts, turns, forward, inverse, gains)


def body(projections, flats, block_start, bp_weights):
    angles_dev, rows_dev, width = projections.shape
    assert angles_dev == 1 and rows_dev == SUB and width % (2 * LANES) == 0
    cut = bp_weights.shape[1]
    rows = lax.axis_size("row")
    up = [(i, i + 1) for i in range(rows - 1)]
    down = [(j, i) for i, j in up]
    turns, forward, inverse, gains = (jnp.asarray(t) for t in tables(width, rows_dev + 2 * HALO))
    in_hbm = partial(pltpu.with_memory_space_constraint, memory_space=pltpu.HBM)
    own, first, last = make_contrast(in_hbm(projections), in_hbm(flats))
    above = lax.ppermute(last, "row", up)
    below = lax.ppermute(first, "row", down)
    own_spec = make_own(own, turns, forward, gains)
    outgoing = make_tile(own_spec, above, below, block_start, turns, forward, inverse, gains, cut)
    incoming = lax.all_to_all(outgoing, "ang", split_axis=0, concat_axis=0, tiled=True)
    blocks = incoming.reshape(bp_weights.shape[0], rows_dev, cut)
    return lax.dot_general(
        blocks, bp_weights, (((0, 2), (0, 1)), ((), ())), preferred_element_type=jnp.float32
    )


def solution(mesh):
    placed = (P(("scan", "ang"), "row", None), P(("scan", "row"), None), P(), P(None, None, "ang"))
    return jax.shard_map(
        body, mesh=mesh, in_specs=placed, out_specs=P(("scan", "row"), "ang"), check_vma=False
    )
```

```python
from functools import partial

import jax
import jax.numpy as jnp
import numpy as np
from jax import lax
from jax.experimental import pallas as pl
from jax.experimental.pallas import tpu as pltpu
from jax.sharding import PartitionSpec as P

HALO = 4
LANES = 128
SUB = 8

paganin_beta = 8.0
ramp_gain = 320.0
halo_type = jnp.float32
VMEM = pl.BlockSpec(memory_space=pltpu.VMEM)
ANY = pl.BlockSpec(memory_space=pl.ANY)
HBM = pl.BlockSpec(memory_space=pltpu.HBM)
PARAMS = pltpu.CompilerParams(vmem_limit_bytes=8 * 2**20)


def tables(width, tile_rows):
    blocks = width // LANES
    half = blocks // 2
    lane = np.arange(LANES)
    ks = np.arange(half + 1)
    turn = 2.0 * np.pi / width * (ks[:, None] * lane[None, :])
    turns = np.stack((np.cos(turn), np.sin(turn))).astype(np.float32)
    angle = 2.0 * np.pi / LANES * (lane[:, None] * lane[None, :] % LANES)
    cos, sin = np.cos(angle), np.sin(angle)
    forward = np.block([[cos, -sin], [sin, cos]])

    def split(matrix):
        high = matrix.astype(jnp.bfloat16)
        low = (matrix - high.astype(np.float64)).astype(jnp.bfloat16)
        return np.stack((high, low))

    freq = (ks[:, None] + blocks * lane[None, :]).astype(np.float64)
    row = np.arange(tile_rows, dtype=np.float64)
    lam = 4.0 * np.sin(np.pi * row / tile_rows)[:, None, None] ** 2 + 4.0 * np.sin(np.pi * freq / width) ** 2
    filt = 1.0 / (1.0 + paganin_beta * lam)
    dist = np.arange(tile_rows // 2 + 1)
    gains = np.einsum("du,ukm->dkm", np.cos(2.0 * np.pi / tile_rows * dist[:, None] * row), filt) / tile_rows
    folded = np.minimum(freq, width - freq)
    ramp = ramp_gain * (folded / width) * (0.5 + 0.5 * np.cos(2.0 * np.pi * folded / width))
    twice = np.where((ks == 0) | (ks == half), 1.0, 2.0)
    gains = gains * (ramp * twice[:, None] / width)
    return turns, split(forward), split(forward.T), gains.astype(np.float32)


def plus(terms):
    return sum(terms[1:], terms[0])


def scaled(terms, weights):
    out = None
    for term, weight in zip(terms, weights):
        weight = float(weight)
        if abs(weight) < 1e-12:
            continue
        piece = term if weight == 1.0 else -term if weight == -1.0 else term * weight
        out = piece if out is None else out + piece
    return out


def cosine_sums(terms, blocks):
    half = blocks // 2
    out = [None] * (half + 1)
    for k in range(half // 2 + 1):
        wave = [np.round(np.cos(2.0 * np.pi * a * k / blocks), 15) for a in range(half + 1)]
        even = scaled(terms[0::2], wave[0::2])
        odd = scaled(terms[1::2], wave[1::2])
        out[k] = even if odd is None else even + odd
        if half - k != k:
            out[half - k] = even if odd is None else even - odd
    return out


def sine_sums(terms, blocks):
    half = blocks // 2
    out = [None] * (half + 1)
    for k in range(1, half // 2 + 1):
        wave = [np.round(np.sin(2.0 * np.pi * a * k / blocks), 15) for a in range(half)]
        even = scaled(terms[2:half:2], wave[2::2])
        odd = scaled(terms[1:half:2], wave[1::2])
        if half - k != k:
            out[k] = plus([x for x in (even, odd) if x is not None])
            out[half - k] = odd - even if even is not None else odd
        else:
            out[k] = plus([x for x in (even, odd) if x is not None])
    return out


def accurate_dot(values, matrix_ref):
    high = values.astype(jnp.bfloat16)
    low = (values - high.astype(jnp.float32)).astype(jnp.bfloat16)
    dot = partial(jnp.dot, preferred_element_type=jnp.float32)
    return dot(high, matrix_ref[0]) + dot(low, matrix_ref[0]) + dot(high, matrix_ref[1])


def spectrum(chunks, turns_ref, forward_ref):
    blocks = len(chunks)
    half = blocks // 2
    folds = [chunks[0]] + [chunks[a] + chunks[blocks - a] for a in range(1, half)] + [chunks[half]]
    skews = [None] + [chunks[a] - chunks[blocks - a] for a in range(1, half)] + [None]
    reals = cosine_sums(folds, blocks)
    imags = sine_sums(skews, blocks)
    parts = []
    for k in range(half + 1):
        cos, sin = turns_ref[0, k : k + 1, :], turns_ref[1, k : k + 1, :]
        if k == 0:
            re, im = reals[0], jnp.zeros_like(reals[0])
        elif imags[k] is None:
            re, im = reals[k] * cos, -(reals[k] * sin)
        else:
            re, im = reals[k] * cos - imags[k] * sin, -(imags[k] * cos) - reals[k] * sin
        parts.append(jnp.concatenate((re, im), axis=1))
    return accurate_dot(jnp.concatenate(parts, axis=0), forward_ref)


def columns(spec, turns_ref, inverse_ref, blocks):
    half = blocks // 2
    back = accurate_dot(spec, inverse_ref)
    reals, imags = [], []
    for k in range(half + 1):
        rows = slice(k * SUB, (k + 1) * SUB)
        re, im = back[rows, :LANES], back[rows, LANES:]
        cos, sin = turns_ref[0, k : k + 1, :], turns_ref[1, k : k + 1, :]
        if k == 0:
            reals.append(re)
            imags.append(None)
        else:
            reals.append(re * cos - im * sin)
            imags.append(im * cos + re * sin if k < half else None)
    even = cosine_sums(reals, blocks)
    odd = sine_sums(imags, blocks)
    out = [None] * blocks
    out[0], out[half] = even[0], even[half]
    for a in range(1, half):
        out[a] = even[a] - odd[a]
        out[blocks - a] = even[a] + odd[a]
    return out


def contrast_kernel(proj_hbm, flat_hbm, own_ref, first_ref, last_ref, proj, flat, sems):
    copies = [
        pltpu.make_async_copy(proj_hbm, proj, sems.at[0]),
        pltpu.make_async_copy(flat_hbm, flat, sems.at[1]),
    ]
    for copy in copies:
        copy.start()
    for copy in copies:
        copy.wait()
    own = 1.0 - proj[0].astype(jnp.float32) / flat[...]
    own_ref[...] = own
    first_ref[...] = own[:HALO].astype(first_ref.dtype)
    last_ref[...] = own[SUB - HALO :].astype(last_ref.dtype)


def lanes_of(ref, block):
    return ref[:, block * LANES : (block + 1) * LANES]


def own_kernel(own_ref, turns_ref, forward_ref, gains_ref, out_ref):
    blocks = own_ref.shape[1] // LANES
    spec = spectrum([lanes_of(own_ref, a) for a in range(blocks)], turns_ref, forward_ref)
    row = lax.broadcasted_iota(jnp.int32, (SUB, LANES), 0)
    for k in range(blocks // 2 + 1):
        rows = slice(k * SUB, (k + 1) * SUB)
        for side in (slice(0, LANES), slice(LANES, 2 * LANES)):
            here = spec[rows, side]
            moved = [here] + [pltpu.roll(here, s, axis=0) for s in range(1, SUB)]
            total = here * gains_ref[0, k : k + 1, :]
            for d in range(1, SUB):
                pair = jnp.where(row >= d, moved[d], 0.0) + jnp.where(row < SUB - d, moved[SUB - d], 0.0)
                total += pair * gains_ref[d, k : k + 1, :]
            out_ref[rows, side] = total


def halo_terms(here, row):
    moved = [here] + [pltpu.roll(here, s, axis=0) for s in range(1, SUB)]
    terms = {HALO: moved[0], 2 * HALO: moved[HALO]}
    for d in range(1, HALO):
        s, w = HALO - d, HALO + d
        near_s, near_w = row >= s + HALO, row < w - HALO
        terms[d] = jnp.where(near_s, moved[s], jnp.where(near_w, moved[w], 0.0))
        terms[HALO + s] = jnp.where(near_s, 0.0, moved[s]) + jnp.where(near_w, 0.0, moved[w])
    return terms


def tile_kernel(
    own_ref, below_ref, above_ref, starts_hbm, turns_ref, forward_ref, inverse_ref, gains_ref, out_ref,
    sheet, starts, sem
):
    copy = pltpu.make_async_copy(starts_hbm, starts, sem)
    copy.start()
    blocks = above_ref.shape[1] // LANES
    halo = [
        jnp.concatenate((lanes_of(above_ref, a), lanes_of(below_ref, a)), axis=0).astype(jnp.float32)
        for a in range(blocks)
    ]
    spec = spectrum(halo, turns_ref, forward_ref)
    row = lax.broadcasted_iota(jnp.int32, (SUB, LANES), 0)
    lane = lax.broadcasted_iota(jnp.int32, (SUB, LANES), 1)
    parts = []
    for k in range(blocks // 2 + 1):
        rows = slice(k * SUB, (k + 1) * SUB)
        both = []
        for side in (slice(0, LANES), slice(LANES, 2 * LANES)):
            total = own_ref[rows, side]
            for d, term in halo_terms(spec[rows, side], row).items():
                total += term * gains_ref[d, k : k + 1, :]
            both.append(total)
        parts.append(jnp.concatenate(both, axis=1))
    filtered = columns(jnp.concatenate(parts, axis=0), turns_ref, inverse_ref, blocks)
    for a in range(blocks):
        sheet[:, a * LANES : (a + 1) * LANES] = filtered[a]
    copy.wait()
    mine = lax.axis_index("ang")
    regions = starts.shape[1]
    cut = out_ref.shape[0] * LANES // (regions * SUB)
    per = LANES // cut
    keep = lane // cut == row % per
    packed = []
    for group in range(regions // per):
        gathered = None
        for q in range(per):
            start = starts[mine, group * per + q]
            block = start // LANES
            offset = start - block * LANES
            after = jnp.minimum(block + 1, blocks - 1)
            here = sheet[:, pl.ds(pl.multiple_of(block * LANES, LANES), LANES)]
            then = sheet[:, pl.ds(pl.multiple_of(after * LANES, LANES), LANES)]
            window = jnp.where(lane >= offset, here, then)
            window = pltpu.roll(window, lax.rem(LANES + q * cut - offset, LANES), axis=1)
            gathered = window if q == 0 else jnp.where(lane // cut == q, window, gathered)
        for shift in range(per):
            moved = gathered if shift == 0 else pltpu.roll(gathered, shift * cut, axis=1)
            packed.append(jnp.where(keep, moved, 0.0).astype(jnp.bfloat16))
    lines = out_ref.shape[0]
    want = lax.broadcasted_iota(jnp.int32, (lines, regions * SUB), 0)
    have = lax.broadcasted_iota(jnp.int32, (lines, regions * SUB), 1)
    have_row, have_shift, have_group = have % SUB, have // SUB % per, have // (SUB * per)
    have_region = have_group * per + (have_row % per + per - have_shift) % per
    pick = jnp.where(have_region * (SUB // per) + have_row // per == want, 1.0, 0.0).astype(jnp.bfloat16)
    out = jnp.dot(pick, jnp.concatenate(packed, axis=0), preferred_element_type=jnp.float32)
    out_ref[...] = out.astype(jnp.bfloat16)


def make_contrast(projections, flats):
    shape = flats.shape
    edge = jax.ShapeDtypeStruct((HALO, shape[1]), halo_type)
    return pl.pallas_call(
        contrast_kernel,
        out_shape=(jax.ShapeDtypeStruct(shape, jnp.float32), edge, edge),
        in_specs=[HBM] * 2,
        out_specs=(VMEM,) * 3,
        scratch_shapes=[
            pltpu.VMEM(projections.shape, projections.dtype),
            pltpu.VMEM(flats.shape, flats.dtype),
            pltpu.SemaphoreType.DMA((2,)),
        ],
        compiler_params=PARAMS,
        name="contrast",
    )(projections, flats)


def make_own(own, turns, forward, gains):
    lines = turns.shape[1] * SUB
    return pl.pallas_call(
        own_kernel,
        out_shape=jax.ShapeDtypeStruct((lines, 2 * LANES), jnp.float32),
        in_specs=[VMEM] * 4,
        out_specs=VMEM,
        compiler_params=PARAMS,
        name="own_rows",
    )(own, turns, forward, gains)


def make_tile(own_spec, below, above, starts, turns, forward, inverse, gains, cut):
    regions = starts.shape[1]
    return pl.pallas_call(
        tile_kernel,
        out_shape=jax.ShapeDtypeStruct((regions * SUB * cut // LANES, LANES), jnp.bfloat16),
        in_specs=[VMEM] * 3 + [ANY] + [VMEM] * 4,
        out_specs=VMEM,
        scratch_shapes=[
            pltpu.VMEM((SUB, above.shape[1]), jnp.float32),
            pltpu.SMEM(starts.shape, jnp.int32),
            pltpu.SemaphoreType.DMA,
        ],
        compiler_params=PARAMS,
        name="tile",
    )(own_spec, below, above, starts, turns, forward, inverse, gains)


def body(projections, flats, block_start, bp_weights):
    angles_dev, rows_dev, width = projections.shape
    assert angles_dev == 1 and rows_dev == SUB and width % (2 * LANES) == 0
    cut = bp_weights.shape[1]
    rows = lax.axis_size("row")
    up = [(i, i + 1) for i in range(rows - 1)]
    down = [(j, i) for i, j in up]
    turns, forward, inverse, gains = (jnp.asarray(t) for t in tables(width, rows_dev + 2 * HALO))
    in_hbm = partial(pltpu.with_memory_space_constraint, memory_space=pltpu.HBM)
    own, first, last = make_contrast(in_hbm(projections), in_hbm(flats))
    below = lax.ppermute(first, "row", down)
    above = lax.ppermute(last, "row", up)
    own_spec = make_own(own, turns, forward, gains)
    outgoing = make_tile(own_spec, below, above, block_start, turns, forward, inverse, gains, cut)
    incoming = lax.all_to_all(outgoing, "ang", split_axis=0, concat_axis=0, tiled=True)
    blocks = incoming.reshape(bp_weights.shape[0], rows_dev, cut)
    return lax.dot_general(
        blocks, bp_weights, (((0, 2), (0, 1)), ((), ())), preferred_element_type=jnp.float32
    )


def solution(mesh):
    placed = (P(("scan", "ang"), "row", None), P(("scan", "row"), None), P(), P(None, None, "ang"))
    return jax.shard_map(
        body, mesh=mesh, in_specs=placed, out_specs=P(("scan", "row"), "ang"), check_vma=False
    )
```

```python
from functools import partial

import jax
import jax.numpy as jnp
import numpy as np
from jax import lax
from jax.experimental import pallas as pl
from jax.experimental.pallas import tpu as pltpu
from jax.sharding import PartitionSpec as P

HALO = 4
LANES = 128
SUB = 8

paganin_beta = 8.0
ramp_gain = 320.0
halo_type = jnp.float32
VMEM = pl.BlockSpec(memory_space=pltpu.VMEM)
ANY = pl.BlockSpec(memory_space=pl.ANY)
HBM = pl.BlockSpec(memory_space=pltpu.HBM)
PARAMS = pltpu.CompilerParams(vmem_limit_bytes=8 * 2**20)


def tables(width, tile_rows):
    blocks = width // LANES
    half = blocks // 2
    lane = np.arange(LANES)
    ks = np.arange(half + 1)
    turn = 2.0 * np.pi / width * (ks[:, None] * lane[None, :])
    turns = np.stack((np.cos(turn), np.sin(turn))).astype(np.float32)
    angle = 2.0 * np.pi / LANES * (lane[:, None] * lane[None, :] % LANES)
    cos, sin = np.cos(angle), np.sin(angle)
    forward = np.block([[cos, -sin], [sin, cos]])

    def split(matrix):
        high = matrix.astype(jnp.bfloat16)
        low = (matrix - high.astype(np.float64)).astype(jnp.bfloat16)
        return np.stack((high, low))

    freq = (ks[:, None] + blocks * lane[None, :]).astype(np.float64)
    row = np.arange(tile_rows, dtype=np.float64)
    lam = 4.0 * np.sin(np.pi * row / tile_rows)[:, None, None] ** 2 + 4.0 * np.sin(np.pi * freq / width) ** 2
    filt = 1.0 / (1.0 + paganin_beta * lam)
    dist = np.arange(tile_rows // 2 + 1)
    gains = np.einsum("du,ukm->dkm", np.cos(2.0 * np.pi / tile_rows * dist[:, None] * row), filt) / tile_rows
    folded = np.minimum(freq, width - freq)
    ramp = ramp_gain * (folded / width) * (0.5 + 0.5 * np.cos(2.0 * np.pi * folded / width))
    twice = np.where((ks == 0) | (ks == half), 1.0, 2.0)
    gains = gains * (ramp * twice[:, None] / width)
    rows_dev = tile_rows - 2 * HALO
    out_row = np.arange(rows_dev)
    halo_row = (out_row[None, :] - np.arange(rows_dev)[:, None]) % rows_dev
    apart = np.abs(out_row[None, :] + HALO - np.where(halo_row < HALO, halo_row, halo_row + rows_dev))
    apart = np.minimum(apart, tile_rows - apart)
    halo_gains = np.transpose(gains[apart], (0, 2, 1, 3))
    return turns, split(forward), split(forward.T), gains.astype(np.float32), halo_gains.astype(np.float32)


def plus(terms):
    return sum(terms[1:], terms[0])


def scaled(terms, weights):
    out = None
    for term, weight in zip(terms, weights):
        weight = float(weight)
        if abs(weight) < 1e-12:
            continue
        piece = term if weight == 1.0 else -term if weight == -1.0 else term * weight
        out = piece if out is None else out + piece
    return out


def cosine_sums(terms, blocks):
    half = blocks // 2
    out = [None] * (half + 1)
    for k in range(half // 2 + 1):
        wave = [np.round(np.cos(2.0 * np.pi * a * k / blocks), 15) for a in range(half + 1)]
        even = scaled(terms[0::2], wave[0::2])
        odd = scaled(terms[1::2], wave[1::2])
        out[k] = even if odd is None else even + odd
        if half - k != k:
            out[half - k] = even if odd is None else even - odd
    return out


def sine_sums(terms, blocks):
    half = blocks // 2
    out = [None] * (half + 1)
    for k in range(1, half // 2 + 1):
        wave = [np.round(np.sin(2.0 * np.pi * a * k / blocks), 15) for a in range(half)]
        even = scaled(terms[2:half:2], wave[2::2])
        odd = scaled(terms[1:half:2], wave[1::2])
        if half - k != k:
            out[k] = plus([x for x in (even, odd) if x is not None])
            out[half - k] = odd - even if even is not None else odd
        else:
            out[k] = plus([x for x in (even, odd) if x is not None])
    return out


def accurate_dot(values, matrix_ref):
    high = values.astype(jnp.bfloat16)
    low = (values - high.astype(jnp.float32)).astype(jnp.bfloat16)
    dot = partial(jnp.dot, preferred_element_type=jnp.float32)
    lines = values.shape[0]
    both = dot(jnp.concatenate((high, low), axis=0), matrix_ref[0])
    return both[:lines] + (both[lines:] + dot(high, matrix_ref[1]))


def spectrum(chunks, turns_ref, forward_ref):
    blocks = len(chunks)
    half = blocks // 2
    folds = [chunks[0]] + [chunks[a] + chunks[blocks - a] for a in range(1, half)] + [chunks[half]]
    skews = [None] + [chunks[a] - chunks[blocks - a] for a in range(1, half)] + [None]
    reals = cosine_sums(folds, blocks)
    imags = sine_sums(skews, blocks)
    parts = []
    for k in range(half + 1):
        cos, sin = turns_ref[0, k : k + 1, :], turns_ref[1, k : k + 1, :]
        if k == 0:
            re, im = reals[0], jnp.zeros_like(reals[0])
        elif imags[k] is None:
            re, im = reals[k] * cos, -(reals[k] * sin)
        else:
            re, im = reals[k] * cos - imags[k] * sin, -(imags[k] * cos) - reals[k] * sin
        parts.append(jnp.concatenate((re, im), axis=1))
    return accurate_dot(jnp.concatenate(parts, axis=0), forward_ref)


def columns(spec, turns_ref, inverse_ref, blocks):
    half = blocks // 2
    back = accurate_dot(spec, inverse_ref)
    reals, imags = [], []
    for k in range(half + 1):
        rows = slice(k * SUB, (k + 1) * SUB)
        re, im = back[rows, :LANES], back[rows, LANES:]
        cos, sin = turns_ref[0, k : k + 1, :], turns_ref[1, k : k + 1, :]
        if k == 0:
            reals.append(re)
            imags.append(None)
        else:
            reals.append(re * cos - im * sin)
            imags.append(im * cos + re * sin if k < half else None)
    even = cosine_sums(reals, blocks)
    odd = sine_sums(imags, blocks)
    out = [None] * blocks
    out[0], out[half] = even[0], even[half]
    for a in range(1, half):
        out[a] = even[a] - odd[a]
        out[blocks - a] = even[a] + odd[a]
    return out


def contrast_kernel(proj_hbm, flat_hbm, own_ref, first_ref, last_ref, proj, flat, sems):
    copies = [
        pltpu.make_async_copy(proj_hbm, proj, sems.at[0]),
        pltpu.make_async_copy(flat_hbm, flat, sems.at[1]),
    ]
    for copy in copies:
        copy.start()
    for copy in copies:
        copy.wait()
    own = 1.0 - proj[0].astype(jnp.float32) / flat[...]
    own_ref[...] = own
    first_ref[...] = own[:HALO].astype(first_ref.dtype)
    last_ref[...] = own[SUB - HALO :].astype(last_ref.dtype)


def lanes_of(ref, block):
    return ref[:, block * LANES : (block + 1) * LANES]


def own_kernel(own_ref, turns_ref, forward_ref, gains_ref, out_ref):
    blocks = own_ref.shape[1] // LANES
    spec = spectrum([lanes_of(own_ref, a) for a in range(blocks)], turns_ref, forward_ref)
    row = lax.broadcasted_iota(jnp.int32, (SUB, LANES), 0)
    for k in range(blocks // 2 + 1):
        rows = slice(k * SUB, (k + 1) * SUB)
        for side in (slice(0, LANES), slice(LANES, 2 * LANES)):
            here = spec[rows, side]
            moved = [here] + [pltpu.roll(here, s, axis=0) for s in range(1, SUB)]
            total = here * gains_ref[0, k : k + 1, :]
            for d in range(1, SUB):
                pair = jnp.where(row >= d, moved[d], 0.0) + jnp.where(row < SUB - d, moved[SUB - d], 0.0)
                total += pair * gains_ref[d, k : k + 1, :]
            out_ref[rows, side] = total


def tile_kernel(
    own_ref, below_ref, above_ref, starts_hbm, turns_ref, forward_ref, inverse_ref, gains_ref, out_ref,
    sheet, starts, sem
):
    copy = pltpu.make_async_copy(starts_hbm, starts, sem)
    copy.start()
    blocks = above_ref.shape[1] // LANES
    halo = [
        jnp.concatenate((lanes_of(above_ref, a), lanes_of(below_ref, a)), axis=0).astype(jnp.float32)
        for a in range(blocks)
    ]
    spec = spectrum(halo, turns_ref, forward_ref)
    copy.wait()
    mine = lax.axis_index("ang")
    row = lax.broadcasted_iota(jnp.int32, (SUB, LANES), 0)
    lane = lax.broadcasted_iota(jnp.int32, (SUB, LANES), 1)
    parts = []
    for k in range(blocks // 2 + 1):
        rows = slice(k * SUB, (k + 1) * SUB)
        both = []
        for side in (slice(0, LANES), slice(LANES, 2 * LANES)):
            here = spec[rows, side]
            total = own_ref[rows, side] + here * gains_ref[0, k]
            for s in range(1, SUB):
                total += pltpu.roll(here, s, axis=0) * gains_ref[s, k]
            both.append(total)
        parts.append(jnp.concatenate(both, axis=1))
    filtered = columns(jnp.concatenate(parts, axis=0), turns_ref, inverse_ref, blocks)
    for a in range(blocks):
        sheet[a] = filtered[a]
    regions = starts.shape[1]
    cut = out_ref.shape[0] * LANES // (regions * SUB)
    per = LANES // cut
    keep = lane // cut == row % per
    packed = []
    for group in range(regions // per):
        gathered = None
        for q in range(per):
            start = starts[mine, group * per + q]
            block = lax.shift_right_logical(start, 7)
            offset = start & (LANES - 1)
            window = jnp.where(lane >= offset, sheet[block], sheet[block + 1])
            window = pltpu.roll(window, (LANES + q * cut - offset) & (LANES - 1), axis=1)
            gathered = window if q == 0 else jnp.where(lane // cut == q, window, gathered)
        for shift in range(per):
            moved = gathered if shift == 0 else pltpu.roll(gathered, shift * cut, axis=1)
            packed.append(jnp.where(keep, moved, 0.0).astype(jnp.bfloat16))
    lines = out_ref.shape[0]
    want = lax.broadcasted_iota(jnp.int32, (lines, regions * SUB), 0)
    have = lax.broadcasted_iota(jnp.int32, (lines, regions * SUB), 1)
    have_row, have_shift, have_group = have % SUB, have // SUB % per, have // (SUB * per)
    have_region = have_group * per + (have_row % per + per - have_shift) % per
    pick = jnp.where(have_region * (SUB // per) + have_row // per == want, 1.0, 0.0).astype(jnp.bfloat16)
    out = jnp.dot(pick, jnp.concatenate(packed, axis=0), preferred_element_type=jnp.float32)
    out_ref[...] = out.astype(jnp.bfloat16)


def make_contrast(projections, flats):
    shape = flats.shape
    edge = jax.ShapeDtypeStruct((HALO, shape[1]), halo_type)
    return pl.pallas_call(
        contrast_kernel,
        out_shape=(jax.ShapeDtypeStruct(shape, jnp.float32), edge, edge),
        in_specs=[HBM] * 2,
        out_specs=(VMEM,) * 3,
        scratch_shapes=[
            pltpu.VMEM(projections.shape, projections.dtype),
            pltpu.VMEM(flats.shape, flats.dtype),
            pltpu.SemaphoreType.DMA((2,)),
        ],
        compiler_params=PARAMS,
        name="contrast",
    )(projections, flats)


def make_own(own, turns, forward, gains):
    lines = turns.shape[1] * SUB
    return pl.pallas_call(
        own_kernel,
        out_shape=jax.ShapeDtypeStruct((lines, 2 * LANES), jnp.float32),
        in_specs=[VMEM] * 4,
        out_specs=VMEM,
        compiler_params=PARAMS,
        name="own_rows",
    )(own, turns, forward, gains)


def make_tile(own_spec, below, above, starts, turns, forward, inverse, gains, cut):
    regions = starts.shape[1]
    return pl.pallas_call(
        tile_kernel,
        out_shape=jax.ShapeDtypeStruct((regions * SUB * cut // LANES, LANES), jnp.bfloat16),
        in_specs=[VMEM] * 3 + [ANY] + [VMEM] * 4,
        out_specs=VMEM,
        scratch_shapes=[
            pltpu.VMEM((above.shape[1] // LANES + 1, SUB, LANES), jnp.float32),
            pltpu.SMEM(starts.shape, jnp.int32),
            pltpu.SemaphoreType.DMA,
        ],
        compiler_params=PARAMS,
        name="tile",
    )(own_spec, below, above, starts, turns, forward, inverse, gains)


def body(projections, flats, block_start, bp_weights):
    angles_dev, rows_dev, width = projections.shape
    assert angles_dev == 1 and rows_dev == SUB and width % (2 * LANES) == 0
    cut = bp_weights.shape[1]
    rows = lax.axis_size("row")
    up = [(i, i + 1) for i in range(rows - 1)]
    down = [(j, i) for i, j in up]
    turns, forward, inverse, gains, halo_gains = (jnp.asarray(t) for t in tables(width, rows_dev + 2 * HALO))
    in_hbm = partial(pltpu.with_memory_space_constraint, memory_space=pltpu.HBM)
    own, first, last = make_contrast(in_hbm(projections), in_hbm(flats))
    below = lax.ppermute(first, "row", down)
    above = lax.ppermute(last, "row", up)
    own_spec = make_own(own, turns, forward, gains)
    outgoing = make_tile(own_spec, below, above, block_start, turns, forward, inverse, halo_gains, cut)
    incoming = lax.all_to_all(outgoing, "ang", split_axis=0, concat_axis=0, tiled=True)
    blocks = incoming.reshape(bp_weights.shape[0], rows_dev, cut)
    return lax.dot_general(
        blocks, bp_weights, (((0, 2), (0, 1)), ((), ())), preferred_element_type=jnp.float32
    )


def solution(mesh):
    placed = (P(("scan", "ang"), "row", None), P(("scan", "row"), None), P(), P(None, None, "ang"))
    return jax.shard_map(
        body, mesh=mesh, in_specs=placed, out_specs=P(("scan", "row"), "ang"), check_vma=False
    )
```

```python
from functools import partial

import jax
import jax.numpy as jnp
import numpy as np
from jax import lax
from jax.experimental import pallas as pl
from jax.experimental.pallas import tpu as pltpu
from jax.sharding import PartitionSpec as P

HALO = 4
LANES = 128
SUB = 8

paganin_beta = 8.0
ramp_gain = 320.0
halo_type = jnp.float32
VMEM = pl.BlockSpec(memory_space=pltpu.VMEM)
ANY = pl.BlockSpec(memory_space=pl.ANY)
HBM = pl.BlockSpec(memory_space=pltpu.HBM)
PARAMS = pltpu.CompilerParams(vmem_limit_bytes=8 * 2**20)


def tables(width, tile_rows):
    blocks = width // LANES
    half = blocks // 2
    lane = np.arange(LANES)
    ks = np.arange(half + 1)
    turn = 2.0 * np.pi / width * (ks[:, None] * lane[None, :])
    turns = np.stack((np.cos(turn), np.sin(turn))).astype(np.float32)
    angle = 2.0 * np.pi / LANES * (lane[:, None] * lane[None, :] % LANES)
    cos, sin = np.cos(angle), np.sin(angle)
    forward = np.block([[cos, -sin], [sin, cos]])

    def split(matrix):
        high = matrix.astype(jnp.bfloat16)
        low = (matrix - high.astype(np.float64)).astype(jnp.bfloat16)
        return np.stack((high, low))

    freq = (ks[:, None] + blocks * lane[None, :]).astype(np.float64)
    row = np.arange(tile_rows, dtype=np.float64)
    lam = 4.0 * np.sin(np.pi * row / tile_rows)[:, None, None] ** 2 + 4.0 * np.sin(np.pi * freq / width) ** 2
    filt = 1.0 / (1.0 + paganin_beta * lam)
    dist = np.arange(tile_rows // 2 + 1)
    gains = np.einsum("du,ukm->dkm", np.cos(2.0 * np.pi / tile_rows * dist[:, None] * row), filt) / tile_rows
    folded = np.minimum(freq, width - freq)
    ramp = ramp_gain * (folded / width) * (0.5 + 0.5 * np.cos(2.0 * np.pi * folded / width))
    twice = np.where((ks == 0) | (ks == half), 1.0, 2.0)
    gains = gains * (ramp * twice[:, None] / width)
    return turns, split(forward), split(forward.T), gains.astype(np.float32)


def plus(terms):
    return sum(terms[1:], terms[0])


def scaled(terms, weights):
    out = None
    for term, weight in zip(terms, weights):
        weight = float(weight)
        if abs(weight) < 1e-12:
            continue
        piece = term if weight == 1.0 else -term if weight == -1.0 else term * weight
        out = piece if out is None else out + piece
    return out


def cosine_sums(terms, blocks):
    half = blocks // 2
    out = [None] * (half + 1)
    for k in range(half // 2 + 1):
        wave = [np.round(np.cos(2.0 * np.pi * a * k / blocks), 15) for a in range(half + 1)]
        even = scaled(terms[0::2], wave[0::2])
        odd = scaled(terms[1::2], wave[1::2])
        out[k] = even if odd is None else even + odd
        if half - k != k:
            out[half - k] = even if odd is None else even - odd
    return out


def sine_sums(terms, blocks):
    half = blocks // 2
    out = [None] * (half + 1)
    for k in range(1, half // 2 + 1):
        wave = [np.round(np.sin(2.0 * np.pi * a * k / blocks), 15) for a in range(half)]
        even = scaled(terms[2:half:2], wave[2::2])
        odd = scaled(terms[1:half:2], wave[1::2])
        if half - k != k:
            out[k] = plus([x for x in (even, odd) if x is not None])
            out[half - k] = odd - even if even is not None else odd
        else:
            out[k] = plus([x for x in (even, odd) if x is not None])
    return out


def accurate_dot(values, matrix_ref):
    high = values.astype(jnp.bfloat16)
    low = (values - high.astype(jnp.float32)).astype(jnp.bfloat16)
    dot = partial(jnp.dot, preferred_element_type=jnp.float32)
    lines = values.shape[0]
    both = dot(jnp.concatenate((high, low), axis=0), matrix_ref[0])
    return both[:lines] + (both[lines:] + dot(high, matrix_ref[1]))


def spectrum(chunks, turns_ref, forward_ref):
    blocks = len(chunks)
    half = blocks // 2
    folds = [chunks[0]] + [chunks[a] + chunks[blocks - a] for a in range(1, half)] + [chunks[half]]
    skews = [None] + [chunks[a] - chunks[blocks - a] for a in range(1, half)] + [None]
    reals = cosine_sums(folds, blocks)
    imags = sine_sums(skews, blocks)
    parts = []
    for k in range(half + 1):
        cos, sin = turns_ref[0, k : k + 1, :], turns_ref[1, k : k + 1, :]
        if k == 0:
            re, im = reals[0], jnp.zeros_like(reals[0])
        elif imags[k] is None:
            re, im = reals[k] * cos, -(reals[k] * sin)
        else:
            re, im = reals[k] * cos - imags[k] * sin, -(imags[k] * cos) - reals[k] * sin
        parts.append(jnp.concatenate((re, im), axis=1))
    return accurate_dot(jnp.concatenate(parts, axis=0), forward_ref)


def columns(spec, turns_ref, inverse_ref, blocks):
    half = blocks // 2
    back = accurate_dot(spec, inverse_ref)
    reals, imags = [], []
    for k in range(half + 1):
        rows = slice(k * SUB, (k + 1) * SUB)
        re, im = back[rows, :LANES], back[rows, LANES:]
        cos, sin = turns_ref[0, k : k + 1, :], turns_ref[1, k : k + 1, :]
        if k == 0:
            reals.append(re)
            imags.append(None)
        else:
            reals.append(re * cos - im * sin)
            imags.append(im * cos + re * sin if k < half else None)
    even = cosine_sums(reals, blocks)
    odd = sine_sums(imags, blocks)
    out = [None] * blocks
    out[0], out[half] = even[0], even[half]
    for a in range(1, half):
        out[a] = even[a] - odd[a]
        out[blocks - a] = even[a] + odd[a]
    return out


def contrast_kernel(proj_hbm, flat_hbm, own_ref, first_ref, last_ref, proj, flat, sems):
    copies = [
        pltpu.make_async_copy(proj_hbm, proj, sems.at[0]),
        pltpu.make_async_copy(flat_hbm, flat, sems.at[1]),
    ]
    for copy in copies:
        copy.start()
    for copy in copies:
        copy.wait()
    own = 1.0 - proj[0].astype(jnp.float32) / flat[...]
    own_ref[...] = own
    first_ref[...] = own[:HALO].astype(first_ref.dtype)
    last_ref[...] = own[SUB - HALO :].astype(last_ref.dtype)


def lanes_of(ref, block):
    return ref[:, block * LANES : (block + 1) * LANES]


def halo_gains(gains_ref, k, row):
    gains = [jnp.broadcast_to(gains_ref[d, k : k + 1, :], (SUB, LANES)) for d in range(2 * HALO + 1)]
    for s in range(SUB):
        far = gains[2 * HALO - abs(s - HALO)]
        near = gains[abs(s - HALO)]
        if s < HALO:
            yield s, jnp.where(row >= s + HALO, near, far)
        else:
            yield s, jnp.where(row < s - HALO, near, far)


def own_kernel(
    own_ref, turns_ref, gains_ref, forward_hbm, inverse_hbm, out_ref, forward_ref, inverse_ref, halo_ref, sems
):
    forward_copy = pltpu.make_async_copy(forward_hbm, forward_ref, sems.at[0])
    inverse_copy = pltpu.make_async_copy(inverse_hbm, inverse_ref, sems.at[1])
    forward_copy.start()
    inverse_copy.start()
    row = lax.broadcasted_iota(jnp.int32, (SUB, LANES), 0)
    for k in range(gains_ref.shape[1]):
        for s, gain in halo_gains(gains_ref, k, row):
            halo_ref[s, k] = gain
    forward_copy.wait()
    blocks = own_ref.shape[1] // LANES
    spec = spectrum([lanes_of(own_ref, a) for a in range(blocks)], turns_ref, forward_ref)
    for k in range(blocks // 2 + 1):
        rows = slice(k * SUB, (k + 1) * SUB)
        for side in (slice(0, LANES), slice(LANES, 2 * LANES)):
            here = spec[rows, side]
            moved = [here] + [pltpu.roll(here, s, axis=0) for s in range(1, SUB)]
            total = here * gains_ref[0, k : k + 1, :]
            for d in range(1, SUB):
                pair = jnp.where(row >= d, moved[d], 0.0) + jnp.where(row < SUB - d, moved[SUB - d], 0.0)
                total += pair * gains_ref[d, k : k + 1, :]
            out_ref[rows, side] = total
    inverse_copy.wait()


def tile_kernel(
    own_ref, below_ref, above_ref, starts_hbm, turns_ref, forward_ref, inverse_ref, gains_ref, out_ref,
    sheet, starts, sem
):
    copy = pltpu.make_async_copy(starts_hbm, starts, sem)
    copy.start()
    blocks = above_ref.shape[1] // LANES
    halo = [
        jnp.concatenate((lanes_of(above_ref, a), lanes_of(below_ref, a)), axis=0).astype(jnp.float32)
        for a in range(blocks)
    ]
    spec = spectrum(halo, turns_ref, forward_ref)
    row = lax.broadcasted_iota(jnp.int32, (SUB, LANES), 0)
    lane = lax.broadcasted_iota(jnp.int32, (SUB, LANES), 1)
    parts = []
    for k in range(blocks // 2 + 1):
        rows = slice(k * SUB, (k + 1) * SUB)
        both = []
        for side in (slice(0, LANES), slice(LANES, 2 * LANES)):
            here = spec[rows, side]
            total = own_ref[rows, side] + here * gains_ref[0, k]
            for s in range(1, SUB):
                total += pltpu.roll(here, s, axis=0) * gains_ref[s, k]
            both.append(total)
        parts.append(jnp.concatenate(both, axis=1))
    filtered = columns(jnp.concatenate(parts, axis=0), turns_ref, inverse_ref, blocks)
    for a in range(blocks):
        sheet[a] = filtered[a]
    copy.wait()
    mine = lax.axis_index("ang")
    regions = starts.shape[1]
    cut = out_ref.shape[0] * LANES // (regions * SUB)
    per = LANES // cut
    keep = lane // cut == row % per
    packed = []
    for group in range(regions // per):
        gathered = None
        for q in range(per):
            start = starts[mine, group * per + q]
            block = lax.shift_right_logical(start, 7)
            offset = start & (LANES - 1)
            window = jnp.where(lane >= offset, sheet[block], sheet[block + 1])
            window = pltpu.roll(window, (LANES + q * cut - offset) & (LANES - 1), axis=1)
            gathered = window if q == 0 else jnp.where(lane // cut == q, window, gathered)
        for shift in range(per):
            moved = gathered if shift == 0 else pltpu.roll(gathered, shift * cut, axis=1)
            packed.append(jnp.where(keep, moved, 0.0).astype(jnp.bfloat16))
    lines = out_ref.shape[0]
    want = lax.broadcasted_iota(jnp.int32, (lines, regions * SUB), 0)
    have = lax.broadcasted_iota(jnp.int32, (lines, regions * SUB), 1)
    have_row, have_shift, have_group = have % SUB, have // SUB % per, have // (SUB * per)
    have_region = have_group * per + (have_row % per + per - have_shift) % per
    pick = jnp.where(have_region * (SUB // per) + have_row // per == want, 1.0, 0.0).astype(jnp.bfloat16)
    out = jnp.dot(pick, jnp.concatenate(packed, axis=0), preferred_element_type=jnp.float32)
    out_ref[...] = out.astype(jnp.bfloat16)


def in_hbm(array):
    return pltpu.with_memory_space_constraint(array, pltpu.HBM)


def make_contrast(projections, flats):
    shape = flats.shape
    edge = jax.ShapeDtypeStruct((HALO, shape[1]), halo_type)
    return pl.pallas_call(
        contrast_kernel,
        out_shape=(jax.ShapeDtypeStruct(shape, jnp.float32), edge, edge),
        in_specs=[HBM] * 2,
        out_specs=(VMEM,) * 3,
        scratch_shapes=[
            pltpu.VMEM(projections.shape, projections.dtype),
            pltpu.VMEM(flats.shape, flats.dtype),
            pltpu.SemaphoreType.DMA((2,)),
        ],
        compiler_params=PARAMS,
        name="contrast",
    )(in_hbm(projections), in_hbm(flats))


def make_own(own, turns, forward, inverse, gains):
    groups = turns.shape[1]
    return pl.pallas_call(
        own_kernel,
        out_shape=(
            jax.ShapeDtypeStruct((groups * SUB, 2 * LANES), jnp.float32),
            jax.ShapeDtypeStruct(forward.shape, forward.dtype),
            jax.ShapeDtypeStruct(inverse.shape, inverse.dtype),
            jax.ShapeDtypeStruct((SUB, groups, SUB, LANES), jnp.float32),
        ),
        in_specs=[VMEM] * 3 + [HBM] * 2,
        out_specs=(VMEM,) * 4,
        scratch_shapes=[pltpu.SemaphoreType.DMA((2,))],
        compiler_params=PARAMS,
        name="own_rows",
    )(own, turns, gains, in_hbm(forward), in_hbm(inverse))


def make_tile(own_spec, below, above, starts, turns, forward, inverse, gains, cut):
    regions = starts.shape[1]
    return pl.pallas_call(
        tile_kernel,
        out_shape=jax.ShapeDtypeStruct((regions * SUB * cut // LANES, LANES), jnp.bfloat16),
        in_specs=[VMEM] * 3 + [ANY] + [VMEM] * 4,
        out_specs=VMEM,
        scratch_shapes=[
            pltpu.VMEM((above.shape[1] // LANES + 1, SUB, LANES), jnp.float32),
            pltpu.SMEM(starts.shape, jnp.int32),
            pltpu.SemaphoreType.DMA,
        ],
        compiler_params=PARAMS,
        name="tile",
    )(own_spec, below, above, starts, turns, forward, inverse, gains)


def body(projections, flats, block_start, bp_weights):
    angles_dev, rows_dev, width = projections.shape
    assert angles_dev == 1 and rows_dev == SUB and width % (2 * LANES) == 0
    cut = bp_weights.shape[1]
    rows = lax.axis_size("row")
    up = [(i, i + 1) for i in range(rows - 1)]
    down = [(j, i) for i, j in up]
    turns, forward, inverse, gains = (jnp.asarray(t) for t in tables(width, rows_dev + 2 * HALO))
    own, first, last = make_contrast(projections, flats)
    below = lax.ppermute(first, "row", down)
    above = lax.ppermute(last, "row", up)
    own_spec, forward, inverse, gains = make_own(own, turns, forward, inverse, gains)
    outgoing = make_tile(own_spec, below, above, block_start, turns, forward, inverse, gains, cut)
    incoming = lax.all_to_all(outgoing, "ang", split_axis=0, concat_axis=0, tiled=True)
    blocks = incoming.reshape(bp_weights.shape[0], rows_dev, cut)
    return lax.dot_general(
        blocks, bp_weights, (((0, 2), (0, 1)), ((), ())), preferred_element_type=jnp.float32
    )


def solution(mesh):
    placed = (P(("scan", "ang"), "row", None), P(("scan", "row"), None), P(), P(None, None, "ang"))
    return jax.shard_map(
        body, mesh=mesh, in_specs=placed, out_specs=P(("scan", "row"), "ang"), check_vma=False
    )
```

```python
from functools import partial

import jax
import jax.numpy as jnp
import numpy as np
from jax import lax
from jax.experimental import pallas as pl
from jax.experimental.pallas import tpu as pltpu
from jax.sharding import PartitionSpec as P

HALO = 4
LANES = 128
SUB = 8

paganin_beta = 8.0
ramp_gain = 320.0
halo_type = jnp.float32
VMEM = pl.BlockSpec(memory_space=pltpu.VMEM)
SMEM = pl.BlockSpec(memory_space=pltpu.SMEM)
HBM = pl.BlockSpec(memory_space=pltpu.HBM)
PARAMS = pltpu.CompilerParams(vmem_limit_bytes=8 * 2**20)


def tables(width, tile_rows):
    blocks = width // LANES
    half = blocks // 2
    lane = np.arange(LANES)
    ks = np.arange(half + 1)
    turn = 2.0 * np.pi / width * (ks[:, None] * lane[None, :])
    turns = np.stack((np.cos(turn), np.sin(turn))).astype(np.float32)
    angle = 2.0 * np.pi / LANES * (lane[:, None] * lane[None, :] % LANES)
    cos, sin = np.cos(angle), np.sin(angle)
    forward = np.block([[cos, -sin], [sin, cos]])

    def split(matrix):
        high = matrix.astype(jnp.bfloat16)
        low = (matrix - high.astype(np.float64)).astype(jnp.bfloat16)
        return np.stack((high, low))

    freq = (ks[:, None] + blocks * lane[None, :]).astype(np.float64)
    row = np.arange(tile_rows, dtype=np.float64)
    lam = 4.0 * np.sin(np.pi * row / tile_rows)[:, None, None] ** 2 + 4.0 * np.sin(np.pi * freq / width) ** 2
    filt = 1.0 / (1.0 + paganin_beta * lam)
    dist = np.arange(tile_rows // 2 + 1)
    gains = np.einsum("du,ukm->dkm", np.cos(2.0 * np.pi / tile_rows * dist[:, None] * row), filt) / tile_rows
    folded = np.minimum(freq, width - freq)
    ramp = ramp_gain * (folded / width) * (0.5 + 0.5 * np.cos(2.0 * np.pi * folded / width))
    twice = np.where((ks == 0) | (ks == half), 1.0, 2.0)
    gains = gains * (ramp * twice[:, None] / width)
    return turns, split(forward), split(forward.T), gains.astype(np.float32)


def plus(terms):
    return sum(terms[1:], terms[0])


def scaled(terms, weights):
    out = None
    for term, weight in zip(terms, weights):
        weight = float(weight)
        if abs(weight) < 1e-12:
            continue
        piece = term if weight == 1.0 else -term if weight == -1.0 else term * weight
        out = piece if out is None else out + piece
    return out


def cosine_sums(terms, blocks):
    half = blocks // 2
    out = [None] * (half + 1)
    for k in range(half // 2 + 1):
        wave = [np.round(np.cos(2.0 * np.pi * a * k / blocks), 15) for a in range(half + 1)]
        even = scaled(terms[0::2], wave[0::2])
        odd = scaled(terms[1::2], wave[1::2])
        out[k] = even if odd is None else even + odd
        if half - k != k:
            out[half - k] = even if odd is None else even - odd
    return out


def sine_sums(terms, blocks):
    half = blocks // 2
    out = [None] * (half + 1)
    for k in range(1, half // 2 + 1):
        wave = [np.round(np.sin(2.0 * np.pi * a * k / blocks), 15) for a in range(half)]
        even = scaled(terms[2:half:2], wave[2::2])
        odd = scaled(terms[1:half:2], wave[1::2])
        if half - k != k:
            out[k] = plus([x for x in (even, odd) if x is not None])
            out[half - k] = odd - even if even is not None else odd
        else:
            out[k] = plus([x for x in (even, odd) if x is not None])
    return out


def accurate_dot(values, matrix_ref):
    high = values.astype(jnp.bfloat16)
    low = (values - high.astype(jnp.float32)).astype(jnp.bfloat16)
    dot = partial(jnp.dot, preferred_element_type=jnp.float32)
    lines = values.shape[0]
    both = dot(jnp.concatenate((high, low), axis=0), matrix_ref[0])
    return both[:lines] + (both[lines:] + dot(high, matrix_ref[1]))


def spectrum(chunks, turns_ref, forward_ref):
    blocks = len(chunks)
    half = blocks // 2
    folds = [chunks[0]] + [chunks[a] + chunks[blocks - a] for a in range(1, half)] + [chunks[half]]
    skews = [None] + [chunks[a] - chunks[blocks - a] for a in range(1, half)] + [None]
    reals = cosine_sums(folds, blocks)
    imags = sine_sums(skews, blocks)
    parts = []
    for k in range(half + 1):
        cos, sin = turns_ref[0, k : k + 1, :], turns_ref[1, k : k + 1, :]
        if k == 0:
            re, im = reals[0], jnp.zeros_like(reals[0])
        elif imags[k] is None:
            re, im = reals[k] * cos, -(reals[k] * sin)
        else:
            re, im = reals[k] * cos - imags[k] * sin, -(imags[k] * cos) - reals[k] * sin
        parts.append(jnp.concatenate((re, im), axis=1))
    return accurate_dot(jnp.concatenate(parts, axis=0), forward_ref)


def columns(spec, turns_ref, inverse_ref, blocks):
    half = blocks // 2
    back = accurate_dot(spec, inverse_ref)
    reals, imags = [], []
    for k in range(half + 1):
        rows = slice(k * SUB, (k + 1) * SUB)
        re, im = back[rows, :LANES], back[rows, LANES:]
        cos, sin = turns_ref[0, k : k + 1, :], turns_ref[1, k : k + 1, :]
        if k == 0:
            reals.append(re)
            imags.append(None)
        else:
            reals.append(re * cos - im * sin)
            imags.append(im * cos + re * sin if k < half else None)
    even = cosine_sums(reals, blocks)
    odd = sine_sums(imags, blocks)
    out = [None] * blocks
    out[0], out[half] = even[0], even[half]
    for a in range(1, half):
        out[a] = even[a] - odd[a]
        out[blocks - a] = even[a] + odd[a]
    return out


def contrast_kernel(proj_hbm, flat_hbm, own_ref, first_ref, last_ref, proj, flat, sems):
    copies = [
        pltpu.make_async_copy(proj_hbm, proj, sems.at[0]),
        pltpu.make_async_copy(flat_hbm, flat, sems.at[1]),
    ]
    for copy in copies:
        copy.start()
    for copy in copies:
        copy.wait()
    own = 1.0 - proj[0].astype(jnp.float32) / flat[...]
    own_ref[...] = own
    first_ref[...] = own[:HALO].astype(first_ref.dtype)
    last_ref[...] = own[SUB - HALO :].astype(last_ref.dtype)


def lanes_of(ref, block):
    return ref[:, block * LANES : (block + 1) * LANES]


def halo_gains(gains_ref, k, row):
    gains = [jnp.broadcast_to(gains_ref[d, k : k + 1, :], (SUB, LANES)) for d in range(2 * HALO + 1)]
    for s in range(SUB):
        far = gains[2 * HALO - abs(s - HALO)]
        near = gains[abs(s - HALO)]
        if s < HALO:
            yield s, jnp.where(row >= s + HALO, near, far)
        else:
            yield s, jnp.where(row < s - HALO, near, far)


def own_kernel(
    own_ref, turns_ref, gains_ref, forward_hbm, inverse_hbm, starts_hbm,
    out_ref, forward_ref, inverse_ref, halo_ref, starts_ref, sems
):
    forward_copy = pltpu.make_async_copy(forward_hbm, forward_ref, sems.at[0])
    inverse_copy = pltpu.make_async_copy(inverse_hbm, inverse_ref, sems.at[1])
    starts_copy = pltpu.make_async_copy(starts_hbm.at[pl.ds(lax.axis_index("ang"), 1)], starts_ref, sems.at[2])
    forward_copy.start()
    inverse_copy.start()
    starts_copy.start()
    row = lax.broadcasted_iota(jnp.int32, (SUB, LANES), 0)
    for k in range(gains_ref.shape[1]):
        for s, gain in halo_gains(gains_ref, k, row):
            halo_ref[s, k] = gain
    forward_copy.wait()
    blocks = own_ref.shape[1] // LANES
    spec = spectrum([lanes_of(own_ref, a) for a in range(blocks)], turns_ref, forward_ref)
    for k in range(blocks // 2 + 1):
        rows = slice(k * SUB, (k + 1) * SUB)
        for side in (slice(0, LANES), slice(LANES, 2 * LANES)):
            here = spec[rows, side]
            moved = [here] + [pltpu.roll(here, s, axis=0) for s in range(1, SUB)]
            total = here * gains_ref[0, k : k + 1, :]
            for d in range(1, SUB):
                pair = jnp.where(row >= d, moved[d], 0.0) + jnp.where(row < SUB - d, moved[SUB - d], 0.0)
                total += pair * gains_ref[d, k : k + 1, :]
            out_ref[rows, side] = total
    inverse_copy.wait()
    starts_copy.wait()


def tile_kernel(
    own_ref, below_ref, above_ref, starts, turns_ref, forward_ref, inverse_ref, gains_ref, out_ref,
    sheet
):
    blocks = above_ref.shape[1] // LANES
    halo = [
        jnp.concatenate((lanes_of(above_ref, a), lanes_of(below_ref, a)), axis=0).astype(jnp.float32)
        for a in range(blocks)
    ]
    spec = spectrum(halo, turns_ref, forward_ref)
    row = lax.broadcasted_iota(jnp.int32, (SUB, LANES), 0)
    lane = lax.broadcasted_iota(jnp.int32, (SUB, LANES), 1)
    parts = []
    for k in range(blocks // 2 + 1):
        rows = slice(k * SUB, (k + 1) * SUB)
        both = []
        for side in (slice(0, LANES), slice(LANES, 2 * LANES)):
            here = spec[rows, side]
            total = own_ref[rows, side] + here * gains_ref[0, k]
            for s in range(1, SUB):
                total += pltpu.roll(here, s, axis=0) * gains_ref[s, k]
            both.append(total)
        parts.append(jnp.concatenate(both, axis=1))
    filtered = columns(jnp.concatenate(parts, axis=0), turns_ref, inverse_ref, blocks)
    for a in range(blocks):
        sheet[a] = filtered[a]
    regions = starts.shape[1]
    cut = out_ref.shape[0] * LANES // (regions * SUB)
    per = LANES // cut
    keep = lane // cut == row % per
    packed = []
    for group in range(regions // per):
        gathered = None
        for q in range(per):
            start = starts[0, group * per + q]
            block = lax.shift_right_logical(start, 7)
            offset = start & (LANES - 1)
            window = jnp.where(lane >= offset, sheet[block], sheet[block + 1])
            window = pltpu.roll(window, (LANES + q * cut - offset) & (LANES - 1), axis=1)
            gathered = window if q == 0 else jnp.where(lane // cut == q, window, gathered)
        for shift in range(per):
            moved = gathered if shift == 0 else pltpu.roll(gathered, shift * cut, axis=1)
            packed.append(jnp.where(keep, moved, 0.0).astype(jnp.bfloat16))
    lines = out_ref.shape[0]
    want = lax.broadcasted_iota(jnp.int32, (lines, regions * SUB), 0)
    have = lax.broadcasted_iota(jnp.int32, (lines, regions * SUB), 1)
    have_row, have_shift, have_group = have % SUB, have // SUB % per, have // (SUB * per)
    have_region = have_group * per + (have_row % per + per - have_shift) % per
    pick = jnp.where(have_region * (SUB // per) + have_row // per == want, 1.0, 0.0).astype(jnp.bfloat16)
    out = jnp.dot(pick, jnp.concatenate(packed, axis=0), preferred_element_type=jnp.float32)
    out_ref[...] = out.astype(jnp.bfloat16)


def in_hbm(array):
    return pltpu.with_memory_space_constraint(array, pltpu.HBM)


def make_contrast(projections, flats):
    shape = flats.shape
    edge = jax.ShapeDtypeStruct((HALO, shape[1]), halo_type)
    return pl.pallas_call(
        contrast_kernel,
        out_shape=(jax.ShapeDtypeStruct(shape, jnp.float32), edge, edge),
        in_specs=[HBM] * 2,
        out_specs=(VMEM,) * 3,
        scratch_shapes=[
            pltpu.VMEM(projections.shape, projections.dtype),
            pltpu.VMEM(flats.shape, flats.dtype),
            pltpu.SemaphoreType.DMA((2,)),
        ],
        compiler_params=PARAMS,
        name="contrast",
    )(in_hbm(projections), in_hbm(flats))


def make_own(own, turns, forward, inverse, gains, starts):
    groups = turns.shape[1]
    return pl.pallas_call(
        own_kernel,
        out_shape=(
            jax.ShapeDtypeStruct((groups * SUB, 2 * LANES), jnp.float32),
            jax.ShapeDtypeStruct(forward.shape, forward.dtype),
            jax.ShapeDtypeStruct(inverse.shape, inverse.dtype),
            jax.ShapeDtypeStruct((SUB, groups, SUB, LANES), jnp.float32),
            pltpu.SMEM((1, starts.shape[1]), jnp.int32),
        ),
        in_specs=[VMEM] * 3 + [HBM] * 3,
        out_specs=(VMEM,) * 4 + (SMEM,),
        scratch_shapes=[pltpu.SemaphoreType.DMA((3,))],
        compiler_params=PARAMS,
        name="own_rows",
    )(own, turns, gains, in_hbm(forward), in_hbm(inverse), in_hbm(starts))


def make_tile(own_spec, below, above, starts, turns, forward, inverse, gains, cut):
    regions = starts.shape[1]
    return pl.pallas_call(
        tile_kernel,
        out_shape=jax.ShapeDtypeStruct((regions * SUB * cut // LANES, LANES), jnp.bfloat16),
        in_specs=[VMEM] * 3 + [SMEM] + [VMEM] * 4,
        out_specs=VMEM,
        scratch_shapes=[
            pltpu.VMEM((above.shape[1] // LANES + 1, SUB, LANES), jnp.float32),
        ],
        compiler_params=PARAMS,
        name="tile",
    )(own_spec, below, above, starts, turns, forward, inverse, gains)


def body(projections, flats, block_start, bp_weights):
    angles_dev, rows_dev, width = projections.shape
    assert angles_dev == 1 and rows_dev == SUB and width % (2 * LANES) == 0
    cut = bp_weights.shape[1]
    rows = lax.axis_size("row")
    up = [(i, i + 1) for i in range(rows - 1)]
    down = [(j, i) for i, j in up]
    turns, forward, inverse, gains = (jnp.asarray(t) for t in tables(width, rows_dev + 2 * HALO))
    own, first, last = make_contrast(projections, flats)
    below = lax.ppermute(first, "row", down)
    above = lax.ppermute(last, "row", up)
    own_spec, forward, inverse, gains, starts = make_own(own, turns, forward, inverse, gains, block_start)
    outgoing = make_tile(own_spec, below, above, starts, turns, forward, inverse, gains, cut)
    incoming = lax.all_to_all(outgoing, "ang", split_axis=0, concat_axis=0, tiled=True)
    blocks = incoming.reshape(bp_weights.shape[0], rows_dev, cut)
    return lax.dot_general(
        blocks, bp_weights, (((0, 2), (0, 1)), ((), ())), preferred_element_type=jnp.float32
    )


def solution(mesh):
    placed = (P(("scan", "ang"), "row", None), P(("scan", "row"), None), P(), P(None, None, "ang"))
    return jax.shard_map(
        body, mesh=mesh, in_specs=placed, out_specs=P(("scan", "row"), "ang"), check_vma=False
    )
```

```python
from functools import partial

import jax
import jax.numpy as jnp
import numpy as np
from jax import lax
from jax.experimental import pallas as pl
from jax.experimental.pallas import tpu as pltpu
from jax.sharding import PartitionSpec as P

HALO = 4
LANES = 128
SUB = 8

paganin_beta = 8.0
ramp_gain = 320.0
halo_type = jnp.float32
VMEM = pl.BlockSpec(memory_space=pltpu.VMEM)
SMEM = pl.BlockSpec(memory_space=pltpu.SMEM)
HBM = pl.BlockSpec(memory_space=pltpu.HBM)
PARAMS = pltpu.CompilerParams(vmem_limit_bytes=8 * 2**20)


def tables(width, tile_rows):
    blocks = width // LANES
    half = blocks // 2
    lane = np.arange(LANES)
    ks = np.arange(half + 1)
    turn = 2.0 * np.pi / width * (ks[:, None] * lane[None, :])
    turns = np.stack((np.cos(turn), np.sin(turn))).astype(np.float32)
    angle = 2.0 * np.pi / LANES * (lane[:, None] * lane[None, :] % LANES)
    cos, sin = np.cos(angle), np.sin(angle)
    forward = np.block([[cos, -sin], [sin, cos]])

    def split(matrix):
        high = matrix.astype(jnp.bfloat16)
        low = (matrix - high.astype(np.float64)).astype(jnp.bfloat16)
        return np.stack((high, low))

    freq = (ks[:, None] + blocks * lane[None, :]).astype(np.float64)
    row = np.arange(tile_rows, dtype=np.float64)
    lam = 4.0 * np.sin(np.pi * row / tile_rows)[:, None, None] ** 2 + 4.0 * np.sin(np.pi * freq / width) ** 2
    filt = 1.0 / (1.0 + paganin_beta * lam)
    dist = np.arange(tile_rows // 2 + 1)
    gains = np.einsum("du,ukm->dkm", np.cos(2.0 * np.pi / tile_rows * dist[:, None] * row), filt) / tile_rows
    folded = np.minimum(freq, width - freq)
    ramp = ramp_gain * (folded / width) * (0.5 + 0.5 * np.cos(2.0 * np.pi * folded / width))
    twice = np.where((ks == 0) | (ks == half), 1.0, 2.0)
    gains = gains * (ramp * twice[:, None] / width)
    return turns, split(forward), split(forward.T), gains.astype(np.float32)


def plus(terms):
    return sum(terms[1:], terms[0])


def scaled(terms, weights):
    out = None
    for term, weight in zip(terms, weights):
        weight = float(weight)
        if abs(weight) < 1e-12:
            continue
        piece = term if weight == 1.0 else -term if weight == -1.0 else term * weight
        out = piece if out is None else out + piece
    return out


def cosine_sums(terms, blocks):
    half = blocks // 2
    out = [None] * (half + 1)
    for k in range(half // 2 + 1):
        wave = [np.round(np.cos(2.0 * np.pi * a * k / blocks), 15) for a in range(half + 1)]
        even = scaled(terms[0::2], wave[0::2])
        odd = scaled(terms[1::2], wave[1::2])
        out[k] = even if odd is None else even + odd
        if half - k != k:
            out[half - k] = even if odd is None else even - odd
    return out


def sine_sums(terms, blocks):
    half = blocks // 2
    out = [None] * (half + 1)
    for k in range(1, half // 2 + 1):
        wave = [np.round(np.sin(2.0 * np.pi * a * k / blocks), 15) for a in range(half)]
        even = scaled(terms[2:half:2], wave[2::2])
        odd = scaled(terms[1:half:2], wave[1::2])
        if half - k != k:
            out[k] = plus([x for x in (even, odd) if x is not None])
            out[half - k] = odd - even if even is not None else odd
        else:
            out[k] = plus([x for x in (even, odd) if x is not None])
    return out


def accurate_dot(values, matrix_ref):
    high = values.astype(jnp.bfloat16)
    low = (values - high.astype(jnp.float32)).astype(jnp.bfloat16)
    dot = partial(jnp.dot, preferred_element_type=jnp.float32)
    lines = values.shape[0]
    both = dot(jnp.concatenate((high, low), axis=0), matrix_ref[0])
    return both[:lines] + (both[lines:] + dot(high, matrix_ref[1]))


def spectrum(chunks, turns_ref, forward_ref):
    blocks = len(chunks)
    half = blocks // 2
    folds = [chunks[0]] + [chunks[a] + chunks[blocks - a] for a in range(1, half)] + [chunks[half]]
    skews = [None] + [chunks[a] - chunks[blocks - a] for a in range(1, half)] + [None]
    reals = cosine_sums(folds, blocks)
    imags = sine_sums(skews, blocks)
    parts = []
    for k in range(half + 1):
        cos, sin = turns_ref[0, k : k + 1, :], turns_ref[1, k : k + 1, :]
        if k == 0:
            re, im = reals[0], jnp.zeros_like(reals[0])
        elif imags[k] is None:
            re, im = reals[k] * cos, -(reals[k] * sin)
        else:
            re, im = reals[k] * cos - imags[k] * sin, -(imags[k] * cos) - reals[k] * sin
        parts.append(jnp.concatenate((re, im), axis=1))
    return accurate_dot(jnp.concatenate(parts, axis=0), forward_ref)


def columns(spec, turns_ref, inverse_ref, blocks):
    half = blocks // 2
    back = accurate_dot(spec, inverse_ref)
    reals, imags = [], []
    for k in range(half + 1):
        rows = slice(k * SUB, (k + 1) * SUB)
        re, im = back[rows, :LANES], back[rows, LANES:]
        cos, sin = turns_ref[0, k : k + 1, :], turns_ref[1, k : k + 1, :]
        if k == 0:
            reals.append(re)
            imags.append(None)
        else:
            reals.append(re * cos - im * sin)
            imags.append(im * cos + re * sin if k < half else None)
    even = cosine_sums(reals, blocks)
    odd = sine_sums(imags, blocks)
    out = [None] * blocks
    out[0], out[half] = even[0], even[half]
    for a in range(1, half):
        out[a] = even[a] - odd[a]
        out[blocks - a] = even[a] + odd[a]
    return out


def contrast_kernel(proj_hbm, flat_hbm, own_ref, first_ref, last_ref, proj, flat, sems):
    copies = [
        pltpu.make_async_copy(proj_hbm, proj, sems.at[0]),
        pltpu.make_async_copy(flat_hbm, flat, sems.at[1]),
    ]
    for copy in copies:
        copy.start()
    for copy in copies:
        copy.wait()
    own = 1.0 - proj[0].astype(jnp.float32) / flat[...]
    own_ref[...] = own
    first_ref[...] = own[:HALO].astype(first_ref.dtype)
    last_ref[...] = own[SUB - HALO :].astype(last_ref.dtype)


def lanes_of(ref, block):
    return ref[:, block * LANES : (block + 1) * LANES]


def halo_gains(gains_ref, k, row):
    gains = [jnp.broadcast_to(gains_ref[d, k : k + 1, :], (SUB, LANES)) for d in range(2 * HALO + 1)]
    for s in range(SUB):
        far = gains[2 * HALO - abs(s - HALO)]
        near = gains[abs(s - HALO)]
        if s < HALO:
            yield s, jnp.where(row >= s + HALO, near, far)
        else:
            yield s, jnp.where(row < s - HALO, near, far)


def own_kernel(
    own_ref, turns_ref, gains_ref, forward_hbm, inverse_hbm, starts_hbm,
    out_ref, forward_ref, inverse_ref, halo_ref, starts_ref, sems
):
    forward_copy = pltpu.make_async_copy(forward_hbm, forward_ref, sems.at[0])
    inverse_copy = pltpu.make_async_copy(inverse_hbm, inverse_ref, sems.at[1])
    starts_copy = pltpu.make_async_copy(starts_hbm.at[pl.ds(lax.axis_index("ang"), 1)], starts_ref, sems.at[2])
    forward_copy.start()
    inverse_copy.start()
    starts_copy.start()
    row = lax.broadcasted_iota(jnp.int32, (SUB, LANES), 0)
    for k in range(gains_ref.shape[1]):
        for s, gain in halo_gains(gains_ref, k, row):
            halo_ref[s, k] = gain
    forward_copy.wait()
    blocks = own_ref.shape[1] // LANES
    spec = spectrum([lanes_of(own_ref, a) for a in range(blocks)], turns_ref, forward_ref)
    for k in range(blocks // 2 + 1):
        rows = slice(k * SUB, (k + 1) * SUB)
        for side in (slice(0, LANES), slice(LANES, 2 * LANES)):
            here = spec[rows, side]
            moved = [here] + [pltpu.roll(here, s, axis=0) for s in range(1, SUB)]
            total = here * gains_ref[0, k : k + 1, :]
            for d in range(1, SUB):
                pair = jnp.where(row >= d, moved[d], 0.0) + jnp.where(row < SUB - d, moved[SUB - d], 0.0)
                total += pair * gains_ref[d, k : k + 1, :]
            out_ref[rows, side] = total
    inverse_copy.wait()
    starts_copy.wait()


def tile_kernel(
    own_ref, below_ref, above_ref, starts, turns_ref, forward_ref, inverse_ref, gains_ref, out_ref,
    sheet
):
    blocks = above_ref.shape[1] // LANES
    halo = [
        jnp.concatenate((lanes_of(above_ref, a), lanes_of(below_ref, a)), axis=0).astype(jnp.float32)
        for a in range(blocks)
    ]
    spec = spectrum(halo, turns_ref, forward_ref)
    row = lax.broadcasted_iota(jnp.int32, (SUB, LANES), 0)
    lane = lax.broadcasted_iota(jnp.int32, (SUB, LANES), 1)
    parts = []
    for k in range(blocks // 2 + 1):
        rows = slice(k * SUB, (k + 1) * SUB)
        both = []
        for side in (slice(0, LANES), slice(LANES, 2 * LANES)):
            here = spec[rows, side]
            total = own_ref[rows, side] + here * gains_ref[0, k]
            for s in range(1, SUB):
                total += pltpu.roll(here, s, axis=0) * gains_ref[s, k]
            both.append(total)
        parts.append(jnp.concatenate(both, axis=1))
    filtered = columns(jnp.concatenate(parts, axis=0), turns_ref, inverse_ref, blocks)
    for a in range(blocks):
        sheet[a] = filtered[a]
    regions = starts.shape[1]
    cut = out_ref.shape[0] * LANES // (regions * SUB)
    per = LANES // cut
    keep = lane // cut == row % per
    packed = []
    for group in range(regions // per):
        gathered = None
        for q in range(per):
            start = starts[0, group * per + q]
            block = lax.shift_right_logical(start, 7)
            offset = start & (LANES - 1)
            window = jnp.where(lane >= offset, sheet[block], sheet[block + 1])
            window = pltpu.roll(window, (LANES + q * cut - offset) & (LANES - 1), axis=1)
            gathered = window if q == 0 else jnp.where(lane // cut == q, window, gathered)
        for shift in range(per):
            moved = gathered if shift == 0 else pltpu.roll(gathered, shift * cut, axis=1)
            packed.append(jnp.where(keep, moved, 0.0).astype(jnp.bfloat16))
    lines = out_ref.shape[0]
    want = lax.broadcasted_iota(jnp.int32, (lines, regions * SUB), 0)
    have = lax.broadcasted_iota(jnp.int32, (lines, regions * SUB), 1)
    have_row, have_shift, have_group = have % SUB, have // SUB % per, have // (SUB * per)
    have_region = have_group * per + (have_row % per + per - have_shift) % per
    pick = jnp.where(have_region * (SUB // per) + have_row // per == want, 1.0, 0.0).astype(jnp.bfloat16)
    out = jnp.dot(pick, jnp.concatenate(packed, axis=0), preferred_element_type=jnp.float32)
    out_ref[...] = out.astype(jnp.bfloat16)


def pixels_kernel(lines_ref, weights_ref, out_ref, lines, *, angles):
    lines[...] = lines_ref[...].astype(jnp.float32)
    cut = lines_ref.shape[0] * LANES // SUB // angles
    per = LANES // cut
    row = lax.broadcasted_iota(jnp.int32, (SUB, LANES), 0)
    lane = lax.broadcasted_iota(jnp.int32, (SUB, LANES), 1)
    turn = (lane // cut + per - row % per) % per
    parts = []
    for group in range(angles // per):
        spread = []
        for q in range(per):
            at = (group * per + q) * (SUB // per)
            low = jnp.broadcast_to(lines[at : at + 1, :], (SUB, LANES))
            high = jnp.broadcast_to(lines[at + 1 : at + 2, :], (SUB, LANES))
            spread.append(jnp.where(row < per, low, high))
        part = None
        for shift in range(per):
            mixed = spread[shift]
            for j in range(1, per):
                mixed = jnp.where(row % per == j, spread[(j + shift) % per], mixed)
            if shift > 0:
                mixed = pltpu.roll(mixed, shift * cut, axis=1)
            part = mixed if shift == 0 else jnp.where(turn == shift, mixed, part)
        parts.append(part.astype(jnp.bfloat16))
    out_ref[...] = jnp.dot(jnp.concatenate(parts, axis=1), weights_ref[...], preferred_element_type=jnp.float32)


def in_hbm(array):
    return pltpu.with_memory_space_constraint(array, pltpu.HBM)


def make_contrast(projections, flats):
    shape = flats.shape
    edge = jax.ShapeDtypeStruct((HALO, shape[1]), halo_type)
    return pl.pallas_call(
        contrast_kernel,
        out_shape=(jax.ShapeDtypeStruct(shape, jnp.float32), edge, edge),
        in_specs=[HBM] * 2,
        out_specs=(VMEM,) * 3,
        scratch_shapes=[
            pltpu.VMEM(projections.shape, projections.dtype),
            pltpu.VMEM(flats.shape, flats.dtype),
            pltpu.SemaphoreType.DMA((2,)),
        ],
        compiler_params=PARAMS,
        name="contrast",
    )(in_hbm(projections), in_hbm(flats))


def make_own(own, turns, forward, inverse, gains, starts):
    groups = turns.shape[1]
    return pl.pallas_call(
        own_kernel,
        out_shape=(
            jax.ShapeDtypeStruct((groups * SUB, 2 * LANES), jnp.float32),
            jax.ShapeDtypeStruct(forward.shape, forward.dtype),
            jax.ShapeDtypeStruct(inverse.shape, inverse.dtype),
            jax.ShapeDtypeStruct((SUB, groups, SUB, LANES), jnp.float32),
            pltpu.SMEM((1, starts.shape[1]), jnp.int32),
        ),
        in_specs=[VMEM] * 3 + [HBM] * 3,
        out_specs=(VMEM,) * 4 + (SMEM,),
        scratch_shapes=[pltpu.SemaphoreType.DMA((3,))],
        compiler_params=PARAMS,
        name="own_rows",
    )(own, turns, gains, in_hbm(forward), in_hbm(inverse), in_hbm(starts))


def make_tile(own_spec, below, above, starts, turns, forward, inverse, gains, cut):
    regions = starts.shape[1]
    return pl.pallas_call(
        tile_kernel,
        out_shape=jax.ShapeDtypeStruct((regions * SUB * cut // LANES, LANES), jnp.bfloat16),
        in_specs=[VMEM] * 3 + [SMEM] + [VMEM] * 4,
        out_specs=VMEM,
        scratch_shapes=[
            pltpu.VMEM((above.shape[1] // LANES + 1, SUB, LANES), jnp.float32),
        ],
        compiler_params=PARAMS,
        name="tile",
    )(own_spec, below, above, starts, turns, forward, inverse, gains)


def make_pixels(lines, weights):
    angles, cut, pixels = weights.shape
    return pl.pallas_call(
        partial(pixels_kernel, angles=angles),
        out_shape=jax.ShapeDtypeStruct((SUB, pixels), jnp.float32),
        in_specs=[VMEM] * 2,
        out_specs=VMEM,
        scratch_shapes=[pltpu.VMEM(lines.shape, jnp.float32)],
        compiler_params=PARAMS,
        name="pixels",
    )(lines, weights.reshape(angles * cut, pixels))


def body(projections, flats, block_start, bp_weights):
    angles_dev, rows_dev, width = projections.shape
    cut = bp_weights.shape[1]
    assert angles_dev == 1 and rows_dev == SUB and width % (2 * LANES) == 0 and SUB * cut == 2 * LANES
    rows = lax.axis_size("row")
    up = [(i, i + 1) for i in range(rows - 1)]
    down = [(j, i) for i, j in up]
    turns, forward, inverse, gains = (jnp.asarray(t) for t in tables(width, rows_dev + 2 * HALO))
    own, first, last = make_contrast(projections, flats)
    below = lax.ppermute(first, "row", down)
    above = lax.ppermute(last, "row", up)
    own_spec, forward, inverse, gains, starts = make_own(own, turns, forward, inverse, gains, block_start)
    outgoing = make_tile(own_spec, below, above, starts, turns, forward, inverse, gains, cut)
    incoming = lax.all_to_all(outgoing, "ang", split_axis=0, concat_axis=0, tiled=True)
    return make_pixels(incoming, bp_weights)


def solution(mesh):
    placed = (P(("scan", "ang"), "row", None), P(("scan", "row"), None), P(), P(None, None, "ang"))
    return jax.shard_map(
        body, mesh=mesh, in_specs=placed, out_specs=P(("scan", "row"), "ang"), check_vma=False
    )
```

```python
from functools import partial

import jax
import jax.numpy as jnp
import numpy as np
from jax import lax
from jax.experimental import pallas as pl
from jax.experimental.pallas import tpu as pltpu
from jax.sharding import PartitionSpec as P

HALO = 4
LANES = 128
SUB = 8

paganin_beta = 8.0
ramp_gain = 320.0
halo_type = jnp.float32
VMEM = pl.BlockSpec(memory_space=pltpu.VMEM)
SMEM = pl.BlockSpec(memory_space=pltpu.SMEM)
HBM = pl.BlockSpec(memory_space=pltpu.HBM)
PARAMS = pltpu.CompilerParams(vmem_limit_bytes=8 * 2**20)


def tables(width, tile_rows):
    blocks = width // LANES
    half = blocks // 2
    lane = np.arange(LANES)
    ks = np.arange(half + 1)
    turn = 2.0 * np.pi / width * (ks[:, None] * lane[None, :])
    turns = np.stack((np.cos(turn), np.sin(turn))).astype(np.float32)
    angle = 2.0 * np.pi / LANES * (lane[:, None] * lane[None, :] % LANES)
    cos, sin = np.cos(angle), np.sin(angle)
    forward = np.block([[cos, -sin], [sin, cos]])

    def split(matrix):
        high = matrix.astype(jnp.bfloat16)
        low = (matrix - high.astype(np.float64)).astype(jnp.bfloat16)
        return np.stack((high, low))

    freq = (ks[:, None] + blocks * lane[None, :]).astype(np.float64)
    row = np.arange(tile_rows, dtype=np.float64)
    lam = 4.0 * np.sin(np.pi * row / tile_rows)[:, None, None] ** 2 + 4.0 * np.sin(np.pi * freq / width) ** 2
    filt = 1.0 / (1.0 + paganin_beta * lam)
    dist = np.arange(tile_rows // 2 + 1)
    gains = np.einsum("du,ukm->dkm", np.cos(2.0 * np.pi / tile_rows * dist[:, None] * row), filt) / tile_rows
    folded = np.minimum(freq, width - freq)
    ramp = ramp_gain * (folded / width) * (0.5 + 0.5 * np.cos(2.0 * np.pi * folded / width))
    twice = np.where((ks == 0) | (ks == half), 1.0, 2.0)
    gains = gains * (ramp * twice[:, None] / width)
    return turns, split(forward), split(forward.T), gains.astype(np.float32)


def plus(terms):
    return sum(terms[1:], terms[0])


def scaled(terms, weights):
    out = None
    for term, weight in zip(terms, weights):
        weight = float(weight)
        if abs(weight) < 1e-12:
            continue
        piece = term if weight == 1.0 else -term if weight == -1.0 else term * weight
        out = piece if out is None else out + piece
    return out


def cosine_sums(terms, blocks):
    half = blocks // 2
    out = [None] * (half + 1)
    for k in range(half // 2 + 1):
        wave = [np.round(np.cos(2.0 * np.pi * a * k / blocks), 15) for a in range(half + 1)]
        even = scaled(terms[0::2], wave[0::2])
        odd = scaled(terms[1::2], wave[1::2])
        out[k] = even if odd is None else even + odd
        if half - k != k:
            out[half - k] = even if odd is None else even - odd
    return out


def sine_sums(terms, blocks):
    half = blocks // 2
    out = [None] * (half + 1)
    for k in range(1, half // 2 + 1):
        wave = [np.round(np.sin(2.0 * np.pi * a * k / blocks), 15) for a in range(half)]
        even = scaled(terms[2:half:2], wave[2::2])
        odd = scaled(terms[1:half:2], wave[1::2])
        if half - k != k:
            out[k] = plus([x for x in (even, odd) if x is not None])
            out[half - k] = odd - even if even is not None else odd
        else:
            out[k] = plus([x for x in (even, odd) if x is not None])
    return out


def accurate_dot(values, matrix_ref):
    high = values.astype(jnp.bfloat16)
    low = (values - high.astype(jnp.float32)).astype(jnp.bfloat16)
    dot = partial(jnp.dot, preferred_element_type=jnp.float32)
    lines = values.shape[0]
    both = dot(jnp.concatenate((high, low), axis=0), matrix_ref[0])
    return both[:lines] + (both[lines:] + dot(high, matrix_ref[1]))


def spectrum(chunks, turns_ref, forward_ref):
    blocks = len(chunks)
    half = blocks // 2
    folds = [chunks[0]] + [chunks[a] + chunks[blocks - a] for a in range(1, half)] + [chunks[half]]
    skews = [None] + [chunks[a] - chunks[blocks - a] for a in range(1, half)] + [None]
    reals = cosine_sums(folds, blocks)
    imags = sine_sums(skews, blocks)
    parts = []
    for k in range(half + 1):
        cos, sin = turns_ref[0, k : k + 1, :], turns_ref[1, k : k + 1, :]
        if k == 0:
            re, im = reals[0], jnp.zeros_like(reals[0])
        elif imags[k] is None:
            re, im = reals[k] * cos, -(reals[k] * sin)
        else:
            re, im = reals[k] * cos - imags[k] * sin, -(imags[k] * cos) - reals[k] * sin
        parts.append(jnp.concatenate((re, im), axis=1))
    return accurate_dot(jnp.concatenate(parts, axis=0), forward_ref)


def columns(spec, turns_ref, inverse_ref, blocks):
    half = blocks // 2
    back = accurate_dot(spec, inverse_ref)
    reals, imags = [], []
    for k in range(half + 1):
        rows = slice(k * SUB, (k + 1) * SUB)
        re, im = back[rows, :LANES], back[rows, LANES:]
        cos, sin = turns_ref[0, k : k + 1, :], turns_ref[1, k : k + 1, :]
        if k == 0:
            reals.append(re)
            imags.append(None)
        else:
            reals.append(re * cos - im * sin)
            imags.append(im * cos + re * sin if k < half else None)
    even = cosine_sums(reals, blocks)
    odd = sine_sums(imags, blocks)
    out = [None] * blocks
    out[0], out[half] = even[0], even[half]
    for a in range(1, half):
        out[a] = even[a] - odd[a]
        out[blocks - a] = even[a] + odd[a]
    return out


def contrast_kernel(proj_hbm, flat_hbm, own_ref, first_ref, last_ref, proj, flat, sems):
    copies = [
        pltpu.make_async_copy(proj_hbm, proj, sems.at[0]),
        pltpu.make_async_copy(flat_hbm, flat, sems.at[1]),
    ]
    for copy in copies:
        copy.start()
    for copy in copies:
        copy.wait()
    own = 1.0 - proj[0].astype(jnp.float32) / flat[...]
    own_ref[...] = own
    first_ref[...] = own[:HALO].astype(first_ref.dtype)
    last_ref[...] = own[SUB - HALO :].astype(last_ref.dtype)


def lanes_of(ref, block):
    return ref[:, block * LANES : (block + 1) * LANES]


def halo_gains(gains_ref, k, row):
    gains = [jnp.broadcast_to(gains_ref[d, k : k + 1, :], (SUB, LANES)) for d in range(2 * HALO + 1)]
    for s in range(SUB):
        far = gains[2 * HALO - abs(s - HALO)]
        near = gains[abs(s - HALO)]
        if s < HALO:
            yield s, jnp.where(row >= s + HALO, near, far)
        else:
            yield s, jnp.where(row < s - HALO, near, far)


def own_kernel(
    own_ref, turns_ref, gains_ref, forward_hbm, inverse_hbm, starts_hbm,
    out_ref, forward_ref, inverse_ref, halo_ref, starts_ref, sems
):
    forward_copy = pltpu.make_async_copy(forward_hbm, forward_ref, sems.at[0])
    inverse_copy = pltpu.make_async_copy(inverse_hbm, inverse_ref, sems.at[1])
    starts_copy = pltpu.make_async_copy(starts_hbm.at[pl.ds(lax.axis_index("ang"), 1)], starts_ref, sems.at[2])
    forward_copy.start()
    inverse_copy.start()
    starts_copy.start()
    row = lax.broadcasted_iota(jnp.int32, (SUB, LANES), 0)
    for k in range(gains_ref.shape[1]):
        for s, gain in halo_gains(gains_ref, k, row):
            halo_ref[s, k] = gain
    forward_copy.wait()
    blocks = own_ref.shape[1] // LANES
    spec = spectrum([lanes_of(own_ref, a) for a in range(blocks)], turns_ref, forward_ref)
    for k in range(blocks // 2 + 1):
        rows = slice(k * SUB, (k + 1) * SUB)
        for side in (slice(0, LANES), slice(LANES, 2 * LANES)):
            here = spec[rows, side]
            moved = [here] + [pltpu.roll(here, s, axis=0) for s in range(1, SUB)]
            total = here * gains_ref[0, k : k + 1, :]
            for d in range(1, SUB):
                pair = jnp.where(row >= d, moved[d], 0.0) + jnp.where(row < SUB - d, moved[SUB - d], 0.0)
                total += pair * gains_ref[d, k : k + 1, :]
            out_ref[rows, side] = total
    inverse_copy.wait()
    starts_copy.wait()


def tile_kernel(
    own_ref, below_ref, above_ref, starts, turns_ref, forward_ref, inverse_ref, gains_ref, out_ref,
    sheet
):
    blocks = above_ref.shape[1] // LANES
    halo = [
        jnp.concatenate((lanes_of(above_ref, a), lanes_of(below_ref, a)), axis=0).astype(jnp.float32)
        for a in range(blocks)
    ]
    spec = spectrum(halo, turns_ref, forward_ref)
    row = lax.broadcasted_iota(jnp.int32, (SUB, LANES), 0)
    lane = lax.broadcasted_iota(jnp.int32, (SUB, LANES), 1)
    parts = []
    for k in range(blocks // 2 + 1):
        rows = slice(k * SUB, (k + 1) * SUB)
        both = []
        for side in (slice(0, LANES), slice(LANES, 2 * LANES)):
            here = spec[rows, side]
            total = own_ref[rows, side] + here * gains_ref[0, k]
            for s in range(1, SUB):
                total += pltpu.roll(here, s, axis=0) * gains_ref[s, k]
            both.append(total)
        parts.append(jnp.concatenate(both, axis=1))
    filtered = columns(jnp.concatenate(parts, axis=0), turns_ref, inverse_ref, blocks)
    for a in range(blocks):
        sheet[a] = filtered[a]
    regions = starts.shape[1]
    cut = out_ref.shape[0] * LANES // (regions * SUB)
    per = LANES // cut
    keep = lane // cut == row % per
    packed = []
    for group in range(regions // per):
        gathered = None
        for q in range(per):
            start = starts[0, group * per + q]
            block = lax.shift_right_logical(start, 7)
            offset = start & (LANES - 1)
            window = jnp.where(lane >= offset, sheet[block], sheet[block + 1])
            window = pltpu.roll(window, (LANES + q * cut - offset) & (LANES - 1), axis=1)
            gathered = window if q == 0 else jnp.where(lane // cut == q, window, gathered)
        for shift in range(per):
            moved = gathered if shift == 0 else pltpu.roll(gathered, shift * cut, axis=1)
            packed.append(jnp.where(keep, moved, 0.0).astype(jnp.bfloat16))
    lines = out_ref.shape[0]
    want = lax.broadcasted_iota(jnp.int32, (lines, regions * SUB), 0)
    have = lax.broadcasted_iota(jnp.int32, (lines, regions * SUB), 1)
    have_row, have_shift, have_group = have % SUB, have // SUB % per, have // (SUB * per)
    have_region = have_group * per + (have_row % per + per - have_shift) % per
    pick = jnp.where(have_region * (SUB // per) + have_row // per == want, 1.0, 0.0).astype(jnp.bfloat16)
    out = jnp.dot(pick, jnp.concatenate(packed, axis=0), preferred_element_type=jnp.float32)
    out_ref[...] = out.astype(jnp.bfloat16)


class Routes:
    UNITS = 4
    AROUND = 16

    def __init__(self, count):
        step = count // self.AROUND
        devices = lambda steps: [s * step + c for s in steps for c in range(step)]
        link = lambda pairs: [p for src, dst in pairs for p in zip(devices([src]), devices([dst]))]
        self.count, self.half = count, count // 2
        self.near = devices((12, 13, 14, 15, 0, 1, 2, 3))
        self.far = devices(range(4, 12))
        self.relays = devices((12, 1, 2, 3))
        first = link(((11, 12), (9, 3), (8, 2), (7, 1)))
        self.enter = [first + [(dst, src) for src, dst in first], link(((10, 12), (4, 3), (5, 2), (6, 1)))]
        self.leave = [link(((12, 11), (13, 9), (14, 7), (15, 5))), link(((12, 10), (13, 8), (14, 6), (15, 4)))]

    def exchange_table(self):
        table = np.zeros((3, self.half * self.UNITS * 2, 3 * self.count * 2), np.float32)

        def put(kind, m, unit, source, region):
            for i in range(2):
                table[kind, (m * self.UNITS + unit) * 2 + i, (source * self.count + region) * 2 + i] = 1.0

        for m, dest in enumerate(self.far):
            put(0, m, 0, 0, dest)
            put(0, m, 1, 1, dest)
        for m, dest in enumerate(self.near):
            put(1, m, 0, 0, dest)
            put(2, m, 0, 0, dest)
            for turn in range(2):
                put(1, m, 1 + turn, 1 + turn, dest)
                for src, final in self.leave[turn]:
                    if src == dest:
                        put(2, m, 1 + turn, 0, final)
        return table.astype(jnp.bfloat16)

    def arrival_table(self):
        size = self.half * self.UNITS
        table = np.zeros((3, self.count * 2, 3 * size * 2), np.float32)

        def put(kind, angle, source, m, unit):
            for i in range(2):
                table[kind, angle * 2 + i, (source * size + m * self.UNITS + unit) * 2 + i] = 1.0

        for m, angle in enumerate(self.near):
            put(0, angle, 0, m, 0)
            for turn in range(2):
                for src, dst in self.enter[turn]:
                    if dst == angle:
                        put(0, src, 0, m, 1 + turn)
                if angle not in self.relays:
                    put(1 + turn, angle, 1 + turn, m, 1 + turn)
        for m, angle in enumerate(self.far):
            for turn in range(2):
                put(1 + turn, angle, 0, m, 0)
                for src, dst in self.enter[0]:
                    if dst == angle:
                        put(1 + turn, src, 0, m, 1)
        return table.astype(jnp.bfloat16)

    @classmethod
    def kinds(cls, device, count):
        step = device // (count // cls.AROUND)
        turned = lax.rem(step + 4, cls.AROUND)
        far = turned >= 8
        other = (turned >= 1) & (turned <= 4)
        return jnp.where(far, 0, jnp.where(other, 2, 1)), jnp.where(far, 2 - step % 2, 0)


def repack_kernel(lines_ref, first_ref, second_ref, table_ref, out_ref):
    kind, _ = Routes.kinds(lax.axis_index("ang"), lax.axis_size("ang"))
    lines = jnp.concatenate((lines_ref[...], first_ref[...], second_ref[...]), axis=0)
    out = jnp.dot(table_ref[kind], lines, preferred_element_type=jnp.float32)
    out_ref[...] = out.astype(out_ref.dtype)


def pixels_kernel(near_ref, first_ref, second_ref, table_ref, weights_ref, out_ref, lines, *, angles):
    _, kind = Routes.kinds(lax.axis_index("ang"), lax.axis_size("ang"))
    held = jnp.concatenate((near_ref[...], first_ref[...], second_ref[...]), axis=0)
    lines[...] = jnp.dot(table_ref[kind], held, preferred_element_type=jnp.float32)
    cut = lines.shape[0] * LANES // SUB // angles
    per = LANES // cut
    row = lax.broadcasted_iota(jnp.int32, (SUB, LANES), 0)
    lane = lax.broadcasted_iota(jnp.int32, (SUB, LANES), 1)
    turn = (lane // cut + per - row % per) % per
    parts = []
    for group in range(angles // per):
        spread = []
        for q in range(per):
            at = (group * per + q) * (SUB // per)
            low = jnp.broadcast_to(lines[at : at + 1, :], (SUB, LANES))
            high = jnp.broadcast_to(lines[at + 1 : at + 2, :], (SUB, LANES))
            spread.append(jnp.where(row < per, low, high))
        part = None
        for shift in range(per):
            mixed = spread[shift]
            for j in range(1, per):
                mixed = jnp.where(row % per == j, spread[(j + shift) % per], mixed)
            if shift > 0:
                mixed = pltpu.roll(mixed, shift * cut, axis=1)
            part = mixed if shift == 0 else jnp.where(turn == shift, mixed, part)
        parts.append(part.astype(jnp.bfloat16))
    out_ref[...] = jnp.dot(jnp.concatenate(parts, axis=1), weights_ref[...], preferred_element_type=jnp.float32)


def in_hbm(array):
    return pltpu.with_memory_space_constraint(array, pltpu.HBM)


def make_contrast(projections, flats):
    shape = flats.shape
    edge = jax.ShapeDtypeStruct((HALO, shape[1]), halo_type)
    return pl.pallas_call(
        contrast_kernel,
        out_shape=(jax.ShapeDtypeStruct(shape, jnp.float32), edge, edge),
        in_specs=[HBM] * 2,
        out_specs=(VMEM,) * 3,
        scratch_shapes=[
            pltpu.VMEM(projections.shape, projections.dtype),
            pltpu.VMEM(flats.shape, flats.dtype),
            pltpu.SemaphoreType.DMA((2,)),
        ],
        compiler_params=PARAMS,
        name="contrast",
    )(in_hbm(projections), in_hbm(flats))


def make_own(own, turns, forward, inverse, gains, starts):
    groups = turns.shape[1]
    return pl.pallas_call(
        own_kernel,
        out_shape=(
            jax.ShapeDtypeStruct((groups * SUB, 2 * LANES), jnp.float32),
            jax.ShapeDtypeStruct(forward.shape, forward.dtype),
            jax.ShapeDtypeStruct(inverse.shape, inverse.dtype),
            jax.ShapeDtypeStruct((SUB, groups, SUB, LANES), jnp.float32),
            pltpu.SMEM((1, starts.shape[1]), jnp.int32),
        ),
        in_specs=[VMEM] * 3 + [HBM] * 3,
        out_specs=(VMEM,) * 4 + (SMEM,),
        scratch_shapes=[pltpu.SemaphoreType.DMA((3,))],
        compiler_params=PARAMS,
        name="own_rows",
    )(own, turns, gains, in_hbm(forward), in_hbm(inverse), in_hbm(starts))


def make_tile(own_spec, below, above, starts, turns, forward, inverse, gains, cut):
    regions = starts.shape[1]
    return pl.pallas_call(
        tile_kernel,
        out_shape=jax.ShapeDtypeStruct((regions * SUB * cut // LANES, LANES), jnp.bfloat16),
        in_specs=[VMEM] * 3 + [SMEM] + [VMEM] * 4,
        out_specs=VMEM,
        scratch_shapes=[
            pltpu.VMEM((above.shape[1] // LANES + 1, SUB, LANES), jnp.float32),
        ],
        compiler_params=PARAMS,
        name="tile",
    )(own_spec, below, above, starts, turns, forward, inverse, gains)


def make_repack(lines, first, second, table):
    return pl.pallas_call(
        repack_kernel,
        out_shape=jax.ShapeDtypeStruct((table.shape[1], LANES), lines.dtype),
        in_specs=[VMEM] * 4,
        out_specs=VMEM,
        compiler_params=PARAMS,
        name="repack",
    )(lines, first, second, table)


def make_pixels(near, first, second, table, weights):
    angles, cut, pixels = weights.shape
    return pl.pallas_call(
        partial(pixels_kernel, angles=angles),
        out_shape=jax.ShapeDtypeStruct((SUB, pixels), jnp.float32),
        in_specs=[VMEM] * 5,
        out_specs=VMEM,
        scratch_shapes=[pltpu.VMEM((table.shape[1], LANES), jnp.float32)],
        compiler_params=PARAMS,
        name="pixels",
    )(near, first, second, table, weights.reshape(angles * cut, pixels))


def body(projections, flats, block_start, bp_weights):
    angles_dev, rows_dev, width = projections.shape
    cut = bp_weights.shape[1]
    assert angles_dev == 1 and rows_dev == SUB and width % (2 * LANES) == 0 and SUB * cut == 2 * LANES
    rows = lax.axis_size("row")
    up = [(i, i + 1) for i in range(rows - 1)]
    down = [(j, i) for i, j in up]
    turns, forward, inverse, gains = (jnp.asarray(t) for t in tables(width, rows_dev + 2 * HALO))
    own, first, last = make_contrast(projections, flats)
    below = lax.ppermute(first, "row", down)
    above = lax.ppermute(last, "row", up)
    own_spec, forward, inverse, gains, starts = make_own(own, turns, forward, inverse, gains, block_start)
    outgoing = make_tile(own_spec, below, above, starts, turns, forward, inverse, gains, cut)
    routes = Routes(lax.axis_size("ang"))
    entered = [lax.ppermute(outgoing, "ang", pairs) for pairs in routes.enter]
    packed = make_repack(outgoing, *entered, jnp.asarray(routes.exchange_table()))
    near = lax.all_to_all(
        packed, "ang", split_axis=0, concat_axis=0, tiled=True, axis_index_groups=[routes.near, routes.far]
    )
    left = [lax.ppermute(near, "ang", pairs) for pairs in routes.leave]
    return make_pixels(near, *left, jnp.asarray(routes.arrival_table()), bp_weights)


def solution(mesh):
    placed = (P(("scan", "ang"), "row", None), P(("scan", "row"), None), P(), P(None, None, "ang"))
    return jax.shard_map(
        body, mesh=mesh, in_specs=placed, out_specs=P(("scan", "row"), "ang"), check_vma=False
    )
```

```python
from functools import partial

import jax
import jax.numpy as jnp
import numpy as np
from jax import lax
from jax.experimental import pallas as pl
from jax.experimental.pallas import tpu as pltpu
from jax.sharding import PartitionSpec as P

HALO = 4
LANES = 128
SUB = 8

paganin_beta = 8.0
ramp_gain = 320.0
halo_type = jnp.float32
VMEM = pl.BlockSpec(memory_space=pltpu.VMEM)
SMEM = pl.BlockSpec(memory_space=pltpu.SMEM)
HBM = pl.BlockSpec(memory_space=pltpu.HBM)
PARAMS = pltpu.CompilerParams(vmem_limit_bytes=8 * 2**20)


def tables(width, tile_rows):
    blocks = width // LANES
    half = blocks // 2
    lane = np.arange(LANES)
    ks = np.arange(half + 1)
    turn = 2.0 * np.pi / width * (ks[:, None] * lane[None, :])
    turns = np.stack((np.cos(turn), np.sin(turn))).astype(np.float32)
    angle = 2.0 * np.pi / LANES * (lane[:, None] * lane[None, :] % LANES)
    cos, sin = np.cos(angle), np.sin(angle)
    forward = np.block([[cos, -sin], [sin, cos]])

    def split(matrix):
        high = matrix.astype(jnp.bfloat16)
        low = (matrix - high.astype(np.float64)).astype(jnp.bfloat16)
        return np.stack((high, low))

    freq = (ks[:, None] + blocks * lane[None, :]).astype(np.float64)
    row = np.arange(tile_rows, dtype=np.float64)
    lam = 4.0 * np.sin(np.pi * row / tile_rows)[:, None, None] ** 2 + 4.0 * np.sin(np.pi * freq / width) ** 2
    filt = 1.0 / (1.0 + paganin_beta * lam)
    dist = np.arange(tile_rows // 2 + 1)
    gains = np.einsum("du,ukm->dkm", np.cos(2.0 * np.pi / tile_rows * dist[:, None] * row), filt) / tile_rows
    folded = np.minimum(freq, width - freq)
    ramp = ramp_gain * (folded / width) * (0.5 + 0.5 * np.cos(2.0 * np.pi * folded / width))
    twice = np.where((ks == 0) | (ks == half), 1.0, 2.0)
    gains = gains * (ramp * twice[:, None] / width)
    return turns, split(forward), split(forward.T), gains.astype(np.float32)


def plus(terms):
    return sum(terms[1:], terms[0])


def scaled(terms, weights):
    out = None
    for term, weight in zip(terms, weights):
        weight = float(weight)
        if abs(weight) < 1e-12:
            continue
        piece = term if weight == 1.0 else -term if weight == -1.0 else term * weight
        out = piece if out is None else out + piece
    return out


def cosine_sums(terms, blocks):
    half = blocks // 2
    out = [None] * (half + 1)
    for k in range(half // 2 + 1):
        wave = [np.round(np.cos(2.0 * np.pi * a * k / blocks), 15) for a in range(half + 1)]
        even = scaled(terms[0::2], wave[0::2])
        odd = scaled(terms[1::2], wave[1::2])
        out[k] = even if odd is None else even + odd
        if half - k != k:
            out[half - k] = even if odd is None else even - odd
    return out


def sine_sums(terms, blocks):
    half = blocks // 2
    out = [None] * (half + 1)
    for k in range(1, half // 2 + 1):
        wave = [np.round(np.sin(2.0 * np.pi * a * k / blocks), 15) for a in range(half)]
        even = scaled(terms[2:half:2], wave[2::2])
        odd = scaled(terms[1:half:2], wave[1::2])
        if half - k != k:
            out[k] = plus([x for x in (even, odd) if x is not None])
            out[half - k] = odd - even if even is not None else odd
        else:
            out[k] = plus([x for x in (even, odd) if x is not None])
    return out


def accurate_dot(values, matrix_ref):
    high = values.astype(jnp.bfloat16)
    low = (values - high.astype(jnp.float32)).astype(jnp.bfloat16)
    dot = partial(jnp.dot, preferred_element_type=jnp.float32)
    lines = values.shape[0]
    both = dot(jnp.concatenate((high, low), axis=0), matrix_ref[0])
    return both[:lines] + (both[lines:] + dot(high, matrix_ref[1]))


def spectrum(chunks, turns_ref, forward_ref):
    blocks = len(chunks)
    half = blocks // 2
    folds = [chunks[0]] + [chunks[a] + chunks[blocks - a] for a in range(1, half)] + [chunks[half]]
    skews = [None] + [chunks[a] - chunks[blocks - a] for a in range(1, half)] + [None]
    reals = cosine_sums(folds, blocks)
    imags = sine_sums(skews, blocks)
    parts = []
    for k in range(half + 1):
        cos, sin = turns_ref[0, k : k + 1, :], turns_ref[1, k : k + 1, :]
        if k == 0:
            re, im = reals[0], jnp.zeros_like(reals[0])
        elif imags[k] is None:
            re, im = reals[k] * cos, -(reals[k] * sin)
        else:
            re, im = reals[k] * cos - imags[k] * sin, -(imags[k] * cos) - reals[k] * sin
        parts.append(jnp.concatenate((re, im), axis=1))
    return accurate_dot(jnp.concatenate(parts, axis=0), forward_ref)


def columns(spec, turns_ref, inverse_ref, blocks):
    half = blocks // 2
    back = accurate_dot(spec, inverse_ref)
    reals, imags = [], []
    for k in range(half + 1):
        rows = slice(k * SUB, (k + 1) * SUB)
        re, im = back[rows, :LANES], back[rows, LANES:]
        cos, sin = turns_ref[0, k : k + 1, :], turns_ref[1, k : k + 1, :]
        if k == 0:
            reals.append(re)
            imags.append(None)
        else:
            reals.append(re * cos - im * sin)
            imags.append(im * cos + re * sin if k < half else None)
    even = cosine_sums(reals, blocks)
    odd = sine_sums(imags, blocks)
    out = [None] * blocks
    out[0], out[half] = even[0], even[half]
    for a in range(1, half):
        out[a] = even[a] - odd[a]
        out[blocks - a] = even[a] + odd[a]
    return out


def contrast_kernel(proj_hbm, flat_hbm, own_ref, first_ref, last_ref, proj, flat, sems):
    copies = [
        pltpu.make_async_copy(proj_hbm, proj, sems.at[0]),
        pltpu.make_async_copy(flat_hbm, flat, sems.at[1]),
    ]
    for copy in copies:
        copy.start()
    for copy in copies:
        copy.wait()
    own = 1.0 - proj[0].astype(jnp.float32) / flat[...]
    own_ref[...] = own
    first_ref[...] = own[:HALO].astype(first_ref.dtype)
    last_ref[...] = own[SUB - HALO :].astype(last_ref.dtype)


def lanes_of(ref, block):
    return ref[:, block * LANES : (block + 1) * LANES]


def halo_gains(gains_ref, k, row):
    gains = [jnp.broadcast_to(gains_ref[d, k : k + 1, :], (SUB, LANES)) for d in range(2 * HALO + 1)]
    for s in range(SUB):
        far = gains[2 * HALO - abs(s - HALO)]
        near = gains[abs(s - HALO)]
        if s < HALO:
            yield s, jnp.where(row >= s + HALO, near, far)
        else:
            yield s, jnp.where(row < s - HALO, near, far)


def own_kernel(
    own_ref, turns_ref, gains_ref, forward_hbm, inverse_hbm, starts_hbm,
    out_ref, forward_ref, inverse_ref, halo_ref, starts_ref, sems
):
    forward_copy = pltpu.make_async_copy(forward_hbm, forward_ref, sems.at[0])
    inverse_copy = pltpu.make_async_copy(inverse_hbm, inverse_ref, sems.at[1])
    starts_copy = pltpu.make_async_copy(starts_hbm.at[pl.ds(lax.axis_index("ang"), 1)], starts_ref, sems.at[2])
    forward_copy.start()
    inverse_copy.start()
    starts_copy.start()
    row = lax.broadcasted_iota(jnp.int32, (SUB, LANES), 0)
    for k in range(gains_ref.shape[1]):
        for s, gain in halo_gains(gains_ref, k, row):
            halo_ref[s, k] = gain
    forward_copy.wait()
    blocks = own_ref.shape[1] // LANES
    spec = spectrum([lanes_of(own_ref, a) for a in range(blocks)], turns_ref, forward_ref)
    for k in range(blocks // 2 + 1):
        rows = slice(k * SUB, (k + 1) * SUB)
        for side in (slice(0, LANES), slice(LANES, 2 * LANES)):
            here = spec[rows, side]
            moved = [here] + [pltpu.roll(here, s, axis=0) for s in range(1, SUB)]
            total = here * gains_ref[0, k : k + 1, :]
            for d in range(1, SUB):
                pair = jnp.where(row >= d, moved[d], 0.0) + jnp.where(row < SUB - d, moved[SUB - d], 0.0)
                total += pair * gains_ref[d, k : k + 1, :]
            out_ref[rows, side] = total
    inverse_copy.wait()
    starts_copy.wait()


def tile_kernel(
    own_ref, below_ref, above_ref, starts, turns_ref, forward_ref, inverse_ref, gains_ref, out_ref,
    sheet
):
    blocks = above_ref.shape[1] // LANES
    halo = [
        jnp.concatenate((lanes_of(above_ref, a), lanes_of(below_ref, a)), axis=0).astype(jnp.float32)
        for a in range(blocks)
    ]
    spec = spectrum(halo, turns_ref, forward_ref)
    row = lax.broadcasted_iota(jnp.int32, (SUB, LANES), 0)
    lane = lax.broadcasted_iota(jnp.int32, (SUB, LANES), 1)
    parts = []
    for k in range(blocks // 2 + 1):
        rows = slice(k * SUB, (k + 1) * SUB)
        both = []
        for side in (slice(0, LANES), slice(LANES, 2 * LANES)):
            here = spec[rows, side]
            total = own_ref[rows, side] + here * gains_ref[0, k]
            for s in range(1, SUB):
                total += pltpu.roll(here, s, axis=0) * gains_ref[s, k]
            both.append(total)
        parts.append(jnp.concatenate(both, axis=1))
    filtered = columns(jnp.concatenate(parts, axis=0), turns_ref, inverse_ref, blocks)
    for a in range(blocks):
        sheet[a] = filtered[a]
    regions = starts.shape[1]
    cut = out_ref.shape[0] * LANES // (regions * SUB)
    per = LANES // cut
    keep = lane // cut == row % per
    packed = []
    for group in range(regions // per):
        gathered = None
        for q in range(per):
            start = starts[0, group * per + q]
            block = lax.shift_right_logical(start, 7)
            offset = start & (LANES - 1)
            window = jnp.where(lane >= offset, sheet[block], sheet[block + 1])
            window = pltpu.roll(window, (LANES + q * cut - offset) & (LANES - 1), axis=1)
            gathered = window if q == 0 else jnp.where(lane // cut == q, window, gathered)
        for shift in range(per):
            moved = gathered if shift == 0 else pltpu.roll(gathered, shift * cut, axis=1)
            packed.append(jnp.where(keep, moved, 0.0).astype(jnp.bfloat16))
    lines = out_ref.shape[0]
    want = lax.broadcasted_iota(jnp.int32, (lines, regions * SUB), 0)
    have = lax.broadcasted_iota(jnp.int32, (lines, regions * SUB), 1)
    have_row, have_shift, have_group = have % SUB, have // SUB % per, have // (SUB * per)
    have_region = have_group * per + (have_row % per + per - have_shift) % per
    pick = jnp.where(have_region * (SUB // per) + have_row // per == want, 1.0, 0.0).astype(jnp.bfloat16)
    out = jnp.dot(pick, jnp.concatenate(packed, axis=0), preferred_element_type=jnp.float32)
    out_ref[...] = out.astype(jnp.bfloat16)


class Routes:
    UNITS = 4
    AROUND = 16

    def __init__(self, count):
        step = count // self.AROUND
        devices = lambda steps: [s * step + c for s in steps for c in range(step)]
        link = lambda pairs: [p for src, dst in pairs for p in zip(devices([src]), devices([dst]))]
        self.count, self.half = count, count // 2
        self.near = devices((12, 13, 14, 15, 0, 1, 2, 3))
        self.far = devices(range(4, 12))
        self.relays = devices((12, 1, 2, 3))
        first = link(((11, 12), (9, 3), (8, 2), (7, 1)))
        self.enter = [first + [(dst, src) for src, dst in first], link(((10, 12), (4, 3), (5, 2), (6, 1)))]
        self.leave = [link(((12, 11), (13, 9), (2, 6), (3, 4))), link(((12, 10), (13, 8), (2, 7), (3, 5)))]

    def exchange_table(self):
        table = np.zeros((3, self.half * self.UNITS * 2, 3 * self.count * 2), np.float32)

        def put(kind, m, unit, source, region):
            for i in range(2):
                table[kind, (m * self.UNITS + unit) * 2 + i, (source * self.count + region) * 2 + i] = 1.0

        for m, dest in enumerate(self.far):
            put(0, m, 0, 0, dest)
            put(0, m, 1, 1, dest)
        for m, dest in enumerate(self.near):
            put(1, m, 0, 0, dest)
            put(2, m, 0, 0, dest)
            for turn in range(2):
                put(1, m, 1 + turn, 1 + turn, dest)
                for src, final in self.leave[turn]:
                    if src == dest:
                        put(2, m, 1 + turn, 0, final)
        return table.astype(jnp.bfloat16)

    def arrival_table(self):
        size = self.half * self.UNITS
        table = np.zeros((3, self.count * 2, 3 * size * 2), np.float32)

        def put(kind, angle, source, m, unit):
            for i in range(2):
                table[kind, angle * 2 + i, (source * size + m * self.UNITS + unit) * 2 + i] = 1.0

        for m, angle in enumerate(self.near):
            put(0, angle, 0, m, 0)
            for turn in range(2):
                for src, dst in self.enter[turn]:
                    if dst == angle:
                        put(0, src, 0, m, 1 + turn)
                if angle not in self.relays:
                    put(1 + turn, angle, 1 + turn, m, 1 + turn)
        for m, angle in enumerate(self.far):
            for turn in range(2):
                put(1 + turn, angle, 0, m, 0)
                for src, dst in self.enter[0]:
                    if dst == angle:
                        put(1 + turn, src, 0, m, 1)
        return table.astype(jnp.bfloat16)

    @classmethod
    def kinds(cls, device, count):
        step = device // (count // cls.AROUND)
        turned = lax.rem(step + 4, cls.AROUND)
        far = turned >= 8
        other = (turned >= 1) & (turned <= 4)
        return jnp.where(far, 0, jnp.where(other, 2, 1)), jnp.where(far, 1 + (step + step // 8) % 2, 0)


def repack_kernel(lines_ref, first_ref, second_ref, table_ref, out_ref):
    kind, _ = Routes.kinds(lax.axis_index("ang"), lax.axis_size("ang"))
    lines = jnp.concatenate((lines_ref[...], first_ref[...], second_ref[...]), axis=0)
    out = jnp.dot(table_ref[kind], lines, preferred_element_type=jnp.float32)
    out_ref[...] = out.astype(out_ref.dtype)


def pixels_kernel(near_ref, first_ref, second_ref, table_ref, weights_ref, out_ref, lines, *, angles):
    _, kind = Routes.kinds(lax.axis_index("ang"), lax.axis_size("ang"))
    held = jnp.concatenate((near_ref[...], first_ref[...], second_ref[...]), axis=0)
    lines[...] = jnp.dot(table_ref[kind], held, preferred_element_type=jnp.float32)
    cut = lines.shape[0] * LANES // SUB // angles
    per = LANES // cut
    row = lax.broadcasted_iota(jnp.int32, (SUB, LANES), 0)
    lane = lax.broadcasted_iota(jnp.int32, (SUB, LANES), 1)
    turn = (lane // cut + per - row % per) % per
    parts = []
    for group in range(angles // per):
        spread = []
        for q in range(per):
            at = (group * per + q) * (SUB // per)
            low = jnp.broadcast_to(lines[at : at + 1, :], (SUB, LANES))
            high = jnp.broadcast_to(lines[at + 1 : at + 2, :], (SUB, LANES))
            spread.append(jnp.where(row < per, low, high))
        part = None
        for shift in range(per):
            mixed = spread[shift]
            for j in range(1, per):
                mixed = jnp.where(row % per == j, spread[(j + shift) % per], mixed)
            if shift > 0:
                mixed = pltpu.roll(mixed, shift * cut, axis=1)
            part = mixed if shift == 0 else jnp.where(turn == shift, mixed, part)
        parts.append(part.astype(jnp.bfloat16))
    out_ref[...] = jnp.dot(jnp.concatenate(parts, axis=1), weights_ref[...], preferred_element_type=jnp.float32)


def in_hbm(array):
    return pltpu.with_memory_space_constraint(array, pltpu.HBM)


def make_contrast(projections, flats):
    shape = flats.shape
    edge = jax.ShapeDtypeStruct((HALO, shape[1]), halo_type)
    return pl.pallas_call(
        contrast_kernel,
        out_shape=(jax.ShapeDtypeStruct(shape, jnp.float32), edge, edge),
        in_specs=[HBM] * 2,
        out_specs=(VMEM,) * 3,
        scratch_shapes=[
            pltpu.VMEM(projections.shape, projections.dtype),
            pltpu.VMEM(flats.shape, flats.dtype),
            pltpu.SemaphoreType.DMA((2,)),
        ],
        compiler_params=PARAMS,
        name="contrast",
    )(in_hbm(projections), in_hbm(flats))


def make_own(own, turns, forward, inverse, gains, starts):
    groups = turns.shape[1]
    return pl.pallas_call(
        own_kernel,
        out_shape=(
            jax.ShapeDtypeStruct((groups * SUB, 2 * LANES), jnp.float32),
            jax.ShapeDtypeStruct(forward.shape, forward.dtype),
            jax.ShapeDtypeStruct(inverse.shape, inverse.dtype),
            jax.ShapeDtypeStruct((SUB, groups, SUB, LANES), jnp.float32),
            pltpu.SMEM((1, starts.shape[1]), jnp.int32),
        ),
        in_specs=[VMEM] * 3 + [HBM] * 3,
        out_specs=(VMEM,) * 4 + (SMEM,),
        scratch_shapes=[pltpu.SemaphoreType.DMA((3,))],
        compiler_params=PARAMS,
        name="own_rows",
    )(own, turns, gains, in_hbm(forward), in_hbm(inverse), in_hbm(starts))


def make_tile(own_spec, below, above, starts, turns, forward, inverse, gains, cut):
    regions = starts.shape[1]
    return pl.pallas_call(
        tile_kernel,
        out_shape=jax.ShapeDtypeStruct((regions * SUB * cut // LANES, LANES), jnp.bfloat16),
        in_specs=[VMEM] * 3 + [SMEM] + [VMEM] * 4,
        out_specs=VMEM,
        scratch_shapes=[
            pltpu.VMEM((above.shape[1] // LANES + 1, SUB, LANES), jnp.float32),
        ],
        compiler_params=PARAMS,
        name="tile",
    )(own_spec, below, above, starts, turns, forward, inverse, gains)


def make_repack(lines, first, second, table):
    return pl.pallas_call(
        repack_kernel,
        out_shape=jax.ShapeDtypeStruct((table.shape[1], LANES), lines.dtype),
        in_specs=[VMEM] * 4,
        out_specs=VMEM,
        compiler_params=PARAMS,
        name="repack",
    )(lines, first, second, table)


def make_pixels(near, first, second, table, weights):
    angles, cut, pixels = weights.shape
    return pl.pallas_call(
        partial(pixels_kernel, angles=angles),
        out_shape=jax.ShapeDtypeStruct((SUB, pixels), jnp.float32),
        in_specs=[VMEM] * 5,
        out_specs=VMEM,
        scratch_shapes=[pltpu.VMEM((table.shape[1], LANES), jnp.float32)],
        compiler_params=PARAMS,
        name="pixels",
    )(near, first, second, table, weights.reshape(angles * cut, pixels))


def body(projections, flats, block_start, bp_weights):
    angles_dev, rows_dev, width = projections.shape
    cut = bp_weights.shape[1]
    assert angles_dev == 1 and rows_dev == SUB and width % (2 * LANES) == 0 and SUB * cut == 2 * LANES
    rows = lax.axis_size("row")
    up = [(i, i + 1) for i in range(rows - 1)]
    down = [(j, i) for i, j in up]
    turns, forward, inverse, gains = (jnp.asarray(t) for t in tables(width, rows_dev + 2 * HALO))
    own, first, last = make_contrast(projections, flats)
    below = lax.ppermute(first, "row", down)
    above = lax.ppermute(last, "row", up)
    own_spec, forward, inverse, gains, starts = make_own(own, turns, forward, inverse, gains, block_start)
    outgoing = make_tile(own_spec, below, above, starts, turns, forward, inverse, gains, cut)
    routes = Routes(lax.axis_size("ang"))
    entered = [lax.ppermute(outgoing, "ang", pairs) for pairs in routes.enter]
    packed = make_repack(outgoing, *entered, jnp.asarray(routes.exchange_table()))
    near = lax.all_to_all(
        packed, "ang", split_axis=0, concat_axis=0, tiled=True, axis_index_groups=[routes.near, routes.far]
    )
    left = [lax.ppermute(near, "ang", pairs) for pairs in routes.leave]
    return make_pixels(near, *left, jnp.asarray(routes.arrival_table()), bp_weights)


def solution(mesh):
    placed = (P(("scan", "ang"), "row", None), P(("scan", "row"), None), P(), P(None, None, "ang"))
    return jax.shard_map(
        body, mesh=mesh, in_specs=placed, out_specs=P(("scan", "row"), "ang"), check_vma=False
    )
```

```python
from functools import partial

import jax
import jax.numpy as jnp
import numpy as np
from jax import lax
from jax.experimental import pallas as pl
from jax.experimental.pallas import tpu as pltpu
from jax.sharding import PartitionSpec as P

HALO = 4
LANES = 128
SUB = 8

paganin_beta = 8.0
ramp_gain = 320.0
halo_type = jnp.float32
VMEM = pl.BlockSpec(memory_space=pltpu.VMEM)
SMEM = pl.BlockSpec(memory_space=pltpu.SMEM)
HBM = pl.BlockSpec(memory_space=pltpu.HBM)
PARAMS = pltpu.CompilerParams(vmem_limit_bytes=8 * 2**20)


def tables(width, tile_rows):
    blocks = width // LANES
    half = blocks // 2
    lane = np.arange(LANES)
    ks = np.arange(half + 1)
    turn = 2.0 * np.pi / width * (ks[:, None] * lane[None, :])
    turns = np.stack((np.cos(turn), np.sin(turn))).astype(np.float32)
    angle = 2.0 * np.pi / LANES * (lane[:, None] * lane[None, :] % LANES)
    cos, sin = np.cos(angle), np.sin(angle)
    forward = np.block([[cos, -sin], [sin, cos]])

    def split(matrix):
        high = matrix.astype(jnp.bfloat16)
        low = (matrix - high.astype(np.float64)).astype(jnp.bfloat16)
        return np.stack((high, low))

    freq = (ks[:, None] + blocks * lane[None, :]).astype(np.float64)
    row = np.arange(tile_rows, dtype=np.float64)
    lam = 4.0 * np.sin(np.pi * row / tile_rows)[:, None, None] ** 2 + 4.0 * np.sin(np.pi * freq / width) ** 2
    filt = 1.0 / (1.0 + paganin_beta * lam)
    dist = np.arange(tile_rows // 2 + 1)
    gains = np.einsum("du,ukm->dkm", np.cos(2.0 * np.pi / tile_rows * dist[:, None] * row), filt) / tile_rows
    folded = np.minimum(freq, width - freq)
    ramp = ramp_gain * (folded / width) * (0.5 + 0.5 * np.cos(2.0 * np.pi * folded / width))
    twice = np.where((ks == 0) | (ks == half), 1.0, 2.0)
    gains = gains * (ramp * twice[:, None] / width)
    return turns, split(forward), split(forward.T), gains.astype(np.float32)


def plus(terms):
    return sum(terms[1:], terms[0])


def scaled(terms, weights):
    out = None
    for term, weight in zip(terms, weights):
        weight = float(weight)
        if abs(weight) < 1e-12:
            continue
        piece = term if weight == 1.0 else -term if weight == -1.0 else term * weight
        out = piece if out is None else out + piece
    return out


def cosine_sums(terms, blocks):
    half = blocks // 2
    out = [None] * (half + 1)
    for k in range(half // 2 + 1):
        wave = [np.round(np.cos(2.0 * np.pi * a * k / blocks), 15) for a in range(half + 1)]
        even = scaled(terms[0::2], wave[0::2])
        odd = scaled(terms[1::2], wave[1::2])
        out[k] = even if odd is None else even + odd
        if half - k != k:
            out[half - k] = even if odd is None else even - odd
    return out


def sine_sums(terms, blocks):
    half = blocks // 2
    out = [None] * (half + 1)
    for k in range(1, half // 2 + 1):
        wave = [np.round(np.sin(2.0 * np.pi * a * k / blocks), 15) for a in range(half)]
        even = scaled(terms[2:half:2], wave[2::2])
        odd = scaled(terms[1:half:2], wave[1::2])
        if half - k != k:
            out[k] = plus([x for x in (even, odd) if x is not None])
            out[half - k] = odd - even if even is not None else odd
        else:
            out[k] = plus([x for x in (even, odd) if x is not None])
    return out


def accurate_dot(values, matrix_ref):
    high = values.astype(jnp.bfloat16)
    low = (values - high.astype(jnp.float32)).astype(jnp.bfloat16)
    dot = partial(jnp.dot, preferred_element_type=jnp.float32)
    lines = values.shape[0]
    both = dot(jnp.concatenate((high, low), axis=0), matrix_ref[0])
    return both[:lines] + (both[lines:] + dot(high, matrix_ref[1]))


def spectrum(chunks, turns_ref, forward_ref):
    blocks = len(chunks)
    half = blocks // 2
    folds = [chunks[0]] + [chunks[a] + chunks[blocks - a] for a in range(1, half)] + [chunks[half]]
    skews = [None] + [chunks[a] - chunks[blocks - a] for a in range(1, half)] + [None]
    reals = cosine_sums(folds, blocks)
    imags = sine_sums(skews, blocks)
    parts = []
    for k in range(half + 1):
        cos, sin = turns_ref[0, k : k + 1, :], turns_ref[1, k : k + 1, :]
        if k == 0:
            re, im = reals[0], jnp.zeros_like(reals[0])
        elif imags[k] is None:
            re, im = reals[k] * cos, -(reals[k] * sin)
        else:
            re, im = reals[k] * cos - imags[k] * sin, -(imags[k] * cos) - reals[k] * sin
        parts.append(jnp.concatenate((re, im), axis=1))
    return accurate_dot(jnp.concatenate(parts, axis=0), forward_ref)


def columns(spec, turns_ref, inverse_ref, blocks):
    half = blocks // 2
    back = accurate_dot(spec, inverse_ref)
    reals, imags = [], []
    for k in range(half + 1):
        rows = slice(k * SUB, (k + 1) * SUB)
        re, im = back[rows, :LANES], back[rows, LANES:]
        cos, sin = turns_ref[0, k : k + 1, :], turns_ref[1, k : k + 1, :]
        if k == 0:
            reals.append(re)
            imags.append(None)
        else:
            reals.append(re * cos - im * sin)
            imags.append(im * cos + re * sin if k < half else None)
    even = cosine_sums(reals, blocks)
    odd = sine_sums(imags, blocks)
    out = [None] * blocks
    out[0], out[half] = even[0], even[half]
    for a in range(1, half):
        out[a] = even[a] - odd[a]
        out[blocks - a] = even[a] + odd[a]
    return out


def contrast_kernel(proj_hbm, flat_hbm, own_ref, first_ref, last_ref, proj, flat, sems):
    copies = [
        pltpu.make_async_copy(proj_hbm, proj, sems.at[0]),
        pltpu.make_async_copy(flat_hbm, flat, sems.at[1]),
    ]
    for copy in copies:
        copy.start()
    for copy in copies:
        copy.wait()
    own = 1.0 - proj[0].astype(jnp.float32) / flat[...]
    own_ref[...] = own
    first_ref[...] = own[:HALO].astype(first_ref.dtype)
    last_ref[...] = own[SUB - HALO :].astype(last_ref.dtype)


def lanes_of(ref, block):
    return ref[:, block * LANES : (block + 1) * LANES]


def halo_gains(gains_ref, k, row):
    gains = [jnp.broadcast_to(gains_ref[d, k : k + 1, :], (SUB, LANES)) for d in range(2 * HALO + 1)]
    for s in range(SUB):
        far = gains[2 * HALO - abs(s - HALO)]
        near = gains[abs(s - HALO)]
        if s < HALO:
            yield s, jnp.where(row >= s + HALO, near, far)
        else:
            yield s, jnp.where(row < s - HALO, near, far)


def own_kernel(
    own_ref, turns_ref, gains_ref, forward_hbm, inverse_hbm, starts_hbm,
    out_ref, forward_ref, inverse_ref, halo_ref, starts_ref, sems
):
    forward_copy = pltpu.make_async_copy(forward_hbm, forward_ref, sems.at[0])
    inverse_copy = pltpu.make_async_copy(inverse_hbm, inverse_ref, sems.at[1])
    starts_copy = pltpu.make_async_copy(starts_hbm.at[pl.ds(lax.axis_index("ang"), 1)], starts_ref, sems.at[2])
    forward_copy.start()
    inverse_copy.start()
    starts_copy.start()
    row = lax.broadcasted_iota(jnp.int32, (SUB, LANES), 0)
    for k in range(gains_ref.shape[1]):
        for s, gain in halo_gains(gains_ref, k, row):
            halo_ref[s, k] = gain
    forward_copy.wait()
    blocks = own_ref.shape[1] // LANES
    spec = spectrum([lanes_of(own_ref, a) for a in range(blocks)], turns_ref, forward_ref)
    for k in range(blocks // 2 + 1):
        rows = slice(k * SUB, (k + 1) * SUB)
        for side in (slice(0, LANES), slice(LANES, 2 * LANES)):
            here = spec[rows, side]
            moved = [here] + [pltpu.roll(here, s, axis=0) for s in range(1, SUB)]
            total = here * gains_ref[0, k : k + 1, :]
            for d in range(1, SUB):
                pair = jnp.where(row >= d, moved[d], 0.0) + jnp.where(row < SUB - d, moved[SUB - d], 0.0)
                total += pair * gains_ref[d, k : k + 1, :]
            out_ref[rows, side] = total
    inverse_copy.wait()
    starts_copy.wait()


def tile_kernel(
    own_ref, below_ref, above_ref, starts, turns_ref, forward_ref, inverse_ref, gains_ref, out_ref,
    sheet
):
    blocks = above_ref.shape[1] // LANES
    halo = [
        jnp.concatenate((lanes_of(above_ref, a), lanes_of(below_ref, a)), axis=0).astype(jnp.float32)
        for a in range(blocks)
    ]
    spec = spectrum(halo, turns_ref, forward_ref)
    row = lax.broadcasted_iota(jnp.int32, (SUB, LANES), 0)
    lane = lax.broadcasted_iota(jnp.int32, (SUB, LANES), 1)
    parts = []
    for k in range(blocks // 2 + 1):
        rows = slice(k * SUB, (k + 1) * SUB)
        both = []
        for side in (slice(0, LANES), slice(LANES, 2 * LANES)):
            here = spec[rows, side]
            total = own_ref[rows, side] + here * gains_ref[0, k]
            for s in range(1, SUB):
                total += pltpu.roll(here, s, axis=0) * gains_ref[s, k]
            both.append(total)
        parts.append(jnp.concatenate(both, axis=1))
    filtered = columns(jnp.concatenate(parts, axis=0), turns_ref, inverse_ref, blocks)
    for a in range(blocks):
        sheet[a] = filtered[a]
    regions = starts.shape[1]
    cut = out_ref.shape[0] * LANES // (regions * SUB)
    per = LANES // cut
    keep = lane // cut == row % per
    packed = []
    for group in range(regions // per):
        gathered = None
        for q in range(per):
            start = starts[0, group * per + q]
            block = lax.shift_right_logical(start, 7)
            offset = start & (LANES - 1)
            window = jnp.where(lane >= offset, sheet[block], sheet[block + 1])
            window = pltpu.roll(window, (LANES + q * cut - offset) & (LANES - 1), axis=1)
            gathered = window if q == 0 else jnp.where(lane // cut == q, window, gathered)
        for shift in range(per):
            moved = gathered if shift == 0 else pltpu.roll(gathered, shift * cut, axis=1)
            packed.append(jnp.where(keep, moved, 0.0).astype(jnp.bfloat16))
    lines = out_ref.shape[0]
    want = lax.broadcasted_iota(jnp.int32, (lines, regions * SUB), 0)
    have = lax.broadcasted_iota(jnp.int32, (lines, regions * SUB), 1)
    have_row, have_shift, have_group = have % SUB, have // SUB % per, have // (SUB * per)
    have_region = have_group * per + (have_row % per + per - have_shift) % per
    pick = jnp.where(have_region * (SUB // per) + have_row // per == want, 1.0, 0.0).astype(jnp.bfloat16)
    out = jnp.dot(pick, jnp.concatenate(packed, axis=0), preferred_element_type=jnp.float32)
    out_ref[...] = out.astype(jnp.bfloat16)


class Routes:
    UNITS = 4
    AROUND = 16

    def __init__(self, count):
        step = count // self.AROUND
        devices = lambda steps: [s * step + c for s in steps for c in range(step)]
        link = lambda pairs: [p for src, dst in pairs for p in zip(devices([src]), devices([dst]))]
        self.count, self.half = count, count // 2
        self.near = devices((12, 13, 14, 15, 0, 1, 2, 3))
        self.far = devices(range(4, 12))
        self.relays = devices((12, 1, 2, 3))
        first = link(((11, 12), (4, 3), (5, 2), (6, 1)))
        self.enter = [first + [(dst, src) for src, dst in first], link(((10, 12), (9, 3), (8, 2), (7, 1)))]
        self.leave = [link(((12, 11), (13, 9), (14, 7), (3, 4))), link(((12, 10), (13, 8), (14, 6), (3, 5)))]

    def exchange_table(self):
        table = np.zeros((3, self.half * self.UNITS * 2, 3 * self.count * 2), np.float32)

        def put(kind, m, unit, source, region):
            for i in range(2):
                table[kind, (m * self.UNITS + unit) * 2 + i, (source * self.count + region) * 2 + i] = 1.0

        for m, dest in enumerate(self.far):
            put(0, m, 0, 0, dest)
            put(0, m, 1, 1, dest)
        for m, dest in enumerate(self.near):
            put(1, m, 0, 0, dest)
            put(2, m, 0, 0, dest)
            for turn in range(2):
                put(1, m, 1 + turn, 1 + turn, dest)
                for src, final in self.leave[turn]:
                    if src == dest:
                        put(2, m, 1 + turn, 0, final)
        return table.astype(jnp.bfloat16)

    def arrival_table(self):
        size = self.half * self.UNITS
        table = np.zeros((3, self.count * 2, 3 * size * 2), np.float32)

        def put(kind, angle, source, m, unit):
            for i in range(2):
                table[kind, angle * 2 + i, (source * size + m * self.UNITS + unit) * 2 + i] = 1.0

        for m, angle in enumerate(self.near):
            put(0, angle, 0, m, 0)
            for turn in range(2):
                for src, dst in self.enter[turn]:
                    if dst == angle:
                        put(0, src, 0, m, 1 + turn)
                if angle not in self.relays:
                    put(1 + turn, angle, 1 + turn, m, 1 + turn)
        for m, angle in enumerate(self.far):
            for turn in range(2):
                put(1 + turn, angle, 0, m, 0)
                for src, dst in self.enter[0]:
                    if dst == angle:
                        put(1 + turn, src, 0, m, 1)
        return table.astype(jnp.bfloat16)

    @classmethod
    def kinds(cls, device, count):
        step = device // (count // cls.AROUND)
        turned = lax.rem(step + 4, cls.AROUND)
        far = turned >= 8
        other = (turned >= 1) & (turned <= 4)
        early = (step == 4) | ((step > 6) & (step % 2 == 1))
        return jnp.where(far, 0, jnp.where(other, 2, 1)), jnp.where(far, jnp.where(early, 1, 2), 0)


def repack_kernel(lines_ref, first_ref, second_ref, table_ref, out_ref):
    kind, _ = Routes.kinds(lax.axis_index("ang"), lax.axis_size("ang"))
    lines = jnp.concatenate((lines_ref[...], first_ref[...], second_ref[...]), axis=0)
    out = jnp.dot(table_ref[kind], lines, preferred_element_type=jnp.float32)
    out_ref[...] = out.astype(out_ref.dtype)


def pixels_kernel(near_ref, first_ref, second_ref, table_ref, weights_ref, out_ref, lines, *, angles):
    _, kind = Routes.kinds(lax.axis_index("ang"), lax.axis_size("ang"))
    held = jnp.concatenate((near_ref[...], first_ref[...], second_ref[...]), axis=0)
    lines[...] = jnp.dot(table_ref[kind], held, preferred_element_type=jnp.float32)
    cut = lines.shape[0] * LANES // SUB // angles
    per = LANES // cut
    row = lax.broadcasted_iota(jnp.int32, (SUB, LANES), 0)
    lane = lax.broadcasted_iota(jnp.int32, (SUB, LANES), 1)
    turn = (lane // cut + per - row % per) % per
    parts = []
    for group in range(angles // per):
        spread = []
        for q in range(per):
            at = (group * per + q) * (SUB // per)
            low = jnp.broadcast_to(lines[at : at + 1, :], (SUB, LANES))
            high = jnp.broadcast_to(lines[at + 1 : at + 2, :], (SUB, LANES))
            spread.append(jnp.where(row < per, low, high))
        part = None
        for shift in range(per):
            mixed = spread[shift]
            for j in range(1, per):
                mixed = jnp.where(row % per == j, spread[(j + shift) % per], mixed)
            if shift > 0:
                mixed = pltpu.roll(mixed, shift * cut, axis=1)
            part = mixed if shift == 0 else jnp.where(turn == shift, mixed, part)
        parts.append(part.astype(jnp.bfloat16))
    out_ref[...] = jnp.dot(jnp.concatenate(parts, axis=1), weights_ref[...], preferred_element_type=jnp.float32)


def in_hbm(array):
    return pltpu.with_memory_space_constraint(array, pltpu.HBM)


def make_contrast(projections, flats):
    shape = flats.shape
    edge = jax.ShapeDtypeStruct((HALO, shape[1]), halo_type)
    return pl.pallas_call(
        contrast_kernel,
        out_shape=(jax.ShapeDtypeStruct(shape, jnp.float32), edge, edge),
        in_specs=[HBM] * 2,
        out_specs=(VMEM,) * 3,
        scratch_shapes=[
            pltpu.VMEM(projections.shape, projections.dtype),
            pltpu.VMEM(flats.shape, flats.dtype),
            pltpu.SemaphoreType.DMA((2,)),
        ],
        compiler_params=PARAMS,
        name="contrast",
    )(in_hbm(projections), in_hbm(flats))


def make_own(own, turns, forward, inverse, gains, starts):
    groups = turns.shape[1]
    return pl.pallas_call(
        own_kernel,
        out_shape=(
            jax.ShapeDtypeStruct((groups * SUB, 2 * LANES), jnp.float32),
            jax.ShapeDtypeStruct(forward.shape, forward.dtype),
            jax.ShapeDtypeStruct(inverse.shape, inverse.dtype),
            jax.ShapeDtypeStruct((SUB, groups, SUB, LANES), jnp.float32),
            pltpu.SMEM((1, starts.shape[1]), jnp.int32),
        ),
        in_specs=[VMEM] * 3 + [HBM] * 3,
        out_specs=(VMEM,) * 4 + (SMEM,),
        scratch_shapes=[pltpu.SemaphoreType.DMA((3,))],
        compiler_params=PARAMS,
        name="own_rows",
    )(own, turns, gains, in_hbm(forward), in_hbm(inverse), in_hbm(starts))


def make_tile(own_spec, below, above, starts, turns, forward, inverse, gains, cut):
    regions = starts.shape[1]
    return pl.pallas_call(
        tile_kernel,
        out_shape=jax.ShapeDtypeStruct((regions * SUB * cut // LANES, LANES), jnp.bfloat16),
        in_specs=[VMEM] * 3 + [SMEM] + [VMEM] * 4,
        out_specs=VMEM,
        scratch_shapes=[
            pltpu.VMEM((above.shape[1] // LANES + 1, SUB, LANES), jnp.float32),
        ],
        compiler_params=PARAMS,
        name="tile",
    )(own_spec, below, above, starts, turns, forward, inverse, gains)


def make_repack(lines, first, second, table):
    return pl.pallas_call(
        repack_kernel,
        out_shape=jax.ShapeDtypeStruct((table.shape[1], LANES), lines.dtype),
        in_specs=[VMEM] * 4,
        out_specs=VMEM,
        compiler_params=PARAMS,
        name="repack",
    )(lines, first, second, table)


def make_pixels(near, first, second, table, weights):
    angles, cut, pixels = weights.shape
    return pl.pallas_call(
        partial(pixels_kernel, angles=angles),
        out_shape=jax.ShapeDtypeStruct((SUB, pixels), jnp.float32),
        in_specs=[VMEM] * 5,
        out_specs=VMEM,
        scratch_shapes=[pltpu.VMEM((table.shape[1], LANES), jnp.float32)],
        compiler_params=PARAMS,
        name="pixels",
    )(near, first, second, table, weights.reshape(angles * cut, pixels))


def body(projections, flats, block_start, bp_weights):
    angles_dev, rows_dev, width = projections.shape
    cut = bp_weights.shape[1]
    assert angles_dev == 1 and rows_dev == SUB and width % (2 * LANES) == 0 and SUB * cut == 2 * LANES
    rows = lax.axis_size("row")
    up = [(i, i + 1) for i in range(rows - 1)]
    down = [(j, i) for i, j in up]
    turns, forward, inverse, gains = (jnp.asarray(t) for t in tables(width, rows_dev + 2 * HALO))
    own, first, last = make_contrast(projections, flats)
    below = lax.ppermute(first, "row", down)
    above = lax.ppermute(last, "row", up)
    own_spec, forward, inverse, gains, starts = make_own(own, turns, forward, inverse, gains, block_start)
    outgoing = make_tile(own_spec, below, above, starts, turns, forward, inverse, gains, cut)
    routes = Routes(lax.axis_size("ang"))
    entered = [lax.ppermute(outgoing, "ang", pairs) for pairs in routes.enter]
    packed = make_repack(outgoing, *entered, jnp.asarray(routes.exchange_table()))
    near = lax.all_to_all(
        packed, "ang", split_axis=0, concat_axis=0, tiled=True, axis_index_groups=[routes.near, routes.far]
    )
    left = [lax.ppermute(near, "ang", pairs) for pairs in routes.leave]
    return make_pixels(near, *left, jnp.asarray(routes.arrival_table()), bp_weights)


def solution(mesh):
    placed = (P(("scan", "ang"), "row", None), P(("scan", "row"), None), P(), P(None, None, "ang"))
    return jax.shard_map(
        body, mesh=mesh, in_specs=placed, out_specs=P(("scan", "row"), "ang"), check_vma=False
    )
```

```python
from functools import partial

import jax
import jax.numpy as jnp
import numpy as np
from jax import lax
from jax.experimental import pallas as pl
from jax.experimental.pallas import tpu as pltpu
from jax.sharding import PartitionSpec as P

HALO = 4
LANES = 128
SUB = 8

paganin_beta = 8.0
ramp_gain = 320.0
halo_type = jnp.float32
VMEM = pl.BlockSpec(memory_space=pltpu.VMEM)
SMEM = pl.BlockSpec(memory_space=pltpu.SMEM)
HBM = pl.BlockSpec(memory_space=pltpu.HBM)
PARAMS = pltpu.CompilerParams(vmem_limit_bytes=8 * 2**20)


def tables(width, tile_rows):
    blocks = width // LANES
    half = blocks // 2
    lane = np.arange(LANES)
    ks = np.arange(half + 1)
    turn = 2.0 * np.pi / width * (ks[:, None] * lane[None, :])
    turns = np.stack((np.cos(turn), np.sin(turn))).astype(np.float32)
    angle = 2.0 * np.pi / LANES * (lane[:, None] * lane[None, :] % LANES)
    cos, sin = np.cos(angle), np.sin(angle)
    forward = np.block([[cos, -sin], [sin, cos]])

    def split(matrix):
        high = matrix.astype(jnp.bfloat16)
        low = (matrix - high.astype(np.float64)).astype(jnp.bfloat16)
        return np.stack((high, low))

    freq = (ks[:, None] + blocks * lane[None, :]).astype(np.float64)
    row = np.arange(tile_rows, dtype=np.float64)
    lam = 4.0 * np.sin(np.pi * row / tile_rows)[:, None, None] ** 2 + 4.0 * np.sin(np.pi * freq / width) ** 2
    filt = 1.0 / (1.0 + paganin_beta * lam)
    dist = np.arange(tile_rows // 2 + 1)
    gains = np.einsum("du,ukm->dkm", np.cos(2.0 * np.pi / tile_rows * dist[:, None] * row), filt) / tile_rows
    folded = np.minimum(freq, width - freq)
    ramp = ramp_gain * (folded / width) * (0.5 + 0.5 * np.cos(2.0 * np.pi * folded / width))
    twice = np.where((ks == 0) | (ks == half), 1.0, 2.0)
    gains = gains * (ramp * twice[:, None] / width)
    return turns, split(forward), split(forward.T), gains.astype(np.float32)


def plus(terms):
    return sum(terms[1:], terms[0])


def scaled(terms, weights):
    out = None
    for term, weight in zip(terms, weights):
        weight = float(weight)
        if abs(weight) < 1e-12:
            continue
        piece = term if weight == 1.0 else -term if weight == -1.0 else term * weight
        out = piece if out is None else out + piece
    return out


def cosine_sums(terms, blocks):
    half = blocks // 2
    out = [None] * (half + 1)
    for k in range(half // 2 + 1):
        wave = [np.round(np.cos(2.0 * np.pi * a * k / blocks), 15) for a in range(half + 1)]
        even = scaled(terms[0::2], wave[0::2])
        odd = scaled(terms[1::2], wave[1::2])
        out[k] = even if odd is None else even + odd
        if half - k != k:
            out[half - k] = even if odd is None else even - odd
    return out


def sine_sums(terms, blocks):
    half = blocks // 2
    out = [None] * (half + 1)
    for k in range(1, half // 2 + 1):
        wave = [np.round(np.sin(2.0 * np.pi * a * k / blocks), 15) for a in range(half)]
        even = scaled(terms[2:half:2], wave[2::2])
        odd = scaled(terms[1:half:2], wave[1::2])
        if half - k != k:
            out[k] = plus([x for x in (even, odd) if x is not None])
            out[half - k] = odd - even if even is not None else odd
        else:
            out[k] = plus([x for x in (even, odd) if x is not None])
    return out


def accurate_dot(values, matrix_ref):
    high = values.astype(jnp.bfloat16)
    low = (values - high.astype(jnp.float32)).astype(jnp.bfloat16)
    dot = partial(jnp.dot, preferred_element_type=jnp.float32)
    lines = values.shape[0]
    both = dot(jnp.concatenate((high, low), axis=0), matrix_ref[0])
    return both[:lines] + (both[lines:] + dot(high, matrix_ref[1]))


def spectrum(chunks, turns_ref, forward_ref):
    blocks = len(chunks)
    half = blocks // 2
    folds = [chunks[0]] + [chunks[a] + chunks[blocks - a] for a in range(1, half)] + [chunks[half]]
    skews = [None] + [chunks[a] - chunks[blocks - a] for a in range(1, half)] + [None]
    reals = cosine_sums(folds, blocks)
    imags = sine_sums(skews, blocks)
    parts = []
    for k in range(half + 1):
        cos, sin = turns_ref[0, k : k + 1, :], turns_ref[1, k : k + 1, :]
        if k == 0:
            re, im = reals[0], jnp.zeros_like(reals[0])
        elif imags[k] is None:
            re, im = reals[k] * cos, -(reals[k] * sin)
        else:
            re, im = reals[k] * cos - imags[k] * sin, -(imags[k] * cos) - reals[k] * sin
        parts.append(jnp.concatenate((re, im), axis=1))
    return accurate_dot(jnp.concatenate(parts, axis=0), forward_ref)


def columns(spec, turns_ref, inverse_ref, blocks):
    half = blocks // 2
    back = accurate_dot(spec, inverse_ref)
    reals, imags = [], []
    for k in range(half + 1):
        rows = slice(k * SUB, (k + 1) * SUB)
        re, im = back[rows, :LANES], back[rows, LANES:]
        cos, sin = turns_ref[0, k : k + 1, :], turns_ref[1, k : k + 1, :]
        if k == 0:
            reals.append(re)
            imags.append(None)
        else:
            reals.append(re * cos - im * sin)
            imags.append(im * cos + re * sin if k < half else None)
    even = cosine_sums(reals, blocks)
    odd = sine_sums(imags, blocks)
    out = [None] * blocks
    out[0], out[half] = even[0], even[half]
    for a in range(1, half):
        out[a] = even[a] - odd[a]
        out[blocks - a] = even[a] + odd[a]
    return out


def contrast_kernel(proj_hbm, flat_hbm, own_ref, first_ref, last_ref, proj, flat, sems):
    copies = [
        pltpu.make_async_copy(proj_hbm, proj, sems.at[0]),
        pltpu.make_async_copy(flat_hbm, flat, sems.at[1]),
    ]
    for copy in copies:
        copy.start()
    for copy in copies:
        copy.wait()
    own = 1.0 - proj[0].astype(jnp.float32) / flat[...]
    own_ref[...] = own
    first_ref[...] = own[:HALO].astype(first_ref.dtype)
    last_ref[...] = own[SUB - HALO :].astype(last_ref.dtype)


def lanes_of(ref, block):
    return ref[:, block * LANES : (block + 1) * LANES]


def halo_gains(gains_ref, k, row):
    gains = [jnp.broadcast_to(gains_ref[d, k : k + 1, :], (SUB, LANES)) for d in range(2 * HALO + 1)]
    for s in range(SUB):
        far = gains[2 * HALO - abs(s - HALO)]
        near = gains[abs(s - HALO)]
        if s < HALO:
            yield s, jnp.where(row >= s + HALO, near, far)
        else:
            yield s, jnp.where(row < s - HALO, near, far)


def own_kernel(
    own_ref, turns_ref, gains_ref, forward_hbm, inverse_hbm, starts_hbm,
    out_ref, forward_ref, inverse_ref, halo_ref, starts_ref, sems
):
    forward_copy = pltpu.make_async_copy(forward_hbm, forward_ref, sems.at[0])
    inverse_copy = pltpu.make_async_copy(inverse_hbm, inverse_ref, sems.at[1])
    starts_copy = pltpu.make_async_copy(starts_hbm.at[pl.ds(lax.axis_index("ang"), 1)], starts_ref, sems.at[2])
    forward_copy.start()
    inverse_copy.start()
    starts_copy.start()
    row = lax.broadcasted_iota(jnp.int32, (SUB, LANES), 0)
    for k in range(gains_ref.shape[1]):
        for s, gain in halo_gains(gains_ref, k, row):
            halo_ref[s, k] = gain
    forward_copy.wait()
    blocks = own_ref.shape[1] // LANES
    spec = spectrum([lanes_of(own_ref, a) for a in range(blocks)], turns_ref, forward_ref)
    for k in range(blocks // 2 + 1):
        rows = slice(k * SUB, (k + 1) * SUB)
        for side in (slice(0, LANES), slice(LANES, 2 * LANES)):
            here = spec[rows, side]
            moved = [here] + [pltpu.roll(here, s, axis=0) for s in range(1, SUB)]
            total = here * gains_ref[0, k : k + 1, :]
            for d in range(1, SUB):
                pair = jnp.where(row >= d, moved[d], 0.0) + jnp.where(row < SUB - d, moved[SUB - d], 0.0)
                total += pair * gains_ref[d, k : k + 1, :]
            out_ref[rows, side] = total
    inverse_copy.wait()
    starts_copy.wait()


def tile_kernel(
    own_ref, below_ref, above_ref, starts, turns_ref, forward_ref, inverse_ref, gains_ref, out_ref,
    sheet
):
    blocks = above_ref.shape[1] // LANES
    halo = [
        jnp.concatenate((lanes_of(above_ref, a), lanes_of(below_ref, a)), axis=0).astype(jnp.float32)
        for a in range(blocks)
    ]
    spec = spectrum(halo, turns_ref, forward_ref)
    row = lax.broadcasted_iota(jnp.int32, (SUB, LANES), 0)
    lane = lax.broadcasted_iota(jnp.int32, (SUB, LANES), 1)
    parts = []
    for k in range(blocks // 2 + 1):
        rows = slice(k * SUB, (k + 1) * SUB)
        both = []
        for side in (slice(0, LANES), slice(LANES, 2 * LANES)):
            here = spec[rows, side]
            total = own_ref[rows, side] + here * gains_ref[0, k]
            for s in range(1, SUB):
                total += pltpu.roll(here, s, axis=0) * gains_ref[s, k]
            both.append(total)
        parts.append(jnp.concatenate(both, axis=1))
    filtered = columns(jnp.concatenate(parts, axis=0), turns_ref, inverse_ref, blocks)
    for a in range(blocks):
        sheet[a] = filtered[a]
    regions = starts.shape[1]
    cut = out_ref.shape[0] * LANES // (regions * SUB)
    per = LANES // cut
    keep = lane // cut == row % per
    packed = []
    for group in range(regions // per):
        gathered = None
        for q in range(per):
            start = starts[0, group * per + q]
            block = lax.shift_right_logical(start, 7)
            offset = start & (LANES - 1)
            window = jnp.where(lane >= offset, sheet[block], sheet[block + 1])
            window = pltpu.roll(window, (LANES + q * cut - offset) & (LANES - 1), axis=1)
            gathered = window if q == 0 else jnp.where(lane // cut == q, window, gathered)
        for shift in range(per):
            moved = gathered if shift == 0 else pltpu.roll(gathered, shift * cut, axis=1)
            packed.append(jnp.where(keep, moved, 0.0).astype(jnp.bfloat16))
    lines = out_ref.shape[0]
    want = lax.broadcasted_iota(jnp.int32, (lines, regions * SUB), 0)
    have = lax.broadcasted_iota(jnp.int32, (lines, regions * SUB), 1)
    have_row, have_shift, have_group = have % SUB, have // SUB % per, have // (SUB * per)
    have_region = have_group * per + (have_row % per + per - have_shift) % per
    pick = jnp.where(have_region * (SUB // per) + have_row // per == want, 1.0, 0.0).astype(jnp.bfloat16)
    out = jnp.dot(pick, jnp.concatenate(packed, axis=0), preferred_element_type=jnp.float32)
    out_ref[...] = out.astype(jnp.bfloat16)


class Routes:
    UNITS = 3
    AROUND = 16

    def __init__(self, count):
        step = count // self.AROUND
        devices = lambda steps: [s * step + c for s in steps for c in range(step)]
        link = lambda pairs: [p for src, dst in pairs for p in zip(devices([src]), devices([dst]))]
        self.count, self.half = count, count // 2
        self.near = devices((12, 13, 14, 15, 0, 1, 2, 3))
        self.far = devices(range(4, 12))
        self.relays = devices((12, 1, 2, 3))
        first = link(((11, 12), (4, 3), (5, 2), (6, 1)))
        self.enter = [first + [(dst, src) for src, dst in first], link(((10, 12), (9, 3), (8, 2), (7, 1)))]
        self.leave = [link(((12, 11), (13, 9), (14, 7), (3, 4))), link(((12, 10), (13, 8), (14, 6), (3, 5)))]

    def exchange_table(self):
        table = np.zeros((3, self.half * self.UNITS * 2, 3 * self.count * 2), np.float32)

        def put(kind, m, unit, source, region):
            for i in range(2):
                table[kind, (m * self.UNITS + unit) * 2 + i, (source * self.count + region) * 2 + i] = 1.0

        for m, dest in enumerate(self.far):
            put(0, m, 0, 0, dest)
            put(0, m, 1, 1, dest)
        for m, dest in enumerate(self.near):
            put(1, m, 0, 0, dest)
            put(2, m, 0, 0, dest)
            for turn in range(2):
                put(1, m, 1 + turn, 1 + turn, dest)
                for src, final in self.leave[turn]:
                    if src == dest:
                        put(2, m, 1 + turn, 0, final)
        return table.astype(jnp.bfloat16)

    def arrival_table(self):
        size = self.half * self.UNITS
        table = np.zeros((3, self.count * 2, 3 * size * 2), np.float32)

        def put(kind, angle, source, m, unit):
            for i in range(2):
                table[kind, angle * 2 + i, (source * size + m * self.UNITS + unit) * 2 + i] = 1.0

        for m, angle in enumerate(self.near):
            put(0, angle, 0, m, 0)
            for turn in range(2):
                for src, dst in self.enter[turn]:
                    if dst == angle:
                        put(0, src, 0, m, 1 + turn)
                if angle not in self.relays:
                    put(1 + turn, angle, 1 + turn, m, 1 + turn)
        for m, angle in enumerate(self.far):
            for turn in range(2):
                put(1 + turn, angle, 0, m, 0)
                for src, dst in self.enter[0]:
                    if dst == angle:
                        put(1 + turn, src, 0, m, 1)
        return table.astype(jnp.bfloat16)

    @classmethod
    def kinds(cls, device, count):
        step = device // (count // cls.AROUND)
        turned = lax.rem(step + 4, cls.AROUND)
        far = turned >= 8
        other = (turned >= 1) & (turned <= 4)
        early = (step == 4) | ((step > 6) & (step % 2 == 1))
        return jnp.where(far, 0, jnp.where(other, 2, 1)), jnp.where(far, jnp.where(early, 1, 2), 0)


def repack_kernel(lines_ref, first_ref, second_ref, table_ref, out_ref):
    kind, _ = Routes.kinds(lax.axis_index("ang"), lax.axis_size("ang"))
    lines = jnp.concatenate((lines_ref[...], first_ref[...], second_ref[...]), axis=0)
    out = jnp.dot(table_ref[kind], lines, preferred_element_type=jnp.float32)
    out_ref[...] = out.astype(out_ref.dtype)


def pixels_kernel(near_ref, first_ref, second_ref, table_ref, weights_ref, out_ref, lines, *, angles):
    _, kind = Routes.kinds(lax.axis_index("ang"), lax.axis_size("ang"))
    held = jnp.concatenate((near_ref[...], first_ref[...], second_ref[...]), axis=0)
    lines[...] = jnp.dot(table_ref[kind], held, preferred_element_type=jnp.float32)
    cut = lines.shape[0] * LANES // SUB // angles
    per = LANES // cut
    row = lax.broadcasted_iota(jnp.int32, (SUB, LANES), 0)
    lane = lax.broadcasted_iota(jnp.int32, (SUB, LANES), 1)
    turn = (lane // cut + per - row % per) % per
    parts = []
    for group in range(angles // per):
        spread = []
        for q in range(per):
            at = (group * per + q) * (SUB // per)
            low = jnp.broadcast_to(lines[at : at + 1, :], (SUB, LANES))
            high = jnp.broadcast_to(lines[at + 1 : at + 2, :], (SUB, LANES))
            spread.append(jnp.where(row < per, low, high))
        part = None
        for shift in range(per):
            mixed = spread[shift]
            for j in range(1, per):
                mixed = jnp.where(row % per == j, spread[(j + shift) % per], mixed)
            if shift > 0:
                mixed = pltpu.roll(mixed, shift * cut, axis=1)
            part = mixed if shift == 0 else jnp.where(turn == shift, mixed, part)
        parts.append(part.astype(jnp.bfloat16))
    out_ref[...] = jnp.dot(jnp.concatenate(parts, axis=1), weights_ref[...], preferred_element_type=jnp.float32)


def in_hbm(array):
    return pltpu.with_memory_space_constraint(array, pltpu.HBM)


def make_contrast(projections, flats):
    shape = flats.shape
    edge = jax.ShapeDtypeStruct((HALO, shape[1]), halo_type)
    return pl.pallas_call(
        contrast_kernel,
        out_shape=(jax.ShapeDtypeStruct(shape, jnp.float32), edge, edge),
        in_specs=[HBM] * 2,
        out_specs=(VMEM,) * 3,
        scratch_shapes=[
            pltpu.VMEM(projections.shape, projections.dtype),
            pltpu.VMEM(flats.shape, flats.dtype),
            pltpu.SemaphoreType.DMA((2,)),
        ],
        compiler_params=PARAMS,
        name="contrast",
    )(in_hbm(projections), in_hbm(flats))


def make_own(own, turns, forward, inverse, gains, starts):
    groups = turns.shape[1]
    return pl.pallas_call(
        own_kernel,
        out_shape=(
            jax.ShapeDtypeStruct((groups * SUB, 2 * LANES), jnp.float32),
            jax.ShapeDtypeStruct(forward.shape, forward.dtype),
            jax.ShapeDtypeStruct(inverse.shape, inverse.dtype),
            jax.ShapeDtypeStruct((SUB, groups, SUB, LANES), jnp.float32),
            pltpu.SMEM((1, starts.shape[1]), jnp.int32),
        ),
        in_specs=[VMEM] * 3 + [HBM] * 3,
        out_specs=(VMEM,) * 4 + (SMEM,),
        scratch_shapes=[pltpu.SemaphoreType.DMA((3,))],
        compiler_params=PARAMS,
        name="own_rows",
    )(own, turns, gains, in_hbm(forward), in_hbm(inverse), in_hbm(starts))


def make_tile(own_spec, below, above, starts, turns, forward, inverse, gains, cut):
    regions = starts.shape[1]
    return pl.pallas_call(
        tile_kernel,
        out_shape=jax.ShapeDtypeStruct((regions * SUB * cut // LANES, LANES), jnp.bfloat16),
        in_specs=[VMEM] * 3 + [SMEM] + [VMEM] * 4,
        out_specs=VMEM,
        scratch_shapes=[
            pltpu.VMEM((above.shape[1] // LANES + 1, SUB, LANES), jnp.float32),
        ],
        compiler_params=PARAMS,
        name="tile",
    )(own_spec, below, above, starts, turns, forward, inverse, gains)


def make_repack(lines, first, second, table):
    return pl.pallas_call(
        repack_kernel,
        out_shape=jax.ShapeDtypeStruct((table.shape[1], LANES), lines.dtype),
        in_specs=[VMEM] * 4,
        out_specs=VMEM,
        compiler_params=PARAMS,
        name="repack",
    )(lines, first, second, table)


def make_pixels(near, first, second, table, weights):
    angles, cut, pixels = weights.shape
    return pl.pallas_call(
        partial(pixels_kernel, angles=angles),
        out_shape=jax.ShapeDtypeStruct((SUB, pixels), jnp.float32),
        in_specs=[VMEM] * 5,
        out_specs=VMEM,
        scratch_shapes=[pltpu.VMEM((table.shape[1], LANES), jnp.float32)],
        compiler_params=PARAMS,
        name="pixels",
    )(near, first, second, table, weights.reshape(angles * cut, pixels))


def body(projections, flats, block_start, bp_weights):
    angles_dev, rows_dev, width = projections.shape
    cut = bp_weights.shape[1]
    assert angles_dev == 1 and rows_dev == SUB and width % (2 * LANES) == 0 and SUB * cut == 2 * LANES
    rows = lax.axis_size("row")
    up = [(i, i + 1) for i in range(rows - 1)]
    down = [(j, i) for i, j in up]
    turns, forward, inverse, gains = (jnp.asarray(t) for t in tables(width, rows_dev + 2 * HALO))
    own, first, last = make_contrast(projections, flats)
    below = lax.ppermute(first, "row", down)
    above = lax.ppermute(last, "row", up)
    own_spec, forward, inverse, gains, starts = make_own(own, turns, forward, inverse, gains, block_start)
    outgoing = make_tile(own_spec, below, above, starts, turns, forward, inverse, gains, cut)
    routes = Routes(lax.axis_size("ang"))
    entered = [lax.ppermute(outgoing, "ang", pairs) for pairs in routes.enter]
    packed = make_repack(outgoing, *entered, jnp.asarray(routes.exchange_table()))
    near = lax.all_to_all(
        packed.reshape(-1, 2, LANES), "ang", split_axis=0, concat_axis=0, tiled=True,
        axis_index_groups=[routes.near, routes.far],
    ).reshape(packed.shape)
    left = [lax.ppermute(near, "ang", pairs) for pairs in routes.leave]
    return make_pixels(near, *left, jnp.asarray(routes.arrival_table()), bp_weights)


def solution(mesh):
    placed = (P(("scan", "ang"), "row", None), P(("scan", "row"), None), P(), P(None, None, "ang"))
    return jax.shard_map(
        body, mesh=mesh, in_specs=placed, out_specs=P(("scan", "row"), "ang"), check_vma=False
    )
```

```python
from functools import partial

import jax
import jax.numpy as jnp
import numpy as np
from jax import lax
from jax.experimental import pallas as pl
from jax.experimental.pallas import tpu as pltpu
from jax.sharding import PartitionSpec as P

HALO = 4
LANES = 128
SUB = 8

paganin_beta = 8.0
ramp_gain = 320.0
halo_type = jnp.float32
VMEM = pl.BlockSpec(memory_space=pltpu.VMEM)
SMEM = pl.BlockSpec(memory_space=pltpu.SMEM)
HBM = pl.BlockSpec(memory_space=pltpu.HBM)
PARAMS = pltpu.CompilerParams(vmem_limit_bytes=8 * 2**20)


def tables(width, tile_rows):
    blocks = width // LANES
    half = blocks // 2
    lane = np.arange(LANES)
    ks = np.arange(half + 1)
    turn = 2.0 * np.pi / width * (ks[:, None] * lane[None, :])
    turns = np.stack((np.cos(turn), np.sin(turn))).astype(np.float32)
    angle = 2.0 * np.pi / LANES * (lane[:, None] * lane[None, :] % LANES)
    cos, sin = np.cos(angle), np.sin(angle)
    forward = np.block([[cos, -sin], [sin, cos]])

    def split(matrix):
        high = matrix.astype(jnp.bfloat16)
        low = (matrix - high.astype(np.float64)).astype(jnp.bfloat16)
        return np.stack((high, low))

    freq = (ks[:, None] + blocks * lane[None, :]).astype(np.float64)
    row = np.arange(tile_rows, dtype=np.float64)
    lam = 4.0 * np.sin(np.pi * row / tile_rows)[:, None, None] ** 2 + 4.0 * np.sin(np.pi * freq / width) ** 2
    filt = 1.0 / (1.0 + paganin_beta * lam)
    dist = np.arange(tile_rows // 2 + 1)
    gains = np.einsum("du,ukm->dkm", np.cos(2.0 * np.pi / tile_rows * dist[:, None] * row), filt) / tile_rows
    folded = np.minimum(freq, width - freq)
    ramp = ramp_gain * (folded / width) * (0.5 + 0.5 * np.cos(2.0 * np.pi * folded / width))
    twice = np.where((ks == 0) | (ks == half), 1.0, 2.0)
    gains = gains * (ramp * twice[:, None] / width)
    return turns, split(forward), split(forward.T), gains.astype(np.float32)


def plus(terms):
    return sum(terms[1:], terms[0])


def scaled(terms, weights):
    out = None
    for term, weight in zip(terms, weights):
        weight = float(weight)
        if abs(weight) < 1e-12:
            continue
        piece = term if weight == 1.0 else -term if weight == -1.0 else term * weight
        out = piece if out is None else out + piece
    return out


def cosine_sums(terms, blocks):
    half = blocks // 2
    out = [None] * (half + 1)
    for k in range(half // 2 + 1):
        wave = [np.round(np.cos(2.0 * np.pi * a * k / blocks), 15) for a in range(half + 1)]
        even = scaled(terms[0::2], wave[0::2])
        odd = scaled(terms[1::2], wave[1::2])
        out[k] = even if odd is None else even + odd
        if half - k != k:
            out[half - k] = even if odd is None else even - odd
    return out


def sine_sums(terms, blocks):
    half = blocks // 2
    out = [None] * (half + 1)
    for k in range(1, half // 2 + 1):
        wave = [np.round(np.sin(2.0 * np.pi * a * k / blocks), 15) for a in range(half)]
        even = scaled(terms[2:half:2], wave[2::2])
        odd = scaled(terms[1:half:2], wave[1::2])
        if half - k != k:
            out[k] = plus([x for x in (even, odd) if x is not None])
            out[half - k] = odd - even if even is not None else odd
        else:
            out[k] = plus([x for x in (even, odd) if x is not None])
    return out


def accurate_dot(values, matrix_ref):
    high = values.astype(jnp.bfloat16)
    low = (values - high.astype(jnp.float32)).astype(jnp.bfloat16)
    dot = partial(jnp.dot, preferred_element_type=jnp.float32)
    lines = values.shape[0]
    both = dot(jnp.concatenate((high, low), axis=0), matrix_ref[0])
    return both[:lines] + (both[lines:] + dot(high, matrix_ref[1]))


def spectrum(chunks, turns_ref, forward_ref):
    blocks = len(chunks)
    half = blocks // 2
    folds = [chunks[0]] + [chunks[a] + chunks[blocks - a] for a in range(1, half)] + [chunks[half]]
    skews = [None] + [chunks[a] - chunks[blocks - a] for a in range(1, half)] + [None]
    reals = cosine_sums(folds, blocks)
    imags = sine_sums(skews, blocks)
    parts = []
    for k in range(half + 1):
        cos, sin = turns_ref[0, k : k + 1, :], turns_ref[1, k : k + 1, :]
        if k == 0:
            re, im = reals[0], jnp.zeros_like(reals[0])
        elif imags[k] is None:
            re, im = reals[k] * cos, -(reals[k] * sin)
        else:
            re, im = reals[k] * cos - imags[k] * sin, -(imags[k] * cos) - reals[k] * sin
        parts.append(jnp.concatenate((re, im), axis=1))
    return accurate_dot(jnp.concatenate(parts, axis=0), forward_ref)


def columns(spec, turns_ref, inverse_ref, blocks):
    half = blocks // 2
    back = accurate_dot(spec, inverse_ref)
    reals, imags = [], []
    for k in range(half + 1):
        rows = slice(k * SUB, (k + 1) * SUB)
        re, im = back[rows, :LANES], back[rows, LANES:]
        cos, sin = turns_ref[0, k : k + 1, :], turns_ref[1, k : k + 1, :]
        if k == 0:
            reals.append(re)
            imags.append(None)
        else:
            reals.append(re * cos - im * sin)
            imags.append(im * cos + re * sin if k < half else None)
    even = cosine_sums(reals, blocks)
    odd = sine_sums(imags, blocks)
    out = [None] * blocks
    out[0], out[half] = even[0], even[half]
    for a in range(1, half):
        out[a] = even[a] - odd[a]
        out[blocks - a] = even[a] + odd[a]
    return out


def contrast_kernel(proj_hbm, flat_hbm, own_ref, first_ref, last_ref, proj, flat, sems):
    copies = [
        pltpu.make_async_copy(proj_hbm, proj, sems.at[0]),
        pltpu.make_async_copy(flat_hbm, flat, sems.at[1]),
    ]
    for copy in copies:
        copy.start()
    for copy in copies:
        copy.wait()
    own = 1.0 - proj[0].astype(jnp.float32) / flat[...]
    own_ref[...] = own
    first_ref[...] = own[:HALO].astype(first_ref.dtype)
    last_ref[...] = own[SUB - HALO :].astype(last_ref.dtype)


def lanes_of(ref, block):
    return ref[:, block * LANES : (block + 1) * LANES]


def halo_gains(gains_ref, k, row):
    gains = [jnp.broadcast_to(gains_ref[d, k : k + 1, :], (SUB, LANES)) for d in range(2 * HALO + 1)]
    for s in range(SUB):
        far = gains[2 * HALO - abs(s - HALO)]
        near = gains[abs(s - HALO)]
        if s < HALO:
            yield s, jnp.where(row >= s + HALO, near, far)
        else:
            yield s, jnp.where(row < s - HALO, near, far)


def own_kernel(
    own_ref, turns_ref, gains_ref, forward_hbm, inverse_hbm, starts_hbm,
    out_ref, forward_ref, inverse_ref, halo_ref, starts_ref, sems
):
    forward_copy = pltpu.make_async_copy(forward_hbm, forward_ref, sems.at[0])
    inverse_copy = pltpu.make_async_copy(inverse_hbm, inverse_ref, sems.at[1])
    starts_copy = pltpu.make_async_copy(starts_hbm.at[pl.ds(lax.axis_index("ang"), 1)], starts_ref, sems.at[2])
    forward_copy.start()
    inverse_copy.start()
    starts_copy.start()
    row = lax.broadcasted_iota(jnp.int32, (SUB, LANES), 0)
    for k in range(gains_ref.shape[1]):
        for s, gain in halo_gains(gains_ref, k, row):
            halo_ref[s, k] = gain
    forward_copy.wait()
    blocks = own_ref.shape[1] // LANES
    spec = spectrum([lanes_of(own_ref, a) for a in range(blocks)], turns_ref, forward_ref)
    for k in range(blocks // 2 + 1):
        rows = slice(k * SUB, (k + 1) * SUB)
        for side in (slice(0, LANES), slice(LANES, 2 * LANES)):
            here = spec[rows, side]
            moved = [here] + [pltpu.roll(here, s, axis=0) for s in range(1, SUB)]
            total = here * gains_ref[0, k : k + 1, :]
            for d in range(1, SUB):
                pair = jnp.where(row >= d, moved[d], 0.0) + jnp.where(row < SUB - d, moved[SUB - d], 0.0)
                total += pair * gains_ref[d, k : k + 1, :]
            out_ref[rows, side] = total
    inverse_copy.wait()
    starts_copy.wait()


def tile_kernel(
    own_ref, below_ref, above_ref, starts, turns_ref, forward_ref, inverse_ref, gains_ref, out_ref,
    sheet
):
    blocks = above_ref.shape[1] // LANES
    halo = [
        jnp.concatenate((lanes_of(above_ref, a), lanes_of(below_ref, a)), axis=0).astype(jnp.float32)
        for a in range(blocks)
    ]
    spec = spectrum(halo, turns_ref, forward_ref)
    row = lax.broadcasted_iota(jnp.int32, (SUB, LANES), 0)
    lane = lax.broadcasted_iota(jnp.int32, (SUB, LANES), 1)
    parts = []
    for k in range(blocks // 2 + 1):
        rows = slice(k * SUB, (k + 1) * SUB)
        both = []
        for side in (slice(0, LANES), slice(LANES, 2 * LANES)):
            here = spec[rows, side]
            total = own_ref[rows, side] + here * gains_ref[0, k]
            for s in range(1, SUB):
                total += pltpu.roll(here, s, axis=0) * gains_ref[s, k]
            both.append(total)
        parts.append(jnp.concatenate(both, axis=1))
    filtered = columns(jnp.concatenate(parts, axis=0), turns_ref, inverse_ref, blocks)
    for a in range(blocks):
        sheet[a] = filtered[a]
    regions = starts.shape[1]
    cut = out_ref.shape[0] * LANES // (regions * SUB)
    per = LANES // cut
    keep = lane // cut == row % per
    packed = []
    for group in range(regions // per):
        gathered = None
        for q in range(per):
            start = starts[0, group * per + q]
            block = lax.shift_right_logical(start, 7)
            offset = start & (LANES - 1)
            window = jnp.where(lane >= offset, sheet[block], sheet[block + 1])
            window = pltpu.roll(window, (LANES + q * cut - offset) & (LANES - 1), axis=1)
            gathered = window if q == 0 else jnp.where(lane // cut == q, window, gathered)
        for shift in range(per):
            moved = gathered if shift == 0 else pltpu.roll(gathered, shift * cut, axis=1)
            packed.append(jnp.where(keep, moved, 0.0).astype(jnp.bfloat16))
    lines = out_ref.shape[0]
    want = lax.broadcasted_iota(jnp.int32, (lines, regions * SUB), 0)
    have = lax.broadcasted_iota(jnp.int32, (lines, regions * SUB), 1)
    have_row, have_shift, have_group = have % SUB, have // SUB % per, have // (SUB * per)
    have_region = have_group * per + (have_row % per + per - have_shift) % per
    pick = jnp.where(have_region * (SUB // per) + have_row // per == want, 1.0, 0.0).astype(jnp.bfloat16)
    out = jnp.dot(pick, jnp.concatenate(packed, axis=0), preferred_element_type=jnp.float32)
    out_ref[...] = out.astype(jnp.bfloat16)


class Routes:
    UNITS = 4
    AROUND = 16

    def __init__(self, count):
        step = count // self.AROUND
        devices = lambda steps: [s * step + c for s in steps for c in range(step)]
        link = lambda pairs: [p for src, dst in pairs for p in zip(devices([src]), devices([dst]))]
        self.count, self.half = count, count // 2
        self.near = devices((12, 13, 14, 15, 0, 1, 2, 3))
        self.far = devices(range(4, 12))
        self.relays = devices((1, 2, 3))
        self.enter = [
            link(((11, 1), (9, 2), (7, 3))),
            link(((10, 1), (8, 2), (6, 3))),
            link(((5, 2), (4, 3), (1, 6), (2, 5), (3, 4))),
        ]
        self.leave = [link(((12, 11), (13, 9), (14, 7), (3, 4))), link(((12, 10), (13, 8), (14, 6), (3, 5)))]

    def exchange_table(self):
        table = np.zeros((3, self.half * self.UNITS * 2, (1 + len(self.enter)) * self.count * 2), np.float32)

        def put(kind, m, unit, source, region):
            for i in range(2):
                table[kind, (m * self.UNITS + unit) * 2 + i, (source * self.count + region) * 2 + i] = 1.0

        for m, dest in enumerate(self.far):
            put(0, m, 0, 0, dest)
            put(0, m, 1, len(self.enter), dest)
        for m, dest in enumerate(self.near):
            put(1, m, 0, 0, dest)
            put(2, m, 0, 0, dest)
            for turn in range(len(self.enter)):
                put(1, m, 1 + turn, 1 + turn, dest)
            for turn in range(len(self.leave)):
                for src, final in self.leave[turn]:
                    if src == dest:
                        put(2, m, 1 + turn, 0, final)
        return table.astype(jnp.bfloat16)

    def arrival_table(self):
        size = self.half * self.UNITS
        table = np.zeros((3, self.count * 2, 3 * size * 2), np.float32)

        def put(kind, angle, source, m, unit):
            for i in range(2):
                table[kind, angle * 2 + i, (source * size + m * self.UNITS + unit) * 2 + i] = 1.0

        for m, angle in enumerate(self.near):
            put(0, angle, 0, m, 0)
            for turn in range(len(self.enter)):
                for src, dst in self.enter[turn]:
                    if dst == angle:
                        put(0, src, 0, m, 1 + turn)
            for turn in range(len(self.leave)):
                if angle not in self.relays:
                    put(1 + turn, angle, 1 + turn, m, 1 + turn)
        for m, angle in enumerate(self.far):
            for turn in range(len(self.leave)):
                put(1 + turn, angle, 0, m, 0)
                for src, dst in self.enter[-1]:
                    if dst == angle:
                        put(1 + turn, src, 0, m, 1)
        return table.astype(jnp.bfloat16)

    @classmethod
    def kinds(cls, device, count):
        step = device // (count // cls.AROUND)
        turned = lax.rem(step + 4, cls.AROUND)
        far = turned >= 8
        other = turned <= 4
        early = (step == 4) | ((step > 6) & (step % 2 == 1))
        return jnp.where(far, 0, jnp.where(other, 2, 1)), jnp.where(far, jnp.where(early, 1, 2), 0)


def repack_kernel(lines_ref, first_ref, second_ref, third_ref, table_ref, out_ref):
    kind, _ = Routes.kinds(lax.axis_index("ang"), lax.axis_size("ang"))
    lines = jnp.concatenate((lines_ref[...], first_ref[...], second_ref[...], third_ref[...]), axis=0)
    out = jnp.dot(table_ref[kind], lines, preferred_element_type=jnp.float32)
    out_ref[...] = out.astype(out_ref.dtype)


def pixels_kernel(near_ref, first_ref, second_ref, table_ref, weights_ref, out_ref, lines, *, angles):
    _, kind = Routes.kinds(lax.axis_index("ang"), lax.axis_size("ang"))
    held = jnp.concatenate((near_ref[...], first_ref[...], second_ref[...]), axis=0)
    lines[...] = jnp.dot(table_ref[kind], held, preferred_element_type=jnp.float32)
    cut = lines.shape[0] * LANES // SUB // angles
    per = LANES // cut
    row = lax.broadcasted_iota(jnp.int32, (SUB, LANES), 0)
    lane = lax.broadcasted_iota(jnp.int32, (SUB, LANES), 1)
    turn = (lane // cut + per - row % per) % per
    parts = []
    for group in range(angles // per):
        spread = []
        for q in range(per):
            at = (group * per + q) * (SUB // per)
            low = jnp.broadcast_to(lines[at : at + 1, :], (SUB, LANES))
            high = jnp.broadcast_to(lines[at + 1 : at + 2, :], (SUB, LANES))
            spread.append(jnp.where(row < per, low, high))
        part = None
        for shift in range(per):
            mixed = spread[shift]
            for j in range(1, per):
                mixed = jnp.where(row % per == j, spread[(j + shift) % per], mixed)
            if shift > 0:
                mixed = pltpu.roll(mixed, shift * cut, axis=1)
            part = mixed if shift == 0 else jnp.where(turn == shift, mixed, part)
        parts.append(part.astype(jnp.bfloat16))
    out_ref[...] = jnp.dot(jnp.concatenate(parts, axis=1), weights_ref[...], preferred_element_type=jnp.float32)


def in_hbm(array):
    return pltpu.with_memory_space_constraint(array, pltpu.HBM)


def make_contrast(projections, flats):
    shape = flats.shape
    edge = jax.ShapeDtypeStruct((HALO, shape[1]), halo_type)
    return pl.pallas_call(
        contrast_kernel,
        out_shape=(jax.ShapeDtypeStruct(shape, jnp.float32), edge, edge),
        in_specs=[HBM] * 2,
        out_specs=(VMEM,) * 3,
        scratch_shapes=[
            pltpu.VMEM(projections.shape, projections.dtype),
            pltpu.VMEM(flats.shape, flats.dtype),
            pltpu.SemaphoreType.DMA((2,)),
        ],
        compiler_params=PARAMS,
        name="contrast",
    )(in_hbm(projections), in_hbm(flats))


def make_own(own, turns, forward, inverse, gains, starts):
    groups = turns.shape[1]
    return pl.pallas_call(
        own_kernel,
        out_shape=(
            jax.ShapeDtypeStruct((groups * SUB, 2 * LANES), jnp.float32),
            jax.ShapeDtypeStruct(forward.shape, forward.dtype),
            jax.ShapeDtypeStruct(inverse.shape, inverse.dtype),
            jax.ShapeDtypeStruct((SUB, groups, SUB, LANES), jnp.float32),
            pltpu.SMEM((1, starts.shape[1]), jnp.int32),
        ),
        in_specs=[VMEM] * 3 + [HBM] * 3,
        out_specs=(VMEM,) * 4 + (SMEM,),
        scratch_shapes=[pltpu.SemaphoreType.DMA((3,))],
        compiler_params=PARAMS,
        name="own_rows",
    )(own, turns, gains, in_hbm(forward), in_hbm(inverse), in_hbm(starts))


def make_tile(own_spec, below, above, starts, turns, forward, inverse, gains, cut):
    regions = starts.shape[1]
    return pl.pallas_call(
        tile_kernel,
        out_shape=jax.ShapeDtypeStruct((regions * SUB * cut // LANES, LANES), jnp.bfloat16),
        in_specs=[VMEM] * 3 + [SMEM] + [VMEM] * 4,
        out_specs=VMEM,
        scratch_shapes=[
            pltpu.VMEM((above.shape[1] // LANES + 1, SUB, LANES), jnp.float32),
        ],
        compiler_params=PARAMS,
        name="tile",
    )(own_spec, below, above, starts, turns, forward, inverse, gains)


def make_repack(lines, first, second, third, table):
    return pl.pallas_call(
        repack_kernel,
        out_shape=jax.ShapeDtypeStruct((table.shape[1], LANES), lines.dtype),
        in_specs=[VMEM] * 5,
        out_specs=VMEM,
        compiler_params=PARAMS,
        name="repack",
    )(lines, first, second, third, table)


def make_pixels(near, first, second, table, weights):
    angles, cut, pixels = weights.shape
    return pl.pallas_call(
        partial(pixels_kernel, angles=angles),
        out_shape=jax.ShapeDtypeStruct((SUB, pixels), jnp.float32),
        in_specs=[VMEM] * 5,
        out_specs=VMEM,
        scratch_shapes=[pltpu.VMEM((table.shape[1], LANES), jnp.float32)],
        compiler_params=PARAMS,
        name="pixels",
    )(near, first, second, table, weights.reshape(angles * cut, pixels))


def body(projections, flats, block_start, bp_weights):
    angles_dev, rows_dev, width = projections.shape
    cut = bp_weights.shape[1]
    assert angles_dev == 1 and rows_dev == SUB and width % (2 * LANES) == 0 and SUB * cut == 2 * LANES
    rows = lax.axis_size("row")
    up = [(i, i + 1) for i in range(rows - 1)]
    down = [(j, i) for i, j in up]
    turns, forward, inverse, gains = (jnp.asarray(t) for t in tables(width, rows_dev + 2 * HALO))
    own, first, last = make_contrast(projections, flats)
    below = lax.ppermute(first, "row", down)
    above = lax.ppermute(last, "row", up)
    own_spec, forward, inverse, gains, starts = make_own(own, turns, forward, inverse, gains, block_start)
    outgoing = make_tile(own_spec, below, above, starts, turns, forward, inverse, gains, cut)
    routes = Routes(lax.axis_size("ang"))
    entered = [lax.ppermute(outgoing, "ang", pairs) for pairs in routes.enter]
    packed = make_repack(outgoing, *entered, jnp.asarray(routes.exchange_table()))
    near = lax.all_to_all(
        packed.reshape(-1, 2, LANES), "ang", split_axis=0, concat_axis=0, tiled=True,
        axis_index_groups=[routes.near, routes.far],
    ).reshape(packed.shape)
    left = [lax.ppermute(near, "ang", pairs) for pairs in routes.leave]
    return make_pixels(near, *left, jnp.asarray(routes.arrival_table()), bp_weights)


def solution(mesh):
    placed = (P(("scan", "ang"), "row", None), P(("scan", "row"), None), P(), P(None, None, "ang"))
    return jax.shard_map(
        body, mesh=mesh, in_specs=placed, out_specs=P(("scan", "row"), "ang"), check_vma=False
    )
```

```python
from functools import partial

import jax
import jax.numpy as jnp
import numpy as np
from jax import lax
from jax.experimental import pallas as pl
from jax.experimental.pallas import tpu as pltpu
from jax.sharding import PartitionSpec as P

HALO = 4
LANES = 128
SUB = 8

paganin_beta = 8.0
ramp_gain = 320.0
halo_type = jnp.float32
VMEM = pl.BlockSpec(memory_space=pltpu.VMEM)
SMEM = pl.BlockSpec(memory_space=pltpu.SMEM)
HBM = pl.BlockSpec(memory_space=pltpu.HBM)
PARAMS = pltpu.CompilerParams(vmem_limit_bytes=8 * 2**20)


def tables(width, tile_rows):
    blocks = width // LANES
    half = blocks // 2
    lane = np.arange(LANES)
    ks = np.arange(half + 1)
    turn = 2.0 * np.pi / width * (ks[:, None] * lane[None, :])
    turns = np.stack((np.cos(turn), np.sin(turn))).astype(np.float32)
    angle = 2.0 * np.pi / LANES * (lane[:, None] * lane[None, :] % LANES)
    cos, sin = np.cos(angle), np.sin(angle)
    forward = np.block([[cos, -sin], [sin, cos]])

    def split(matrix):
        high = matrix.astype(jnp.bfloat16)
        low = (matrix - high.astype(np.float64)).astype(jnp.bfloat16)
        return np.stack((high, low))

    freq = (ks[:, None] + blocks * lane[None, :]).astype(np.float64)
    row = np.arange(tile_rows, dtype=np.float64)
    lam = 4.0 * np.sin(np.pi * row / tile_rows)[:, None, None] ** 2 + 4.0 * np.sin(np.pi * freq / width) ** 2
    filt = 1.0 / (1.0 + paganin_beta * lam)
    dist = np.arange(tile_rows // 2 + 1)
    gains = np.einsum("du,ukm->dkm", np.cos(2.0 * np.pi / tile_rows * dist[:, None] * row), filt) / tile_rows
    folded = np.minimum(freq, width - freq)
    ramp = ramp_gain * (folded / width) * (0.5 + 0.5 * np.cos(2.0 * np.pi * folded / width))
    twice = np.where((ks == 0) | (ks == half), 1.0, 2.0)
    gains = gains * (ramp * twice[:, None] / width)
    return turns, split(forward), split(forward.T), gains.astype(np.float32)


def plus(terms):
    return sum(terms[1:], terms[0])


def scaled(terms, weights):
    out = None
    for term, weight in zip(terms, weights):
        weight = float(weight)
        if abs(weight) < 1e-12:
            continue
        piece = term if weight == 1.0 else -term if weight == -1.0 else term * weight
        out = piece if out is None else out + piece
    return out


def cosine_sums(terms, blocks):
    half = blocks // 2
    out = [None] * (half + 1)
    for k in range(half // 2 + 1):
        wave = [np.round(np.cos(2.0 * np.pi * a * k / blocks), 15) for a in range(half + 1)]
        even = scaled(terms[0::2], wave[0::2])
        odd = scaled(terms[1::2], wave[1::2])
        out[k] = even if odd is None else even + odd
        if half - k != k:
            out[half - k] = even if odd is None else even - odd
    return out


def sine_sums(terms, blocks):
    half = blocks // 2
    out = [None] * (half + 1)
    for k in range(1, half // 2 + 1):
        wave = [np.round(np.sin(2.0 * np.pi * a * k / blocks), 15) for a in range(half)]
        even = scaled(terms[2:half:2], wave[2::2])
        odd = scaled(terms[1:half:2], wave[1::2])
        if half - k != k:
            out[k] = plus([x for x in (even, odd) if x is not None])
            out[half - k] = odd - even if even is not None else odd
        else:
            out[k] = plus([x for x in (even, odd) if x is not None])
    return out


def accurate_dot(values, matrix_ref):
    high = values.astype(jnp.bfloat16)
    low = (values - high.astype(jnp.float32)).astype(jnp.bfloat16)
    dot = partial(jnp.dot, preferred_element_type=jnp.float32)
    lines = values.shape[0]
    both = dot(jnp.concatenate((high, low), axis=0), matrix_ref[0])
    return both[:lines] + (both[lines:] + dot(high, matrix_ref[1]))


def spectrum(chunks, turns_ref, forward_ref):
    blocks = len(chunks)
    half = blocks // 2
    folds = [chunks[0]] + [chunks[a] + chunks[blocks - a] for a in range(1, half)] + [chunks[half]]
    skews = [None] + [chunks[a] - chunks[blocks - a] for a in range(1, half)] + [None]
    reals = cosine_sums(folds, blocks)
    imags = sine_sums(skews, blocks)
    parts = []
    for k in range(half + 1):
        cos, sin = turns_ref[0, k : k + 1, :], turns_ref[1, k : k + 1, :]
        if k == 0:
            re, im = reals[0], jnp.zeros_like(reals[0])
        elif imags[k] is None:
            re, im = reals[k] * cos, -(reals[k] * sin)
        else:
            re, im = reals[k] * cos - imags[k] * sin, -(imags[k] * cos) - reals[k] * sin
        parts.append(jnp.concatenate((re, im), axis=1))
    return accurate_dot(jnp.concatenate(parts, axis=0), forward_ref)


def columns(spec, turns_ref, inverse_ref, blocks):
    half = blocks // 2
    back = accurate_dot(spec, inverse_ref)
    reals, imags = [], []
    for k in range(half + 1):
        rows = slice(k * SUB, (k + 1) * SUB)
        re, im = back[rows, :LANES], back[rows, LANES:]
        cos, sin = turns_ref[0, k : k + 1, :], turns_ref[1, k : k + 1, :]
        if k == 0:
            reals.append(re)
            imags.append(None)
        else:
            reals.append(re * cos - im * sin)
            imags.append(im * cos + re * sin if k < half else None)
    even = cosine_sums(reals, blocks)
    odd = sine_sums(imags, blocks)
    out = [None] * blocks
    out[0], out[half] = even[0], even[half]
    for a in range(1, half):
        out[a] = even[a] - odd[a]
        out[blocks - a] = even[a] + odd[a]
    return out


def contrast_kernel(proj_hbm, flat_hbm, own_ref, first_ref, last_ref, proj, flat, sems):
    copies = [
        pltpu.make_async_copy(proj_hbm, proj, sems.at[0]),
        pltpu.make_async_copy(flat_hbm, flat, sems.at[1]),
    ]
    for copy in copies:
        copy.start()
    for copy in copies:
        copy.wait()
    own = 1.0 - proj[0].astype(jnp.float32) / flat[...]
    own_ref[...] = own
    first_ref[...] = own[:HALO].astype(first_ref.dtype)
    last_ref[...] = own[SUB - HALO :].astype(last_ref.dtype)


def lanes_of(ref, block):
    return ref[:, block * LANES : (block + 1) * LANES]


def halo_gains(gains_ref, k, row):
    gains = [jnp.broadcast_to(gains_ref[d, k : k + 1, :], (SUB, LANES)) for d in range(2 * HALO + 1)]
    for s in range(SUB):
        far = gains[2 * HALO - abs(s - HALO)]
        near = gains[abs(s - HALO)]
        if s < HALO:
            yield s, jnp.where(row >= s + HALO, near, far)
        else:
            yield s, jnp.where(row < s - HALO, near, far)


def own_kernel(
    own_ref, turns_ref, gains_ref, forward_hbm, inverse_hbm, starts_hbm,
    out_ref, forward_ref, inverse_ref, halo_ref, starts_ref, sems
):
    forward_copy = pltpu.make_async_copy(forward_hbm, forward_ref, sems.at[0])
    inverse_copy = pltpu.make_async_copy(inverse_hbm, inverse_ref, sems.at[1])
    starts_copy = pltpu.make_async_copy(starts_hbm.at[pl.ds(lax.axis_index("ang"), 1)], starts_ref, sems.at[2])
    forward_copy.start()
    inverse_copy.start()
    starts_copy.start()
    row = lax.broadcasted_iota(jnp.int32, (SUB, LANES), 0)
    for k in range(gains_ref.shape[1]):
        for s, gain in halo_gains(gains_ref, k, row):
            halo_ref[s, k] = gain
    forward_copy.wait()
    blocks = own_ref.shape[1] // LANES
    spec = spectrum([lanes_of(own_ref, a) for a in range(blocks)], turns_ref, forward_ref)
    for k in range(blocks // 2 + 1):
        rows = slice(k * SUB, (k + 1) * SUB)
        for side in (slice(0, LANES), slice(LANES, 2 * LANES)):
            here = spec[rows, side]
            moved = [here] + [pltpu.roll(here, s, axis=0) for s in range(1, SUB)]
            total = here * gains_ref[0, k : k + 1, :]
            for d in range(1, SUB):
                pair = jnp.where(row >= d, moved[d], 0.0) + jnp.where(row < SUB - d, moved[SUB - d], 0.0)
                total += pair * gains_ref[d, k : k + 1, :]
            out_ref[rows, side] = total
    inverse_copy.wait()
    starts_copy.wait()


def tile_kernel(
    own_ref, below_ref, above_ref, starts, turns_ref, forward_ref, inverse_ref, gains_ref, out_ref,
    sheet
):
    blocks = above_ref.shape[1] // LANES
    halo = [
        jnp.concatenate((lanes_of(above_ref, a), lanes_of(below_ref, a)), axis=0).astype(jnp.float32)
        for a in range(blocks)
    ]
    spec = spectrum(halo, turns_ref, forward_ref)
    row = lax.broadcasted_iota(jnp.int32, (SUB, LANES), 0)
    lane = lax.broadcasted_iota(jnp.int32, (SUB, LANES), 1)
    parts = []
    for k in range(blocks // 2 + 1):
        rows = slice(k * SUB, (k + 1) * SUB)
        both = []
        for side in (slice(0, LANES), slice(LANES, 2 * LANES)):
            here = spec[rows, side]
            total = own_ref[rows, side] + here * gains_ref[0, k]
            for s in range(1, SUB):
                total += pltpu.roll(here, s, axis=0) * gains_ref[s, k]
            both.append(total)
        parts.append(jnp.concatenate(both, axis=1))
    filtered = columns(jnp.concatenate(parts, axis=0), turns_ref, inverse_ref, blocks)
    for a in range(blocks):
        sheet[a] = filtered[a]
    regions = starts.shape[1]
    cut = out_ref.shape[0] * LANES // (regions * SUB)
    per = LANES // cut
    keep = lane // cut == row % per
    packed = []
    for group in range(regions // per):
        gathered = None
        for q in range(per):
            start = starts[0, group * per + q]
            block = lax.shift_right_logical(start, 7)
            offset = start & (LANES - 1)
            window = jnp.where(lane >= offset, sheet[block], sheet[block + 1])
            window = pltpu.roll(window, (LANES + q * cut - offset) & (LANES - 1), axis=1)
            gathered = window if q == 0 else jnp.where(lane // cut == q, window, gathered)
        for shift in range(per):
            moved = gathered if shift == 0 else pltpu.roll(gathered, shift * cut, axis=1)
            packed.append(jnp.where(keep, moved, 0.0).astype(jnp.bfloat16))
    lines = out_ref.shape[0]
    want = lax.broadcasted_iota(jnp.int32, (lines, regions * SUB), 0)
    have = lax.broadcasted_iota(jnp.int32, (lines, regions * SUB), 1)
    have_row, have_shift, have_group = have % SUB, have // SUB % per, have // (SUB * per)
    have_region = have_group * per + (have_row % per + per - have_shift) % per
    pick = jnp.where(have_region * (SUB // per) + have_row // per == want, 1.0, 0.0).astype(jnp.bfloat16)
    out = jnp.dot(pick, jnp.concatenate(packed, axis=0), preferred_element_type=jnp.float32)
    out_ref[...] = out.astype(jnp.bfloat16)


class Routes:
    UNITS = 3
    AROUND = 16

    def __init__(self, count):
        step = count // self.AROUND
        devices = lambda steps: [s * step + c for s in steps for c in range(step)]
        link = lambda pairs: [p for src, dst in pairs for p in zip(devices([src]), devices([dst]))]
        self.count, self.half = count, count // 2
        self.near = devices((12, 13, 14, 15, 3, 2, 1, 0))
        self.far = devices((11, 10, 9, 8, 7, 6, 5, 4))
        self.relays = devices((12, 1, 2, 3))
        first = link(((11, 12), (4, 3), (5, 2), (6, 1)))
        self.enter = [first + [(dst, src) for src, dst in first], link(((10, 12), (9, 3), (8, 2), (7, 1)))]
        self.leave = [link(((12, 11), (13, 9), (14, 7), (3, 4))), link(((12, 10), (13, 8), (14, 6), (3, 5)))]

    def exchange_table(self):
        table = np.zeros((3, self.half * self.UNITS * 2, 3 * self.count * 2), np.float32)

        def put(kind, m, unit, source, region):
            for i in range(2):
                table[kind, (m * self.UNITS + unit) * 2 + i, (source * self.count + region) * 2 + i] = 1.0

        for m, dest in enumerate(self.far):
            put(0, m, 0, 0, dest)
            put(0, m, 1, 1, dest)
        for m, dest in enumerate(self.near):
            put(1, m, 0, 0, dest)
            put(2, m, 0, 0, dest)
            for turn in range(2):
                put(1, m, 1 + turn, 1 + turn, dest)
                for src, final in self.leave[turn]:
                    if src == dest:
                        put(2, m, 1 + turn, 0, final)
        return table.astype(jnp.bfloat16)

    def arrival_table(self):
        size = self.half * self.UNITS
        table = np.zeros((3, self.count * 2, 3 * size * 2), np.float32)

        def put(kind, angle, source, m, unit):
            for i in range(2):
                table[kind, angle * 2 + i, (source * size + m * self.UNITS + unit) * 2 + i] = 1.0

        for m, angle in enumerate(self.near):
            put(0, angle, 0, m, 0)
            for turn in range(2):
                for src, dst in self.enter[turn]:
                    if dst == angle:
                        put(0, src, 0, m, 1 + turn)
                if angle not in self.relays:
                    put(1 + turn, angle, 1 + turn, m, 1 + turn)
        for m, angle in enumerate(self.far):
            for turn in range(2):
                put(1 + turn, angle, 0, m, 0)
                for src, dst in self.enter[0]:
                    if dst == angle:
                        put(1 + turn, src, 0, m, 1)
        return table.astype(jnp.bfloat16)

    @classmethod
    def kinds(cls, device, count):
        step = device // (count // cls.AROUND)
        turned = lax.rem(step + 4, cls.AROUND)
        far = turned >= 8
        other = (turned >= 1) & (turned <= 4)
        early = (step == 4) | ((step > 6) & (step % 2 == 1))
        return jnp.where(far, 0, jnp.where(other, 2, 1)), jnp.where(far, jnp.where(early, 1, 2), 0)


def repack_kernel(lines_ref, first_ref, second_ref, table_ref, out_ref):
    kind, _ = Routes.kinds(lax.axis_index("ang"), lax.axis_size("ang"))
    lines = jnp.concatenate((lines_ref[...], first_ref[...], second_ref[...]), axis=0)
    out = jnp.dot(table_ref[kind], lines, preferred_element_type=jnp.float32)
    out_ref[...] = out.astype(out_ref.dtype)


def pixels_kernel(near_ref, first_ref, second_ref, table_ref, weights_ref, out_ref, lines, *, angles):
    _, kind = Routes.kinds(lax.axis_index("ang"), lax.axis_size("ang"))
    held = jnp.concatenate((near_ref[...], first_ref[...], second_ref[...]), axis=0)
    lines[...] = jnp.dot(table_ref[kind], held, preferred_element_type=jnp.float32)
    cut = lines.shape[0] * LANES // SUB // angles
    per = LANES // cut
    row = lax.broadcasted_iota(jnp.int32, (SUB, LANES), 0)
    lane = lax.broadcasted_iota(jnp.int32, (SUB, LANES), 1)
    turn = (lane // cut + per - row % per) % per
    parts = []
    for group in range(angles // per):
        spread = []
        for q in range(per):
            at = (group * per + q) * (SUB // per)
            low = jnp.broadcast_to(lines[at : at + 1, :], (SUB, LANES))
            high = jnp.broadcast_to(lines[at + 1 : at + 2, :], (SUB, LANES))
            spread.append(jnp.where(row < per, low, high))
        part = None
        for shift in range(per):
            mixed = spread[shift]
            for j in range(1, per):
                mixed = jnp.where(row % per == j, spread[(j + shift) % per], mixed)
            if shift > 0:
                mixed = pltpu.roll(mixed, shift * cut, axis=1)
            part = mixed if shift == 0 else jnp.where(turn == shift, mixed, part)
        parts.append(part.astype(jnp.bfloat16))
    out_ref[...] = jnp.dot(jnp.concatenate(parts, axis=1), weights_ref[...], preferred_element_type=jnp.float32)


def in_hbm(array):
    return pltpu.with_memory_space_constraint(array, pltpu.HBM)


def make_contrast(projections, flats):
    shape = flats.shape
    edge = jax.ShapeDtypeStruct((HALO, shape[1]), halo_type)
    return pl.pallas_call(
        contrast_kernel,
        out_shape=(jax.ShapeDtypeStruct(shape, jnp.float32), edge, edge),
        in_specs=[HBM] * 2,
        out_specs=(VMEM,) * 3,
        scratch_shapes=[
            pltpu.VMEM(projections.shape, projections.dtype),
            pltpu.VMEM(flats.shape, flats.dtype),
            pltpu.SemaphoreType.DMA((2,)),
        ],
        compiler_params=PARAMS,
        name="contrast",
    )(in_hbm(projections), in_hbm(flats))


def make_own(own, turns, forward, inverse, gains, starts):
    groups = turns.shape[1]
    return pl.pallas_call(
        own_kernel,
        out_shape=(
            jax.ShapeDtypeStruct((groups * SUB, 2 * LANES), jnp.float32),
            jax.ShapeDtypeStruct(forward.shape, forward.dtype),
            jax.ShapeDtypeStruct(inverse.shape, inverse.dtype),
            jax.ShapeDtypeStruct((SUB, groups, SUB, LANES), jnp.float32),
            pltpu.SMEM((1, starts.shape[1]), jnp.int32),
        ),
        in_specs=[VMEM] * 3 + [HBM] * 3,
        out_specs=(VMEM,) * 4 + (SMEM,),
        scratch_shapes=[pltpu.SemaphoreType.DMA((3,))],
        compiler_params=PARAMS,
        name="own_rows",
    )(own, turns, gains, in_hbm(forward), in_hbm(inverse), in_hbm(starts))


def make_tile(own_spec, below, above, starts, turns, forward, inverse, gains, cut):
    regions = starts.shape[1]
    return pl.pallas_call(
        tile_kernel,
        out_shape=jax.ShapeDtypeStruct((regions * SUB * cut // LANES, LANES), jnp.bfloat16),
        in_specs=[VMEM] * 3 + [SMEM] + [VMEM] * 4,
        out_specs=VMEM,
        scratch_shapes=[
            pltpu.VMEM((above.shape[1] // LANES + 1, SUB, LANES), jnp.float32),
        ],
        compiler_params=PARAMS,
        name="tile",
    )(own_spec, below, above, starts, turns, forward, inverse, gains)


def make_repack(lines, first, second, table):
    return pl.pallas_call(
        repack_kernel,
        out_shape=jax.ShapeDtypeStruct((table.shape[1], LANES), lines.dtype),
        in_specs=[VMEM] * 4,
        out_specs=VMEM,
        compiler_params=PARAMS,
        name="repack",
    )(lines, first, second, table)


def make_pixels(near, first, second, table, weights):
    angles, cut, pixels = weights.shape
    return pl.pallas_call(
        partial(pixels_kernel, angles=angles),
        out_shape=jax.ShapeDtypeStruct((SUB, pixels), jnp.float32),
        in_specs=[VMEM] * 5,
        out_specs=VMEM,
        scratch_shapes=[pltpu.VMEM((table.shape[1], LANES), jnp.float32)],
        compiler_params=PARAMS,
        name="pixels",
    )(near, first, second, table, weights.reshape(angles * cut, pixels))


def body(projections, flats, block_start, bp_weights):
    angles_dev, rows_dev, width = projections.shape
    cut = bp_weights.shape[1]
    assert angles_dev == 1 and rows_dev == SUB and width % (2 * LANES) == 0 and SUB * cut == 2 * LANES
    rows = lax.axis_size("row")
    up = [(i, i + 1) for i in range(rows - 1)]
    down = [(j, i) for i, j in up]
    turns, forward, inverse, gains = (jnp.asarray(t) for t in tables(width, rows_dev + 2 * HALO))
    own, first, last = make_contrast(projections, flats)
    below = lax.ppermute(first, "row", down)
    above = lax.ppermute(last, "row", up)
    own_spec, forward, inverse, gains, starts = make_own(own, turns, forward, inverse, gains, block_start)
    outgoing = make_tile(own_spec, below, above, starts, turns, forward, inverse, gains, cut)
    routes = Routes(lax.axis_size("ang"))
    entered = [lax.ppermute(outgoing, "ang", pairs) for pairs in routes.enter]
    packed = make_repack(outgoing, *entered, jnp.asarray(routes.exchange_table()))
    near = lax.all_to_all(
        packed.reshape(-1, 2, LANES), "ang", split_axis=0, concat_axis=0, tiled=True,
        axis_index_groups=[routes.near, routes.far],
    ).reshape(packed.shape)
    left = [lax.ppermute(near, "ang", pairs) for pairs in routes.leave]
    return make_pixels(near, *left, jnp.asarray(routes.arrival_table()), bp_weights)


def solution(mesh):
    placed = (P(("scan", "ang"), "row", None), P(("scan", "row"), None), P(), P(None, None, "ang"))
    return jax.shard_map(
        body, mesh=mesh, in_specs=placed, out_specs=P(("scan", "row"), "ang"), check_vma=False
    )
```

```python
from functools import partial

import jax
import jax.numpy as jnp
import numpy as np
from jax import lax
from jax.experimental import pallas as pl
from jax.experimental.pallas import tpu as pltpu
from jax.sharding import PartitionSpec as P

HALO = 4
LANES = 128
SUB = 8

paganin_beta = 8.0
ramp_gain = 320.0
halo_type = jnp.float32
VMEM = pl.BlockSpec(memory_space=pltpu.VMEM)
SMEM = pl.BlockSpec(memory_space=pltpu.SMEM)
HBM = pl.BlockSpec(memory_space=pltpu.HBM)
PARAMS = pltpu.CompilerParams(vmem_limit_bytes=8 * 2**20)


def tables(width, tile_rows):
    blocks = width // LANES
    half = blocks // 2
    lane = np.arange(LANES)
    ks = np.arange(half + 1)
    turn = 2.0 * np.pi / width * (ks[:, None] * lane[None, :])
    turns = np.stack((np.cos(turn), np.sin(turn))).astype(np.float32)
    angle = 2.0 * np.pi / LANES * (lane[:, None] * lane[None, :] % LANES)
    cos, sin = np.cos(angle), np.sin(angle)
    forward = np.block([[cos, -sin], [sin, cos]])

    def split(matrix):
        high = matrix.astype(jnp.bfloat16)
        low = (matrix - high.astype(np.float64)).astype(jnp.bfloat16)
        return np.stack((high, low))

    freq = (ks[:, None] + blocks * lane[None, :]).astype(np.float64)
    row = np.arange(tile_rows, dtype=np.float64)
    lam = 4.0 * np.sin(np.pi * row / tile_rows)[:, None, None] ** 2 + 4.0 * np.sin(np.pi * freq / width) ** 2
    filt = 1.0 / (1.0 + paganin_beta * lam)
    dist = np.arange(tile_rows // 2 + 1)
    gains = np.einsum("du,ukm->dkm", np.cos(2.0 * np.pi / tile_rows * dist[:, None] * row), filt) / tile_rows
    folded = np.minimum(freq, width - freq)
    ramp = ramp_gain * (folded / width) * (0.5 + 0.5 * np.cos(2.0 * np.pi * folded / width))
    twice = np.where((ks == 0) | (ks == half), 1.0, 2.0)
    gains = gains * (ramp * twice[:, None] / width)
    return turns, split(forward), split(forward.T), gains.astype(np.float32)


def plus(terms):
    return sum(terms[1:], terms[0])


def scaled(terms, weights):
    out = None
    for term, weight in zip(terms, weights):
        weight = float(weight)
        if abs(weight) < 1e-12:
            continue
        piece = term if weight == 1.0 else -term if weight == -1.0 else term * weight
        out = piece if out is None else out + piece
    return out


def cosine_sums(terms, blocks):
    half = blocks // 2
    out = [None] * (half + 1)
    for k in range(half // 2 + 1):
        wave = [np.round(np.cos(2.0 * np.pi * a * k / blocks), 15) for a in range(half + 1)]
        even = scaled(terms[0::2], wave[0::2])
        odd = scaled(terms[1::2], wave[1::2])
        out[k] = even if odd is None else even + odd
        if half - k != k:
            out[half - k] = even if odd is None else even - odd
    return out


def sine_sums(terms, blocks):
    half = blocks // 2
    out = [None] * (half + 1)
    for k in range(1, half // 2 + 1):
        wave = [np.round(np.sin(2.0 * np.pi * a * k / blocks), 15) for a in range(half)]
        even = scaled(terms[2:half:2], wave[2::2])
        odd = scaled(terms[1:half:2], wave[1::2])
        if half - k != k:
            out[k] = plus([x for x in (even, odd) if x is not None])
            out[half - k] = odd - even if even is not None else odd
        else:
            out[k] = plus([x for x in (even, odd) if x is not None])
    return out


def accurate_dot(values, matrix_ref):
    high = values.astype(jnp.bfloat16)
    low = (values - high.astype(jnp.float32)).astype(jnp.bfloat16)
    dot = partial(jnp.dot, preferred_element_type=jnp.float32)
    lines = values.shape[0]
    both = dot(jnp.concatenate((high, low), axis=0), matrix_ref[0])
    return both[:lines] + (both[lines:] + dot(high, matrix_ref[1]))


def spectrum(chunks, turns_ref, forward_ref):
    blocks = len(chunks)
    half = blocks // 2
    folds = [chunks[0]] + [chunks[a] + chunks[blocks - a] for a in range(1, half)] + [chunks[half]]
    skews = [None] + [chunks[a] - chunks[blocks - a] for a in range(1, half)] + [None]
    reals = cosine_sums(folds, blocks)
    imags = sine_sums(skews, blocks)
    parts = []
    for k in range(half + 1):
        cos, sin = turns_ref[0, k : k + 1, :], turns_ref[1, k : k + 1, :]
        if k == 0:
            re, im = reals[0], jnp.zeros_like(reals[0])
        elif imags[k] is None:
            re, im = reals[k] * cos, -(reals[k] * sin)
        else:
            re, im = reals[k] * cos - imags[k] * sin, -(imags[k] * cos) - reals[k] * sin
        parts.append(jnp.concatenate((re, im), axis=1))
    return accurate_dot(jnp.concatenate(parts, axis=0), forward_ref)


def columns(spec, turns_ref, inverse_ref, blocks):
    half = blocks // 2
    back = accurate_dot(spec, inverse_ref)
    reals, imags = [], []
    for k in range(half + 1):
        rows = slice(k * SUB, (k + 1) * SUB)
        re, im = back[rows, :LANES], back[rows, LANES:]
        cos, sin = turns_ref[0, k : k + 1, :], turns_ref[1, k : k + 1, :]
        if k == 0:
            reals.append(re)
            imags.append(None)
        else:
            reals.append(re * cos - im * sin)
            imags.append(im * cos + re * sin if k < half else None)
    even = cosine_sums(reals, blocks)
    odd = sine_sums(imags, blocks)
    out = [None] * blocks
    out[0], out[half] = even[0], even[half]
    for a in range(1, half):
        out[a] = even[a] - odd[a]
        out[blocks - a] = even[a] + odd[a]
    return out


def contrast_kernel(proj_hbm, flat_hbm, own_ref, first_ref, last_ref, proj, flat, sems):
    copies = [
        pltpu.make_async_copy(proj_hbm, proj, sems.at[0]),
        pltpu.make_async_copy(flat_hbm, flat, sems.at[1]),
    ]
    for copy in copies:
        copy.start()
    for copy in copies:
        copy.wait()
    own = 1.0 - proj[0].astype(jnp.float32) / flat[...]
    own_ref[...] = own
    first_ref[...] = own[:HALO].astype(first_ref.dtype)
    last_ref[...] = own[SUB - HALO :].astype(last_ref.dtype)


def lanes_of(ref, block):
    return ref[:, block * LANES : (block + 1) * LANES]


def halo_gains(gains_ref, k, row):
    gains = [jnp.broadcast_to(gains_ref[d, k : k + 1, :], (SUB, LANES)) for d in range(2 * HALO + 1)]
    for s in range(SUB):
        far = gains[2 * HALO - abs(s - HALO)]
        near = gains[abs(s - HALO)]
        if s < HALO:
            yield s, jnp.where(row >= s + HALO, near, far)
        else:
            yield s, jnp.where(row < s - HALO, near, far)


def own_kernel(
    own_ref, turns_ref, gains_ref, forward_hbm, inverse_hbm, starts_hbm,
    out_ref, forward_ref, inverse_ref, halo_ref, starts_ref, sems
):
    forward_copy = pltpu.make_async_copy(forward_hbm, forward_ref, sems.at[0])
    inverse_copy = pltpu.make_async_copy(inverse_hbm, inverse_ref, sems.at[1])
    starts_copy = pltpu.make_async_copy(starts_hbm.at[pl.ds(lax.axis_index("ang"), 1)], starts_ref, sems.at[2])
    forward_copy.start()
    inverse_copy.start()
    starts_copy.start()
    row = lax.broadcasted_iota(jnp.int32, (SUB, LANES), 0)
    for k in range(gains_ref.shape[1]):
        for s, gain in halo_gains(gains_ref, k, row):
            halo_ref[s, k] = gain
    forward_copy.wait()
    blocks = own_ref.shape[1] // LANES
    spec = spectrum([lanes_of(own_ref, a) for a in range(blocks)], turns_ref, forward_ref)
    for k in range(blocks // 2 + 1):
        rows = slice(k * SUB, (k + 1) * SUB)
        for side in (slice(0, LANES), slice(LANES, 2 * LANES)):
            here = spec[rows, side]
            moved = [here] + [pltpu.roll(here, s, axis=0) for s in range(1, SUB)]
            total = here * gains_ref[0, k : k + 1, :]
            for d in range(1, SUB):
                pair = jnp.where(row >= d, moved[d], 0.0) + jnp.where(row < SUB - d, moved[SUB - d], 0.0)
                total += pair * gains_ref[d, k : k + 1, :]
            out_ref[rows, side] = total
    inverse_copy.wait()
    starts_copy.wait()


def tile_kernel(
    own_ref, below_ref, above_ref, starts, turns_ref, forward_ref, inverse_ref, gains_ref, out_ref,
    sheet
):
    blocks = above_ref.shape[1] // LANES
    halo = [
        jnp.concatenate((lanes_of(above_ref, a), lanes_of(below_ref, a)), axis=0).astype(jnp.float32)
        for a in range(blocks)
    ]
    spec = spectrum(halo, turns_ref, forward_ref)
    row = lax.broadcasted_iota(jnp.int32, (SUB, LANES), 0)
    lane = lax.broadcasted_iota(jnp.int32, (SUB, LANES), 1)
    parts = []
    for k in range(blocks // 2 + 1):
        rows = slice(k * SUB, (k + 1) * SUB)
        both = []
        for side in (slice(0, LANES), slice(LANES, 2 * LANES)):
            here = spec[rows, side]
            total = own_ref[rows, side] + here * gains_ref[0, k]
            for s in range(1, SUB):
                total += pltpu.roll(here, s, axis=0) * gains_ref[s, k]
            both.append(total)
        parts.append(jnp.concatenate(both, axis=1))
    filtered = columns(jnp.concatenate(parts, axis=0), turns_ref, inverse_ref, blocks)
    for a in range(blocks):
        sheet[a] = filtered[a]
    regions = starts.shape[1]
    cut = out_ref.shape[0] * LANES // (regions * SUB)
    per = LANES // cut
    keep = lane // cut == row % per
    packed = []
    for group in range(regions // per):
        gathered = None
        for q in range(per):
            start = starts[0, group * per + q]
            block = lax.shift_right_logical(start, 7)
            offset = start & (LANES - 1)
            window = jnp.where(lane >= offset, sheet[block], sheet[block + 1])
            window = pltpu.roll(window, (LANES + q * cut - offset) & (LANES - 1), axis=1)
            gathered = window if q == 0 else jnp.where(lane // cut == q, window, gathered)
        for shift in range(per):
            moved = gathered if shift == 0 else pltpu.roll(gathered, shift * cut, axis=1)
            packed.append(jnp.where(keep, moved, 0.0).astype(jnp.bfloat16))
    lines = out_ref.shape[0]
    want = lax.broadcasted_iota(jnp.int32, (lines, regions * SUB), 0)
    have = lax.broadcasted_iota(jnp.int32, (lines, regions * SUB), 1)
    have_row, have_shift, have_group = have % SUB, have // SUB % per, have // (SUB * per)
    have_region = have_group * per + (have_row % per + per - have_shift) % per
    pick = jnp.where(have_region * (SUB // per) + have_row // per == want, 1.0, 0.0).astype(jnp.bfloat16)
    out = jnp.dot(pick, jnp.concatenate(packed, axis=0), preferred_element_type=jnp.float32)
    out_ref[...] = out.astype(jnp.bfloat16)


class Routes:
    UNITS = 3
    AROUND = 16

    def __init__(self, count):
        step = count // self.AROUND
        devices = lambda steps: [s * step + c for s in steps for c in range(step)]
        link = lambda pairs: [p for src, dst in pairs for p in zip(devices([src]), devices([dst]))]
        self.count, self.half = count, count // 2
        self.near = devices((12, 13, 14, 15, 0, 1, 2, 3))
        self.far = devices(range(4, 12))
        self.relays = devices((12, 1, 2, 3))
        first = link(((11, 12), (4, 3), (5, 2), (6, 1)))
        self.enter = [first + [(dst, src) for src, dst in first], link(((10, 12), (9, 3), (8, 2), (7, 1)))]
        self.leave = [link(((12, 11), (13, 9), (14, 7), (3, 4))), link(((12, 10), (13, 8), (14, 6), (3, 5)))]

    def exchange_table(self):
        table = np.zeros((3, self.half * self.UNITS * 2, 3 * self.count * 2), np.float32)

        def put(kind, m, unit, source, region):
            for i in range(2):
                table[kind, (m * self.UNITS + unit) * 2 + i, (source * self.count + region) * 2 + i] = 1.0

        for m, dest in enumerate(self.far):
            put(0, m, 0, 0, dest)
            put(0, m, 1, 1, dest)
        for m, dest in enumerate(self.near):
            put(1, m, 0, 0, dest)
            put(2, m, 0, 0, dest)
            for turn in range(2):
                put(1, m, 1 + turn, 1 + turn, dest)
                for src, final in self.leave[turn]:
                    if src == dest:
                        put(2, m, 1 + turn, 0, final)
        return table.astype(jnp.bfloat16)

    def arrival_table(self):
        size = self.half * self.UNITS
        table = np.zeros((3, self.count * 2, 3 * size * 2), np.float32)

        def put(kind, angle, source, m, unit):
            for i in range(2):
                table[kind, angle * 2 + i, (source * size + m * self.UNITS + unit) * 2 + i] = 1.0

        for m, angle in enumerate(self.near):
            put(0, angle, 0, m, 0)
            for turn in range(2):
                for src, dst in self.enter[turn]:
                    if dst == angle:
                        put(0, src, 0, m, 1 + turn)
                if angle not in self.relays:
                    put(1 + turn, angle, 1 + turn, m, 1 + turn)
        for m, angle in enumerate(self.far):
            for turn in range(2):
                put(1 + turn, angle, 0, m, 0)
                for src, dst in self.enter[0]:
                    if dst == angle:
                        put(1 + turn, src, 0, m, 1)
        return table.astype(jnp.bfloat16)

    @classmethod
    def kinds(cls, device, count):
        step = device // (count // cls.AROUND)
        turned = lax.rem(step + 4, cls.AROUND)
        far = turned >= 8
        other = (turned >= 1) & (turned <= 4)
        early = (step == 4) | ((step > 6) & (step % 2 == 1))
        return jnp.where(far, 0, jnp.where(other, 2, 1)), jnp.where(far, jnp.where(early, 1, 2), 0)

    @classmethod
    def taking_part(cls, device, count):
        step = device // (count // cls.AROUND)
        return (step > 0) & (step < cls.AROUND - 1)


def repack_kernel(lines_ref, first_ref, second_ref, table_ref, out_ref):
    kind, _ = Routes.kinds(lax.axis_index("ang"), lax.axis_size("ang"))
    lines = jnp.concatenate((lines_ref[...], first_ref[...], second_ref[...]), axis=0)
    out = jnp.dot(table_ref[kind], lines, preferred_element_type=jnp.float32)
    out_ref[...] = out.astype(out_ref.dtype)


def pixels_kernel(near_ref, first_ref, second_ref, table_ref, weights_ref, out_ref, lines, *, angles):
    _, kind = Routes.kinds(lax.axis_index("ang"), lax.axis_size("ang"))
    held = jnp.concatenate((near_ref[...], first_ref[...], second_ref[...]), axis=0)
    lines[...] = jnp.dot(table_ref[kind], held, preferred_element_type=jnp.float32)
    cut = lines.shape[0] * LANES // SUB // angles
    per = LANES // cut
    row = lax.broadcasted_iota(jnp.int32, (SUB, LANES), 0)
    lane = lax.broadcasted_iota(jnp.int32, (SUB, LANES), 1)
    turn = (lane // cut + per - row % per) % per
    parts = []
    for group in range(angles // per):
        spread = []
        for q in range(per):
            at = (group * per + q) * (SUB // per)
            low = jnp.broadcast_to(lines[at : at + 1, :], (SUB, LANES))
            high = jnp.broadcast_to(lines[at + 1 : at + 2, :], (SUB, LANES))
            spread.append(jnp.where(row < per, low, high))
        part = None
        for shift in range(per):
            mixed = spread[shift]
            for j in range(1, per):
                mixed = jnp.where(row % per == j, spread[(j + shift) % per], mixed)
            if shift > 0:
                mixed = pltpu.roll(mixed, shift * cut, axis=1)
            part = mixed if shift == 0 else jnp.where(turn == shift, mixed, part)
        parts.append(part.astype(jnp.bfloat16))
    out_ref[...] = jnp.dot(jnp.concatenate(parts, axis=1), weights_ref[...], preferred_element_type=jnp.float32)


def in_hbm(array):
    return pltpu.with_memory_space_constraint(array, pltpu.HBM)


def make_contrast(projections, flats):
    shape = flats.shape
    edge = jax.ShapeDtypeStruct((HALO, shape[1]), halo_type)
    return pl.pallas_call(
        contrast_kernel,
        out_shape=(jax.ShapeDtypeStruct(shape, jnp.float32), edge, edge),
        in_specs=[HBM] * 2,
        out_specs=(VMEM,) * 3,
        scratch_shapes=[
            pltpu.VMEM(projections.shape, projections.dtype),
            pltpu.VMEM(flats.shape, flats.dtype),
            pltpu.SemaphoreType.DMA((2,)),
        ],
        compiler_params=PARAMS,
        name="contrast",
    )(in_hbm(projections), in_hbm(flats))


def make_own(own, turns, forward, inverse, gains, starts):
    groups = turns.shape[1]
    return pl.pallas_call(
        own_kernel,
        out_shape=(
            jax.ShapeDtypeStruct((groups * SUB, 2 * LANES), jnp.float32),
            jax.ShapeDtypeStruct(forward.shape, forward.dtype),
            jax.ShapeDtypeStruct(inverse.shape, inverse.dtype),
            jax.ShapeDtypeStruct((SUB, groups, SUB, LANES), jnp.float32),
            pltpu.SMEM((1, starts.shape[1]), jnp.int32),
        ),
        in_specs=[VMEM] * 3 + [HBM] * 3,
        out_specs=(VMEM,) * 4 + (SMEM,),
        scratch_shapes=[pltpu.SemaphoreType.DMA((3,))],
        compiler_params=PARAMS,
        name="own_rows",
    )(own, turns, gains, in_hbm(forward), in_hbm(inverse), in_hbm(starts))


def make_tile(own_spec, below, above, starts, turns, forward, inverse, gains, cut):
    regions = starts.shape[1]
    return pl.pallas_call(
        tile_kernel,
        out_shape=jax.ShapeDtypeStruct((regions * SUB * cut // LANES, LANES), jnp.bfloat16),
        in_specs=[VMEM] * 3 + [SMEM] + [VMEM] * 4,
        out_specs=VMEM,
        scratch_shapes=[
            pltpu.VMEM((above.shape[1] // LANES + 1, SUB, LANES), jnp.float32),
        ],
        compiler_params=PARAMS,
        name="tile",
    )(own_spec, below, above, starts, turns, forward, inverse, gains)


def make_repack(lines, first, second, table):
    return pl.pallas_call(
        repack_kernel,
        out_shape=jax.ShapeDtypeStruct((table.shape[1], LANES), lines.dtype),
        in_specs=[VMEM] * 4,
        out_specs=VMEM,
        compiler_params=PARAMS,
        name="repack",
    )(lines, first, second, table)


def make_pixels(near, first, second, table, weights):
    angles, cut, pixels = weights.shape
    return pl.pallas_call(
        partial(pixels_kernel, angles=angles),
        out_shape=jax.ShapeDtypeStruct((SUB, pixels), jnp.float32),
        in_specs=[VMEM] * 5,
        out_specs=VMEM,
        scratch_shapes=[pltpu.VMEM((table.shape[1], LANES), jnp.float32)],
        compiler_params=PARAMS,
        name="pixels",
    )(near, first, second, table, weights.reshape(angles * cut, pixels))


def body(projections, flats, block_start, bp_weights):
    angles_dev, rows_dev, width = projections.shape
    cut = bp_weights.shape[1]
    assert angles_dev == 1 and rows_dev == SUB and width % (2 * LANES) == 0 and SUB * cut == 2 * LANES
    rows = lax.axis_size("row")
    up = [(i, i + 1) for i in range(rows - 1)]
    down = [(j, i) for i, j in up]
    turns, forward, inverse, gains = (jnp.asarray(t) for t in tables(width, rows_dev + 2 * HALO))
    own, first, last = make_contrast(projections, flats)
    below = lax.ppermute(first, "row", down)
    above = lax.ppermute(last, "row", up)
    own_spec, forward, inverse, gains, starts = make_own(own, turns, forward, inverse, gains, block_start)
    outgoing = make_tile(own_spec, below, above, starts, turns, forward, inverse, gains, cut)
    routes = Routes(lax.axis_size("ang"))
    relayed = routes.taking_part(lax.axis_index("ang"), routes.count)
    exchange, arrival = jnp.asarray(routes.exchange_table()), jnp.asarray(routes.arrival_table())

    def enter(lines):
        return make_repack(lines, *(lax.ppermute(lines, "ang", pairs) for pairs in routes.enter), exchange)

    def leave(lines):
        return make_pixels(lines, *(lax.ppermute(lines, "ang", pairs) for pairs in routes.leave), arrival, bp_weights)

    packed = lax.cond(relayed, enter, lambda lines: make_repack(lines, lines, lines, exchange), outgoing)
    near = lax.all_to_all(
        packed.reshape(-1, 2, LANES), "ang", split_axis=0, concat_axis=0, tiled=True,
        axis_index_groups=[routes.near, routes.far],
    ).reshape(packed.shape)
    return lax.cond(relayed, leave, lambda lines: make_pixels(lines, lines, lines, arrival, bp_weights), near)


def solution(mesh):
    placed = (P(("scan", "ang"), "row", None), P(("scan", "row"), None), P(), P(None, None, "ang"))
    return jax.shard_map(
        body, mesh=mesh, in_specs=placed, out_specs=P(("scan", "row"), "ang"), check_vma=False
    )
```

```python
from functools import partial

import jax
import jax.numpy as jnp
import numpy as np
from jax import lax
from jax.experimental import pallas as pl
from jax.experimental.pallas import tpu as pltpu
from jax.sharding import PartitionSpec as P

HALO = 4
LANES = 128
SUB = 8

paganin_beta = 8.0
ramp_gain = 320.0
halo_type = jnp.float32
VMEM = pl.BlockSpec(memory_space=pltpu.VMEM)
SMEM = pl.BlockSpec(memory_space=pltpu.SMEM)
HBM = pl.BlockSpec(memory_space=pltpu.HBM)
PARAMS = pltpu.CompilerParams(vmem_limit_bytes=8 * 2**20)


def tables(width, tile_rows):
    blocks = width // LANES
    half = blocks // 2
    lane = np.arange(LANES)
    ks = np.arange(half + 1)
    turn = 2.0 * np.pi / width * (ks[:, None] * lane[None, :])
    turns = np.stack((np.cos(turn), np.sin(turn))).astype(np.float32)
    angle = 2.0 * np.pi / LANES * (lane[:, None] * lane[None, :] % LANES)
    cos, sin = np.cos(angle), np.sin(angle)
    forward = np.block([[cos, -sin], [sin, cos]])

    def split(matrix):
        high = matrix.astype(jnp.bfloat16)
        low = (matrix - high.astype(np.float64)).astype(jnp.bfloat16)
        return np.stack((high, low))

    freq = (ks[:, None] + blocks * lane[None, :]).astype(np.float64)
    row = np.arange(tile_rows, dtype=np.float64)
    lam = 4.0 * np.sin(np.pi * row / tile_rows)[:, None, None] ** 2 + 4.0 * np.sin(np.pi * freq / width) ** 2
    filt = 1.0 / (1.0 + paganin_beta * lam)
    dist = np.arange(tile_rows // 2 + 1)
    gains = np.einsum("du,ukm->dkm", np.cos(2.0 * np.pi / tile_rows * dist[:, None] * row), filt) / tile_rows
    folded = np.minimum(freq, width - freq)
    ramp = ramp_gain * (folded / width) * (0.5 + 0.5 * np.cos(2.0 * np.pi * folded / width))
    twice = np.where((ks == 0) | (ks == half), 1.0, 2.0)
    gains = gains * (ramp * twice[:, None] / width)
    return turns, split(forward), split(forward.T), gains.astype(np.float32)


def plus(terms):
    return sum(terms[1:], terms[0])


def scaled(terms, weights):
    out = None
    for term, weight in zip(terms, weights):
        weight = float(weight)
        if abs(weight) < 1e-12:
            continue
        piece = term if weight == 1.0 else -term if weight == -1.0 else term * weight
        out = piece if out is None else out + piece
    return out


def cosine_sums(terms, blocks):
    half = blocks // 2
    out = [None] * (half + 1)
    for k in range(half // 2 + 1):
        wave = [np.round(np.cos(2.0 * np.pi * a * k / blocks), 15) for a in range(half + 1)]
        even = scaled(terms[0::2], wave[0::2])
        odd = scaled(terms[1::2], wave[1::2])
        out[k] = even if odd is None else even + odd
        if half - k != k:
            out[half - k] = even if odd is None else even - odd
    return out


def sine_sums(terms, blocks):
    half = blocks // 2
    out = [None] * (half + 1)
    for k in range(1, half // 2 + 1):
        wave = [np.round(np.sin(2.0 * np.pi * a * k / blocks), 15) for a in range(half)]
        even = scaled(terms[2:half:2], wave[2::2])
        odd = scaled(terms[1:half:2], wave[1::2])
        if half - k != k:
            out[k] = plus([x for x in (even, odd) if x is not None])
            out[half - k] = odd - even if even is not None else odd
        else:
            out[k] = plus([x for x in (even, odd) if x is not None])
    return out


def accurate_dot(values, matrix_ref):
    high = values.astype(jnp.bfloat16)
    low = (values - high.astype(jnp.float32)).astype(jnp.bfloat16)
    dot = partial(jnp.dot, preferred_element_type=jnp.float32)
    lines = values.shape[0]
    both = dot(jnp.concatenate((high, low), axis=0), matrix_ref[0])
    return both[:lines] + (both[lines:] + dot(high, matrix_ref[1]))


def spectrum(chunks, turns_ref, forward_ref):
    blocks = len(chunks)
    half = blocks // 2
    folds = [chunks[0]] + [chunks[a] + chunks[blocks - a] for a in range(1, half)] + [chunks[half]]
    skews = [None] + [chunks[a] - chunks[blocks - a] for a in range(1, half)] + [None]
    reals = cosine_sums(folds, blocks)
    imags = sine_sums(skews, blocks)
    parts = []
    for k in range(half + 1):
        cos, sin = turns_ref[0, k : k + 1, :], turns_ref[1, k : k + 1, :]
        if k == 0:
            re, im = reals[0], jnp.zeros_like(reals[0])
        elif imags[k] is None:
            re, im = reals[k] * cos, -(reals[k] * sin)
        else:
            re, im = reals[k] * cos - imags[k] * sin, -(imags[k] * cos) - reals[k] * sin
        parts.append(jnp.concatenate((re, im), axis=1))
    return accurate_dot(jnp.concatenate(parts, axis=0), forward_ref)


def columns(spec, turns_ref, inverse_ref, blocks):
    half = blocks // 2
    back = accurate_dot(spec, inverse_ref)
    reals, imags = [], []
    for k in range(half + 1):
        rows = slice(k * SUB, (k + 1) * SUB)
        re, im = back[rows, :LANES], back[rows, LANES:]
        cos, sin = turns_ref[0, k : k + 1, :], turns_ref[1, k : k + 1, :]
        if k == 0:
            reals.append(re)
            imags.append(None)
        else:
            reals.append(re * cos - im * sin)
            imags.append(im * cos + re * sin if k < half else None)
    even = cosine_sums(reals, blocks)
    odd = sine_sums(imags, blocks)
    out = [None] * blocks
    out[0], out[half] = even[0], even[half]
    for a in range(1, half):
        out[a] = even[a] - odd[a]
        out[blocks - a] = even[a] + odd[a]
    return out


def contrast_kernel(proj_hbm, flat_hbm, own_ref, first_ref, last_ref, proj, flat, sems):
    copies = [
        pltpu.make_async_copy(proj_hbm, proj, sems.at[0]),
        pltpu.make_async_copy(flat_hbm, flat, sems.at[1]),
    ]
    for copy in copies:
        copy.start()
    for copy in copies:
        copy.wait()
    own = 1.0 - proj[0].astype(jnp.float32) / flat[...]
    own_ref[...] = own
    first_ref[...] = own[:HALO].astype(first_ref.dtype)
    last_ref[...] = own[SUB - HALO :].astype(last_ref.dtype)


def lanes_of(ref, block):
    return ref[:, block * LANES : (block + 1) * LANES]


def halo_gains(gains_ref, k, row):
    gains = [jnp.broadcast_to(gains_ref[d, k : k + 1, :], (SUB, LANES)) for d in range(2 * HALO + 1)]
    for s in range(SUB):
        far = gains[2 * HALO - abs(s - HALO)]
        near = gains[abs(s - HALO)]
        if s < HALO:
            yield s, jnp.where(row >= s + HALO, near, far)
        else:
            yield s, jnp.where(row < s - HALO, near, far)


def own_kernel(
    own_ref, turns_ref, gains_ref, forward_hbm, inverse_hbm, starts_hbm,
    out_ref, forward_ref, inverse_ref, halo_ref, starts_ref, sems
):
    forward_copy = pltpu.make_async_copy(forward_hbm, forward_ref, sems.at[0])
    inverse_copy = pltpu.make_async_copy(inverse_hbm, inverse_ref, sems.at[1])
    starts_copy = pltpu.make_async_copy(starts_hbm.at[pl.ds(lax.axis_index("ang"), 1)], starts_ref, sems.at[2])
    forward_copy.start()
    inverse_copy.start()
    starts_copy.start()
    row = lax.broadcasted_iota(jnp.int32, (SUB, LANES), 0)
    for k in range(gains_ref.shape[1]):
        for s, gain in halo_gains(gains_ref, k, row):
            halo_ref[s, k] = gain
    forward_copy.wait()
    blocks = own_ref.shape[1] // LANES
    spec = spectrum([lanes_of(own_ref, a) for a in range(blocks)], turns_ref, forward_ref)
    for k in range(blocks // 2 + 1):
        rows = slice(k * SUB, (k + 1) * SUB)
        for side in (slice(0, LANES), slice(LANES, 2 * LANES)):
            here = spec[rows, side]
            moved = [here] + [pltpu.roll(here, s, axis=0) for s in range(1, SUB)]
            total = here * gains_ref[0, k : k + 1, :]
            for d in range(1, SUB):
                pair = jnp.where(row >= d, moved[d], 0.0) + jnp.where(row < SUB - d, moved[SUB - d], 0.0)
                total += pair * gains_ref[d, k : k + 1, :]
            out_ref[rows, side] = total
    inverse_copy.wait()
    starts_copy.wait()


def tile_kernel(
    own_ref, below_ref, above_ref, starts, turns_ref, forward_ref, inverse_ref, gains_ref, out_ref,
    sheet
):
    blocks = above_ref.shape[1] // LANES
    halo = [
        jnp.concatenate((lanes_of(above_ref, a), lanes_of(below_ref, a)), axis=0).astype(jnp.float32)
        for a in range(blocks)
    ]
    spec = spectrum(halo, turns_ref, forward_ref)
    row = lax.broadcasted_iota(jnp.int32, (SUB, LANES), 0)
    lane = lax.broadcasted_iota(jnp.int32, (SUB, LANES), 1)
    parts = []
    for k in range(blocks // 2 + 1):
        rows = slice(k * SUB, (k + 1) * SUB)
        both = []
        for side in (slice(0, LANES), slice(LANES, 2 * LANES)):
            here = spec[rows, side]
            total = own_ref[rows, side] + here * gains_ref[0, k]
            for s in range(1, SUB):
                total += pltpu.roll(here, s, axis=0) * gains_ref[s, k]
            both.append(total)
        parts.append(jnp.concatenate(both, axis=1))
    filtered = columns(jnp.concatenate(parts, axis=0), turns_ref, inverse_ref, blocks)
    for a in range(blocks):
        sheet[a] = filtered[a]
    regions = starts.shape[1]
    cut = out_ref.shape[0] * LANES // (regions * SUB)
    per = LANES // cut
    keep = lane // cut == row % per
    packed = []
    for group in range(regions // per):
        gathered = None
        for q in range(per):
            start = starts[0, group * per + q]
            block = lax.shift_right_logical(start, 7)
            offset = start & (LANES - 1)
            window = jnp.where(lane >= offset, sheet[block], sheet[block + 1])
            window = pltpu.roll(window, (LANES + q * cut - offset) & (LANES - 1), axis=1)
            gathered = window if q == 0 else jnp.where(lane // cut == q, window, gathered)
        for shift in range(per):
            moved = gathered if shift == 0 else pltpu.roll(gathered, shift * cut, axis=1)
            packed.append(jnp.where(keep, moved, 0.0).astype(jnp.bfloat16))
    lines = out_ref.shape[0]
    want = lax.broadcasted_iota(jnp.int32, (lines, regions * SUB), 0)
    have = lax.broadcasted_iota(jnp.int32, (lines, regions * SUB), 1)
    have_row, have_shift, have_group = have % SUB, have // SUB % per, have // (SUB * per)
    have_region = have_group * per + (have_row % per + per - have_shift) % per
    pick = jnp.where(have_region * (SUB // per) + have_row // per == want, 1.0, 0.0).astype(jnp.bfloat16)
    out = jnp.dot(pick, jnp.concatenate(packed, axis=0), preferred_element_type=jnp.float32)
    out_ref[...] = out.astype(jnp.bfloat16)


class Routes:
    UNITS = 4
    AROUND = 16

    def __init__(self, count):
        step = count // self.AROUND
        devices = lambda steps: [s * step + c for s in steps for c in range(step)]
        link = lambda pairs: [p for src, dst in pairs for p in zip(devices([src]), devices([dst]))]
        self.count, self.half = count, count // 2
        self.near = devices((12, 13, 14, 15, 0, 1, 2, 3))
        self.far = devices(range(4, 12))
        self.relays = devices((1, 2, 3))
        self.swaps = 0
        self.enter = [
            link(((5, 2), (4, 3), (1, 6), (2, 5), (3, 4))),
            link(((10, 1), (8, 2), (6, 3))),
            link(((11, 1), (9, 2), (7, 3))),
        ]
        self.leave = [link(((12, 11), (13, 9), (14, 7), (3, 4))), link(((12, 10), (13, 8), (14, 6), (3, 5)))]

    def exchange_table(self):
        table = np.zeros((3, self.half * self.UNITS * 2, (1 + len(self.enter)) * self.count * 2), np.float32)

        def put(kind, m, unit, source, region):
            for i in range(2):
                table[kind, (m * self.UNITS + unit) * 2 + i, (source * self.count + region) * 2 + i] = 1.0

        for m, dest in enumerate(self.far):
            put(0, m, 0, 0, dest)
            put(0, m, 1, 1 + self.swaps, dest)
        for m, dest in enumerate(self.near):
            put(1, m, 0, 0, dest)
            put(2, m, 0, 0, dest)
            for turn in range(len(self.enter)):
                put(1, m, 1 + turn, 1 + turn, dest)
            for turn in range(len(self.leave)):
                for src, final in self.leave[turn]:
                    if src == dest:
                        put(2, m, 1 + turn, 0, final)
        return table.astype(jnp.bfloat16)

    def arrival_table(self):
        size = self.half * self.UNITS
        table = np.zeros((3, self.count * 2, 3 * size * 2), np.float32)

        def put(kind, angle, source, m, unit):
            for i in range(2):
                table[kind, angle * 2 + i, (source * size + m * self.UNITS + unit) * 2 + i] = 1.0

        for m, angle in enumerate(self.near):
            put(0, angle, 0, m, 0)
            for turn in range(len(self.enter)):
                for src, dst in self.enter[turn]:
                    if dst == angle:
                        put(0, src, 0, m, 1 + turn)
            for turn in range(len(self.leave)):
                if angle not in self.relays:
                    put(1 + turn, angle, 1 + turn, m, 1 + turn)
        for m, angle in enumerate(self.far):
            for turn in range(len(self.leave)):
                put(1 + turn, angle, 0, m, 0)
                for src, dst in self.enter[self.swaps]:
                    if dst == angle:
                        put(1 + turn, src, 0, m, 1)
        return table.astype(jnp.bfloat16)

    @classmethod
    def kinds(cls, device, count):
        step = device // (count // cls.AROUND)
        turned = lax.rem(step + 4, cls.AROUND)
        far = turned >= 8
        other = turned <= 4
        early = (step == 4) | ((step > 6) & (step % 2 == 1))
        return jnp.where(far, 0, jnp.where(other, 2, 1)), jnp.where(far, jnp.where(early, 1, 2), 0)

    @classmethod
    def taking_part(cls, device, count):
        step = device // (count // cls.AROUND)
        return (step > 0) & (step < cls.AROUND - 1)


def repack_kernel(lines_ref, first_ref, second_ref, third_ref, table_ref, out_ref):
    kind, _ = Routes.kinds(lax.axis_index("ang"), lax.axis_size("ang"))
    lines = jnp.concatenate((lines_ref[...], first_ref[...], second_ref[...], third_ref[...]), axis=0)
    out = jnp.dot(table_ref[kind], lines, preferred_element_type=jnp.float32)
    out_ref[...] = out.astype(out_ref.dtype)


def pixels_kernel(near_ref, first_ref, second_ref, table_ref, weights_ref, out_ref, lines, *, angles):
    _, kind = Routes.kinds(lax.axis_index("ang"), lax.axis_size("ang"))
    held = jnp.concatenate((near_ref[...], first_ref[...], second_ref[...]), axis=0)
    lines[...] = jnp.dot(table_ref[kind], held, preferred_element_type=jnp.float32)
    cut = lines.shape[0] * LANES // SUB // angles
    per = LANES // cut
    row = lax.broadcasted_iota(jnp.int32, (SUB, LANES), 0)
    lane = lax.broadcasted_iota(jnp.int32, (SUB, LANES), 1)
    turn = (lane // cut + per - row % per) % per
    parts = []
    for group in range(angles // per):
        spread = []
        for q in range(per):
            at = (group * per + q) * (SUB // per)
            low = jnp.broadcast_to(lines[at : at + 1, :], (SUB, LANES))
            high = jnp.broadcast_to(lines[at + 1 : at + 2, :], (SUB, LANES))
            spread.append(jnp.where(row < per, low, high))
        part = None
        for shift in range(per):
            mixed = spread[shift]
            for j in range(1, per):
                mixed = jnp.where(row % per == j, spread[(j + shift) % per], mixed)
            if shift > 0:
                mixed = pltpu.roll(mixed, shift * cut, axis=1)
            part = mixed if shift == 0 else jnp.where(turn == shift, mixed, part)
        parts.append(part.astype(jnp.bfloat16))
    out_ref[...] = jnp.dot(jnp.concatenate(parts, axis=1), weights_ref[...], preferred_element_type=jnp.float32)


def in_hbm(array):
    return pltpu.with_memory_space_constraint(array, pltpu.HBM)


def make_contrast(projections, flats):
    shape = flats.shape
    edge = jax.ShapeDtypeStruct((HALO, shape[1]), halo_type)
    return pl.pallas_call(
        contrast_kernel,
        out_shape=(jax.ShapeDtypeStruct(shape, jnp.float32), edge, edge),
        in_specs=[HBM] * 2,
        out_specs=(VMEM,) * 3,
        scratch_shapes=[
            pltpu.VMEM(projections.shape, projections.dtype),
            pltpu.VMEM(flats.shape, flats.dtype),
            pltpu.SemaphoreType.DMA((2,)),
        ],
        compiler_params=PARAMS,
        name="contrast",
    )(in_hbm(projections), in_hbm(flats))


def make_own(own, turns, forward, inverse, gains, starts):
    groups = turns.shape[1]
    return pl.pallas_call(
        own_kernel,
        out_shape=(
            jax.ShapeDtypeStruct((groups * SUB, 2 * LANES), jnp.float32),
            jax.ShapeDtypeStruct(forward.shape, forward.dtype),
            jax.ShapeDtypeStruct(inverse.shape, inverse.dtype),
            jax.ShapeDtypeStruct((SUB, groups, SUB, LANES), jnp.float32),
            pltpu.SMEM((1, starts.shape[1]), jnp.int32),
        ),
        in_specs=[VMEM] * 3 + [HBM] * 3,
        out_specs=(VMEM,) * 4 + (SMEM,),
        scratch_shapes=[pltpu.SemaphoreType.DMA((3,))],
        compiler_params=PARAMS,
        name="own_rows",
    )(own, turns, gains, in_hbm(forward), in_hbm(inverse), in_hbm(starts))


def make_tile(own_spec, below, above, starts, turns, forward, inverse, gains, cut):
    regions = starts.shape[1]
    return pl.pallas_call(
        tile_kernel,
        out_shape=jax.ShapeDtypeStruct((regions * SUB * cut // LANES, LANES), jnp.bfloat16),
        in_specs=[VMEM] * 3 + [SMEM] + [VMEM] * 4,
        out_specs=VMEM,
        scratch_shapes=[
            pltpu.VMEM((above.shape[1] // LANES + 1, SUB, LANES), jnp.float32),
        ],
        compiler_params=PARAMS,
        name="tile",
    )(own_spec, below, above, starts, turns, forward, inverse, gains)


def make_repack(lines, first, second, third, table):
    return pl.pallas_call(
        repack_kernel,
        out_shape=jax.ShapeDtypeStruct((table.shape[1], LANES), lines.dtype),
        in_specs=[VMEM] * 5,
        out_specs=VMEM,
        compiler_params=PARAMS,
        name="repack",
    )(lines, first, second, third, table)


def make_pixels(near, first, second, table, weights):
    angles, cut, pixels = weights.shape
    return pl.pallas_call(
        partial(pixels_kernel, angles=angles),
        out_shape=jax.ShapeDtypeStruct((SUB, pixels), jnp.float32),
        in_specs=[VMEM] * 5,
        out_specs=VMEM,
        scratch_shapes=[pltpu.VMEM((table.shape[1], LANES), jnp.float32)],
        compiler_params=PARAMS,
        name="pixels",
    )(near, first, second, table, weights.reshape(angles * cut, pixels))


def body(projections, flats, block_start, bp_weights):
    angles_dev, rows_dev, width = projections.shape
    cut = bp_weights.shape[1]
    assert angles_dev == 1 and rows_dev == SUB and width % (2 * LANES) == 0 and SUB * cut == 2 * LANES
    rows = lax.axis_size("row")
    up = [(i, i + 1) for i in range(rows - 1)]
    down = [(j, i) for i, j in up]
    turns, forward, inverse, gains = (jnp.asarray(t) for t in tables(width, rows_dev + 2 * HALO))
    own, first, last = make_contrast(projections, flats)
    below = lax.ppermute(first, "row", down)
    above = lax.ppermute(last, "row", up)
    own_spec, forward, inverse, gains, starts = make_own(own, turns, forward, inverse, gains, block_start)
    outgoing = make_tile(own_spec, below, above, starts, turns, forward, inverse, gains, cut)
    routes = Routes(lax.axis_size("ang"))
    relayed = routes.taking_part(lax.axis_index("ang"), routes.count)
    exchange, arrival = jnp.asarray(routes.exchange_table()), jnp.asarray(routes.arrival_table())

    def enter(lines):
        return make_repack(lines, *(lax.ppermute(lines, "ang", pairs) for pairs in routes.enter), exchange)

    def leave(lines):
        return make_pixels(lines, *(lax.ppermute(lines, "ang", pairs) for pairs in routes.leave), arrival, bp_weights)

    packed = lax.cond(relayed, enter, lambda lines: make_repack(lines, lines, lines, lines, exchange), outgoing)
    near = lax.all_to_all(
        packed.reshape(-1, 2, LANES), "ang", split_axis=0, concat_axis=0, tiled=True,
        axis_index_groups=[routes.near, routes.far],
    ).reshape(packed.shape)
    return lax.cond(relayed, leave, lambda lines: make_pixels(lines, lines, lines, arrival, bp_weights), near)


def solution(mesh):
    placed = (P(("scan", "ang"), "row", None), P(("scan", "row"), None), P(), P(None, None, "ang"))
    return jax.shard_map(
        body, mesh=mesh, in_specs=placed, out_specs=P(("scan", "row"), "ang"), check_vma=False
    )
```

```python
from functools import partial

import jax
import jax.numpy as jnp
import numpy as np
from jax import lax
from jax.experimental import pallas as pl
from jax.experimental.pallas import tpu as pltpu
from jax.sharding import PartitionSpec as P

HALO = 4
LANES = 128
SUB = 8

paganin_beta = 8.0
ramp_gain = 320.0
halo_type = jnp.float32
VMEM = pl.BlockSpec(memory_space=pltpu.VMEM)
SMEM = pl.BlockSpec(memory_space=pltpu.SMEM)
HBM = pl.BlockSpec(memory_space=pltpu.HBM)
PARAMS = pltpu.CompilerParams(vmem_limit_bytes=8 * 2**20)


def tables(width, tile_rows):
    blocks = width // LANES
    half = blocks // 2
    lane = np.arange(LANES)
    ks = np.arange(half + 1)
    turn = 2.0 * np.pi / width * (ks[:, None] * lane[None, :])
    turns = np.stack((np.cos(turn), np.sin(turn))).astype(np.float32)
    angle = 2.0 * np.pi / LANES * (lane[:, None] * lane[None, :] % LANES)
    cos, sin = np.cos(angle), np.sin(angle)
    forward = np.block([[cos, -sin], [sin, cos]])

    def split(matrix):
        high = matrix.astype(jnp.bfloat16)
        low = (matrix - high.astype(np.float64)).astype(jnp.bfloat16)
        return np.stack((high, low))

    freq = (ks[:, None] + blocks * lane[None, :]).astype(np.float64)
    row = np.arange(tile_rows, dtype=np.float64)
    lam = 4.0 * np.sin(np.pi * row / tile_rows)[:, None, None] ** 2 + 4.0 * np.sin(np.pi * freq / width) ** 2
    filt = 1.0 / (1.0 + paganin_beta * lam)
    dist = np.arange(tile_rows // 2 + 1)
    gains = np.einsum("du,ukm->dkm", np.cos(2.0 * np.pi / tile_rows * dist[:, None] * row), filt) / tile_rows
    folded = np.minimum(freq, width - freq)
    ramp = ramp_gain * (folded / width) * (0.5 + 0.5 * np.cos(2.0 * np.pi * folded / width))
    twice = np.where((ks == 0) | (ks == half), 1.0, 2.0)
    gains = gains * (ramp * twice[:, None] / width)
    return turns, split(forward), split(forward.T), gains.astype(np.float32)


def plus(terms):
    return sum(terms[1:], terms[0])


def scaled(terms, weights):
    out = None
    for term, weight in zip(terms, weights):
        weight = float(weight)
        if abs(weight) < 1e-12:
            continue
        piece = term if weight == 1.0 else -term if weight == -1.0 else term * weight
        out = piece if out is None else out + piece
    return out


def cosine_sums(terms, blocks):
    half = blocks // 2
    out = [None] * (half + 1)
    for k in range(half // 2 + 1):
        wave = [np.round(np.cos(2.0 * np.pi * a * k / blocks), 15) for a in range(half + 1)]
        even = scaled(terms[0::2], wave[0::2])
        odd = scaled(terms[1::2], wave[1::2])
        out[k] = even if odd is None else even + odd
        if half - k != k:
            out[half - k] = even if odd is None else even - odd
    return out


def sine_sums(terms, blocks):
    half = blocks // 2
    out = [None] * (half + 1)
    for k in range(1, half // 2 + 1):
        wave = [np.round(np.sin(2.0 * np.pi * a * k / blocks), 15) for a in range(half)]
        even = scaled(terms[2:half:2], wave[2::2])
        odd = scaled(terms[1:half:2], wave[1::2])
        if half - k != k:
            out[k] = plus([x for x in (even, odd) if x is not None])
            out[half - k] = odd - even if even is not None else odd
        else:
            out[k] = plus([x for x in (even, odd) if x is not None])
    return out


def accurate_dot(values, matrix_ref):
    high = values.astype(jnp.bfloat16)
    low = (values - high.astype(jnp.float32)).astype(jnp.bfloat16)
    dot = partial(jnp.dot, preferred_element_type=jnp.float32)
    lines = values.shape[0]
    both = dot(jnp.concatenate((high, low), axis=0), matrix_ref[0])
    return both[:lines] + (both[lines:] + dot(high, matrix_ref[1]))


def spectrum(chunks, turns_ref, forward_ref):
    blocks = len(chunks)
    half = blocks // 2
    folds = [chunks[0]] + [chunks[a] + chunks[blocks - a] for a in range(1, half)] + [chunks[half]]
    skews = [None] + [chunks[a] - chunks[blocks - a] for a in range(1, half)] + [None]
    reals = cosine_sums(folds, blocks)
    imags = sine_sums(skews, blocks)
    parts = []
    for k in range(half + 1):
        cos, sin = turns_ref[0, k : k + 1, :], turns_ref[1, k : k + 1, :]
        if k == 0:
            re, im = reals[0], jnp.zeros_like(reals[0])
        elif imags[k] is None:
            re, im = reals[k] * cos, -(reals[k] * sin)
        else:
            re, im = reals[k] * cos - imags[k] * sin, -(imags[k] * cos) - reals[k] * sin
        parts.append(jnp.concatenate((re, im), axis=1))
    return accurate_dot(jnp.concatenate(parts, axis=0), forward_ref)


def columns(spec, turns_ref, inverse_ref, blocks):
    half = blocks // 2
    back = accurate_dot(spec, inverse_ref)
    reals, imags = [], []
    for k in range(half + 1):
        rows = slice(k * SUB, (k + 1) * SUB)
        re, im = back[rows, :LANES], back[rows, LANES:]
        cos, sin = turns_ref[0, k : k + 1, :], turns_ref[1, k : k + 1, :]
        if k == 0:
            reals.append(re)
            imags.append(None)
        else:
            reals.append(re * cos - im * sin)
            imags.append(im * cos + re * sin if k < half else None)
    even = cosine_sums(reals, blocks)
    odd = sine_sums(imags, blocks)
    out = [None] * blocks
    out[0], out[half] = even[0], even[half]
    for a in range(1, half):
        out[a] = even[a] - odd[a]
        out[blocks - a] = even[a] + odd[a]
    return out


def contrast_kernel(proj_hbm, flat_hbm, own_ref, first_ref, last_ref, proj, flat, sems):
    copies = [
        pltpu.make_async_copy(proj_hbm, proj, sems.at[0]),
        pltpu.make_async_copy(flat_hbm, flat, sems.at[1]),
    ]
    for copy in copies:
        copy.start()
    for copy in copies:
        copy.wait()
    own = 1.0 - proj[0].astype(jnp.float32) / flat[...]
    own_ref[...] = own
    first_ref[...] = own[:HALO].astype(first_ref.dtype)
    last_ref[...] = own[SUB - HALO :].astype(last_ref.dtype)


def lanes_of(ref, block):
    return ref[:, block * LANES : (block + 1) * LANES]


def halo_gains(gains_ref, k, row):
    gains = [jnp.broadcast_to(gains_ref[d, k : k + 1, :], (SUB, LANES)) for d in range(2 * HALO + 1)]
    for s in range(SUB):
        far = gains[2 * HALO - abs(s - HALO)]
        near = gains[abs(s - HALO)]
        if s < HALO:
            yield s, jnp.where(row >= s + HALO, near, far)
        else:
            yield s, jnp.where(row < s - HALO, near, far)


def own_kernel(
    own_ref, turns_ref, gains_ref, forward_hbm, inverse_hbm, starts_hbm, exchange_hbm,
    out_ref, forward_ref, inverse_ref, halo_ref, starts_ref, exchange_ref, sems
):
    forward_copy = pltpu.make_async_copy(forward_hbm, forward_ref, sems.at[0])
    inverse_copy = pltpu.make_async_copy(inverse_hbm, inverse_ref, sems.at[1])
    starts_copy = pltpu.make_async_copy(starts_hbm.at[pl.ds(lax.axis_index("ang"), 1)], starts_ref, sems.at[2])
    forward_copy.start()
    inverse_copy.start()
    starts_copy.start()
    exchange_copy = pltpu.make_async_copy(exchange_hbm, exchange_ref, sems.at[3])
    exchange_copy.start()
    row = lax.broadcasted_iota(jnp.int32, (SUB, LANES), 0)
    for k in range(gains_ref.shape[1]):
        for s, gain in halo_gains(gains_ref, k, row):
            halo_ref[s, k] = gain
    forward_copy.wait()
    blocks = own_ref.shape[1] // LANES
    spec = spectrum([lanes_of(own_ref, a) for a in range(blocks)], turns_ref, forward_ref)
    for k in range(blocks // 2 + 1):
        rows = slice(k * SUB, (k + 1) * SUB)
        for side in (slice(0, LANES), slice(LANES, 2 * LANES)):
            here = spec[rows, side]
            moved = [here] + [pltpu.roll(here, s, axis=0) for s in range(1, SUB)]
            total = here * gains_ref[0, k : k + 1, :]
            for d in range(1, SUB):
                pair = jnp.where(row >= d, moved[d], 0.0) + jnp.where(row < SUB - d, moved[SUB - d], 0.0)
                total += pair * gains_ref[d, k : k + 1, :]
            out_ref[rows, side] = total
    inverse_copy.wait()
    starts_copy.wait()
    exchange_copy.wait()


def tile_kernel(
    own_ref, below_ref, above_ref, starts, turns_ref, forward_ref, inverse_ref, gains_ref, out_ref,
    sheet
):
    blocks = above_ref.shape[1] // LANES
    halo = [
        jnp.concatenate((lanes_of(above_ref, a), lanes_of(below_ref, a)), axis=0).astype(jnp.float32)
        for a in range(blocks)
    ]
    spec = spectrum(halo, turns_ref, forward_ref)
    row = lax.broadcasted_iota(jnp.int32, (SUB, LANES), 0)
    lane = lax.broadcasted_iota(jnp.int32, (SUB, LANES), 1)
    parts = []
    for k in range(blocks // 2 + 1):
        rows = slice(k * SUB, (k + 1) * SUB)
        both = []
        for side in (slice(0, LANES), slice(LANES, 2 * LANES)):
            here = spec[rows, side]
            total = own_ref[rows, side] + here * gains_ref[0, k]
            for s in range(1, SUB):
                total += pltpu.roll(here, s, axis=0) * gains_ref[s, k]
            both.append(total)
        parts.append(jnp.concatenate(both, axis=1))
    filtered = columns(jnp.concatenate(parts, axis=0), turns_ref, inverse_ref, blocks)
    for a in range(blocks):
        sheet[a] = filtered[a]
    regions = starts.shape[1]
    cut = out_ref.shape[0] * LANES // (regions * SUB)
    per = LANES // cut
    keep = lane // cut == row % per
    packed = []
    for group in range(regions // per):
        gathered = None
        for q in range(per):
            start = starts[0, group * per + q]
            block = lax.shift_right_logical(start, 7)
            offset = start & (LANES - 1)
            window = jnp.where(lane >= offset, sheet[block], sheet[block + 1])
            window = pltpu.roll(window, (LANES + q * cut - offset) & (LANES - 1), axis=1)
            gathered = window if q == 0 else jnp.where(lane // cut == q, window, gathered)
        for shift in range(per):
            moved = gathered if shift == 0 else pltpu.roll(gathered, shift * cut, axis=1)
            packed.append(jnp.where(keep, moved, 0.0).astype(jnp.bfloat16))
    lines = out_ref.shape[0]
    want = lax.broadcasted_iota(jnp.int32, (lines, regions * SUB), 0)
    have = lax.broadcasted_iota(jnp.int32, (lines, regions * SUB), 1)
    have_row, have_shift, have_group = have % SUB, have // SUB % per, have // (SUB * per)
    have_region = have_group * per + (have_row % per + per - have_shift) % per
    pick = jnp.where(have_region * (SUB // per) + have_row // per == want, 1.0, 0.0).astype(jnp.bfloat16)
    out = jnp.dot(pick, jnp.concatenate(packed, axis=0), preferred_element_type=jnp.float32)
    out_ref[...] = out.astype(jnp.bfloat16)


class Routes:
    UNITS = 4
    AROUND = 16

    def __init__(self, count):
        step = count // self.AROUND
        devices = lambda steps: [s * step + c for s in steps for c in range(step)]
        link = lambda pairs: [p for src, dst in pairs for p in zip(devices([src]), devices([dst]))]
        self.count, self.half = count, count // 2
        self.near = devices((12, 13, 14, 15, 0, 1, 2, 3))
        self.far = devices(range(4, 12))
        self.relays = devices((1, 2, 3))
        self.swaps = 0
        self.enter = [
            link(((5, 2), (4, 3), (1, 6), (2, 5), (3, 4))),
            link(((10, 1), (8, 2), (6, 3))),
            link(((11, 1), (9, 2), (7, 3))),
        ]
        self.leave = [link(((12, 11), (13, 9), (14, 7), (3, 4))), link(((12, 10), (13, 8), (14, 6), (3, 5)))]

    def exchange_table(self):
        table = np.zeros((3, self.half * self.UNITS * 2, (1 + len(self.enter)) * self.count * 2), np.float32)

        def put(kind, m, unit, source, region):
            for i in range(2):
                table[kind, (m * self.UNITS + unit) * 2 + i, (source * self.count + region) * 2 + i] = 1.0

        for m, dest in enumerate(self.far):
            put(0, m, 0, 0, dest)
            put(0, m, 1, 1 + self.swaps, dest)
        for m, dest in enumerate(self.near):
            put(1, m, 0, 0, dest)
            put(2, m, 0, 0, dest)
            for turn in range(len(self.enter)):
                put(1, m, 1 + turn, 1 + turn, dest)
            for turn in range(len(self.leave)):
                for src, final in self.leave[turn]:
                    if src == dest:
                        put(2, m, 1 + turn, 0, final)
        return table.astype(jnp.bfloat16)

    def arrival_table(self):
        size = self.half * self.UNITS
        table = np.zeros((3, self.count * 2, 3 * size * 2), np.float32)

        def put(kind, angle, source, m, unit):
            for i in range(2):
                table[kind, angle * 2 + i, (source * size + m * self.UNITS + unit) * 2 + i] = 1.0

        for m, angle in enumerate(self.near):
            put(0, angle, 0, m, 0)
            for turn in range(len(self.enter)):
                for src, dst in self.enter[turn]:
                    if dst == angle:
                        put(0, src, 0, m, 1 + turn)
            for turn in range(len(self.leave)):
                if angle not in self.relays:
                    put(1 + turn, angle, 1 + turn, m, 1 + turn)
        for m, angle in enumerate(self.far):
            for turn in range(len(self.leave)):
                put(1 + turn, angle, 0, m, 0)
                for src, dst in self.enter[self.swaps]:
                    if dst == angle:
                        put(1 + turn, src, 0, m, 1)
        return table.astype(jnp.bfloat16)

    @classmethod
    def kinds(cls, device, count):
        step = device // (count // cls.AROUND)
        turned = lax.rem(step + 4, cls.AROUND)
        far = turned >= 8
        other = turned <= 4
        early = (step == 4) | ((step > 6) & (step % 2 == 1))
        return jnp.where(far, 0, jnp.where(other, 2, 1)), jnp.where(far, jnp.where(early, 1, 2), 0)

    @classmethod
    def taking_part(cls, device, count):
        step = device // (count // cls.AROUND)
        return (step > 0) & (step < cls.AROUND - 1)


def repack_kernel(lines_ref, first_ref, second_ref, third_ref, table_ref, out_ref):
    kind, _ = Routes.kinds(lax.axis_index("ang"), lax.axis_size("ang"))
    lines = jnp.concatenate((lines_ref[...], first_ref[...], second_ref[...], third_ref[...]), axis=0)
    out = jnp.dot(table_ref[kind], lines, preferred_element_type=jnp.float32)
    out_ref[...] = out.astype(out_ref.dtype)


def pixels_kernel(*refs, angles):
    _, kind = Routes.kinds(lax.axis_index("ang"), lax.axis_size("ang"))
    *held_refs, table_ref, weights_ref, out_ref, lines = refs
    held = jnp.concatenate([ref[...] for ref in held_refs], axis=0)
    table = table_ref[kind if len(held_refs) > 1 else 0, :, : held.shape[0]]
    lines[...] = jnp.dot(table, held, preferred_element_type=jnp.float32)
    cut = lines.shape[0] * LANES // SUB // angles
    per = LANES // cut
    row = lax.broadcasted_iota(jnp.int32, (SUB, LANES), 0)
    lane = lax.broadcasted_iota(jnp.int32, (SUB, LANES), 1)
    turn = (lane // cut + per - row % per) % per
    parts = []
    for group in range(angles // per):
        spread = []
        for q in range(per):
            at = (group * per + q) * (SUB // per)
            low = jnp.broadcast_to(lines[at : at + 1, :], (SUB, LANES))
            high = jnp.broadcast_to(lines[at + 1 : at + 2, :], (SUB, LANES))
            spread.append(jnp.where(row < per, low, high))
        part = None
        for shift in range(per):
            mixed = spread[shift]
            for j in range(1, per):
                mixed = jnp.where(row % per == j, spread[(j + shift) % per], mixed)
            if shift > 0:
                mixed = pltpu.roll(mixed, shift * cut, axis=1)
            part = mixed if shift == 0 else jnp.where(turn == shift, mixed, part)
        parts.append(part.astype(jnp.bfloat16))
    out_ref[...] = jnp.dot(jnp.concatenate(parts, axis=1), weights_ref[...], preferred_element_type=jnp.float32)


def in_hbm(array):
    return pltpu.with_memory_space_constraint(array, pltpu.HBM)


def make_contrast(projections, flats):
    shape = flats.shape
    edge = jax.ShapeDtypeStruct((HALO, shape[1]), halo_type)
    return pl.pallas_call(
        contrast_kernel,
        out_shape=(jax.ShapeDtypeStruct(shape, jnp.float32), edge, edge),
        in_specs=[HBM] * 2,
        out_specs=(VMEM,) * 3,
        scratch_shapes=[
            pltpu.VMEM(projections.shape, projections.dtype),
            pltpu.VMEM(flats.shape, flats.dtype),
            pltpu.SemaphoreType.DMA((2,)),
        ],
        compiler_params=PARAMS,
        name="contrast",
    )(in_hbm(projections), in_hbm(flats))


def make_own(own, turns, forward, inverse, gains, starts, exchange):
    groups = turns.shape[1]
    return pl.pallas_call(
        own_kernel,
        out_shape=(
            jax.ShapeDtypeStruct((groups * SUB, 2 * LANES), jnp.float32),
            jax.ShapeDtypeStruct(forward.shape, forward.dtype),
            jax.ShapeDtypeStruct(inverse.shape, inverse.dtype),
            jax.ShapeDtypeStruct((SUB, groups, SUB, LANES), jnp.float32),
            pltpu.SMEM((1, starts.shape[1]), jnp.int32),
            jax.ShapeDtypeStruct(exchange.shape, exchange.dtype),
        ),
        in_specs=[VMEM] * 3 + [HBM] * 4,
        out_specs=(VMEM,) * 4 + (SMEM, VMEM),
        scratch_shapes=[pltpu.SemaphoreType.DMA((4,))],
        compiler_params=PARAMS,
        name="own_rows",
    )(own, turns, gains, in_hbm(forward), in_hbm(inverse), in_hbm(starts), in_hbm(exchange))


def make_tile(own_spec, below, above, starts, turns, forward, inverse, gains, cut):
    regions = starts.shape[1]
    return pl.pallas_call(
        tile_kernel,
        out_shape=jax.ShapeDtypeStruct((regions * SUB * cut // LANES, LANES), jnp.bfloat16),
        in_specs=[VMEM] * 3 + [SMEM] + [VMEM] * 4,
        out_specs=VMEM,
        scratch_shapes=[
            pltpu.VMEM((above.shape[1] // LANES + 1, SUB, LANES), jnp.float32),
        ],
        compiler_params=PARAMS,
        name="tile",
    )(own_spec, below, above, starts, turns, forward, inverse, gains)


def make_repack(lines, first, second, third, table):
    return pl.pallas_call(
        repack_kernel,
        out_shape=jax.ShapeDtypeStruct((table.shape[1], LANES), lines.dtype),
        in_specs=[VMEM] * 5,
        out_specs=VMEM,
        compiler_params=PARAMS,
        name="repack",
    )(lines, first, second, third, table)


def make_pixels(held, table, weights):
    angles, cut, pixels = weights.shape
    return pl.pallas_call(
        partial(pixels_kernel, angles=angles),
        out_shape=jax.ShapeDtypeStruct((SUB, pixels), jnp.float32),
        in_specs=[VMEM] * (len(held) + 2),
        out_specs=VMEM,
        scratch_shapes=[pltpu.VMEM((table.shape[1], LANES), jnp.float32)],
        compiler_params=PARAMS,
        name="pixels",
    )(*held, table, weights.reshape(angles * cut, pixels))


def body(projections, flats, block_start, bp_weights):
    angles_dev, rows_dev, width = projections.shape
    cut = bp_weights.shape[1]
    assert angles_dev == 1 and rows_dev == SUB and width % (2 * LANES) == 0 and SUB * cut == 2 * LANES
    rows = lax.axis_size("row")
    up = [(i, i + 1) for i in range(rows - 1)]
    down = [(j, i) for i, j in up]
    turns, forward, inverse, gains = (jnp.asarray(t) for t in tables(width, rows_dev + 2 * HALO))
    own, first, last = make_contrast(projections, flats)
    below = lax.ppermute(first, "row", down)
    above = lax.ppermute(last, "row", up)
    routes = Routes(lax.axis_size("ang"))
    exchange, arrival = jnp.asarray(routes.exchange_table()), jnp.asarray(routes.arrival_table())
    own_spec, forward, inverse, gains, starts, exchange = make_own(
        own, turns, forward, inverse, gains, block_start, exchange
    )
    outgoing = make_tile(own_spec, below, above, starts, turns, forward, inverse, gains, cut)
    relayed = routes.taking_part(lax.axis_index("ang"), routes.count)

    def enter(lines):
        return make_repack(lines, *(lax.ppermute(lines, "ang", pairs) for pairs in routes.enter), exchange)

    def leave(lines):
        return make_pixels([lines, *(lax.ppermute(lines, "ang", pairs) for pairs in routes.leave)], arrival, bp_weights)

    packed = lax.cond(relayed, enter, lambda lines: make_repack(lines, lines, lines, lines, exchange), outgoing)
    near = lax.all_to_all(
        packed.reshape(-1, 2, LANES), "ang", split_axis=0, concat_axis=0, tiled=True,
        axis_index_groups=[routes.near, routes.far],
    ).reshape(packed.shape)
    return lax.cond(relayed, leave, lambda lines: make_pixels([lines], arrival, bp_weights), near)


def solution(mesh):
    placed = (P(("scan", "ang"), "row", None), P(("scan", "row"), None), P(), P(None, None, "ang"))
    return jax.shard_map(
        body, mesh=mesh, in_specs=placed, out_specs=P(("scan", "row"), "ang"), check_vma=False
    )
```

```python
from functools import partial

import jax
import jax.numpy as jnp
import numpy as np
from jax import lax
from jax.experimental import pallas as pl
from jax.experimental.pallas import tpu as pltpu
from jax.sharding import PartitionSpec as P

HALO = 4
LANES = 128
SUB = 8

paganin_beta = 8.0
ramp_gain = 320.0
halo_type = jnp.float32
VMEM = pl.BlockSpec(memory_space=pltpu.VMEM)
SMEM = pl.BlockSpec(memory_space=pltpu.SMEM)
HBM = pl.BlockSpec(memory_space=pltpu.HBM)
PARAMS = pltpu.CompilerParams(vmem_limit_bytes=8 * 2**20)


def tables(width, tile_rows):
    blocks = width // LANES
    half = blocks // 2
    lane = np.arange(LANES)
    ks = np.arange(half + 1)
    turn = 2.0 * np.pi / width * (ks[:, None] * lane[None, :])
    turns = np.stack((np.cos(turn), np.sin(turn))).astype(np.float32)
    angle = 2.0 * np.pi / LANES * (lane[:, None] * lane[None, :] % LANES)
    cos, sin = np.cos(angle), np.sin(angle)
    forward = np.block([[cos, -sin], [sin, cos]])

    def split(matrix):
        high = matrix.astype(jnp.bfloat16)
        low = (matrix - high.astype(np.float64)).astype(jnp.bfloat16)
        return np.stack((high, low))

    freq = (ks[:, None] + blocks * lane[None, :]).astype(np.float64)
    row = np.arange(tile_rows, dtype=np.float64)
    lam = 4.0 * np.sin(np.pi * row / tile_rows)[:, None, None] ** 2 + 4.0 * np.sin(np.pi * freq / width) ** 2
    filt = 1.0 / (1.0 + paganin_beta * lam)
    dist = np.arange(tile_rows // 2 + 1)
    gains = np.einsum("du,ukm->dkm", np.cos(2.0 * np.pi / tile_rows * dist[:, None] * row), filt) / tile_rows
    folded = np.minimum(freq, width - freq)
    ramp = ramp_gain * (folded / width) * (0.5 + 0.5 * np.cos(2.0 * np.pi * folded / width))
    twice = np.where((ks == 0) | (ks == half), 1.0, 2.0)
    gains = gains * (ramp * twice[:, None] / width)
    return turns, split(forward), split(forward.T), gains.astype(np.float32)


def plus(terms):
    return sum(terms[1:], terms[0])


def scaled(terms, weights):
    out = None
    for term, weight in zip(terms, weights):
        weight = float(weight)
        if abs(weight) < 1e-12:
            continue
        piece = term if weight == 1.0 else -term if weight == -1.0 else term * weight
        out = piece if out is None else out + piece
    return out


def cosine_sums(terms, blocks):
    half = blocks // 2
    out = [None] * (half + 1)
    for k in range(half // 2 + 1):
        wave = [np.round(np.cos(2.0 * np.pi * a * k / blocks), 15) for a in range(half + 1)]
        even = scaled(terms[0::2], wave[0::2])
        odd = scaled(terms[1::2], wave[1::2])
        out[k] = even if odd is None else even + odd
        if half - k != k:
            out[half - k] = even if odd is None else even - odd
    return out


def sine_sums(terms, blocks):
    half = blocks // 2
    out = [None] * (half + 1)
    for k in range(1, half // 2 + 1):
        wave = [np.round(np.sin(2.0 * np.pi * a * k / blocks), 15) for a in range(half)]
        even = scaled(terms[2:half:2], wave[2::2])
        odd = scaled(terms[1:half:2], wave[1::2])
        if half - k != k:
            out[k] = plus([x for x in (even, odd) if x is not None])
            out[half - k] = odd - even if even is not None else odd
        else:
            out[k] = plus([x for x in (even, odd) if x is not None])
    return out


def accurate_dot(values, matrix_ref):
    high = values.astype(jnp.bfloat16)
    low = (values - high.astype(jnp.float32)).astype(jnp.bfloat16)
    dot = partial(jnp.dot, preferred_element_type=jnp.float32)
    lines = values.shape[0]
    both = dot(jnp.concatenate((high, low), axis=0), matrix_ref[0])
    return both[:lines] + (both[lines:] + dot(high, matrix_ref[1]))


def spectrum(chunks, turns_ref, forward_ref):
    blocks = len(chunks)
    half = blocks // 2
    folds = [chunks[0]] + [chunks[a] + chunks[blocks - a] for a in range(1, half)] + [chunks[half]]
    skews = [None] + [chunks[a] - chunks[blocks - a] for a in range(1, half)] + [None]
    reals = cosine_sums(folds, blocks)
    imags = sine_sums(skews, blocks)
    parts = []
    for k in range(half + 1):
        cos, sin = turns_ref[0, k : k + 1, :], turns_ref[1, k : k + 1, :]
        if k == 0:
            re, im = reals[0], jnp.zeros_like(reals[0])
        elif imags[k] is None:
            re, im = reals[k] * cos, -(reals[k] * sin)
        else:
            re, im = reals[k] * cos - imags[k] * sin, -(imags[k] * cos) - reals[k] * sin
        parts.append(jnp.concatenate((re, im), axis=1))
    return accurate_dot(jnp.concatenate(parts, axis=0), forward_ref)


def columns(spec, turns_ref, inverse_ref, blocks):
    half = blocks // 2
    back = accurate_dot(spec, inverse_ref)
    reals, imags = [], []
    for k in range(half + 1):
        rows = slice(k * SUB, (k + 1) * SUB)
        re, im = back[rows, :LANES], back[rows, LANES:]
        cos, sin = turns_ref[0, k : k + 1, :], turns_ref[1, k : k + 1, :]
        if k == 0:
            reals.append(re)
            imags.append(None)
        else:
            reals.append(re * cos - im * sin)
            imags.append(im * cos + re * sin if k < half else None)
    even = cosine_sums(reals, blocks)
    odd = sine_sums(imags, blocks)
    out = [None] * blocks
    out[0], out[half] = even[0], even[half]
    for a in range(1, half):
        out[a] = even[a] - odd[a]
        out[blocks - a] = even[a] + odd[a]
    return out


def contrast_kernel(proj_hbm, flat_hbm, own_ref, first_ref, last_ref, proj, flat, sems):
    copies = [
        pltpu.make_async_copy(proj_hbm, proj, sems.at[0]),
        pltpu.make_async_copy(flat_hbm, flat, sems.at[1]),
    ]
    for copy in copies:
        copy.start()
    for copy in copies:
        copy.wait()
    own = 1.0 - proj[0].astype(jnp.float32) / flat[...]
    own_ref[...] = own
    first_ref[...] = own[:HALO].astype(first_ref.dtype)
    last_ref[...] = own[SUB - HALO :].astype(last_ref.dtype)


def lanes_of(ref, block):
    return ref[:, block * LANES : (block + 1) * LANES]


def halo_gains(gains_ref, k, row):
    gains = [jnp.broadcast_to(gains_ref[d, k : k + 1, :], (SUB, LANES)) for d in range(2 * HALO + 1)]
    for s in range(SUB):
        far = gains[2 * HALO - abs(s - HALO)]
        near = gains[abs(s - HALO)]
        if s < HALO:
            yield s, jnp.where(row >= s + HALO, near, far)
        else:
            yield s, jnp.where(row < s - HALO, near, far)


def own_kernel(
    own_ref, turns_ref, gains_ref, forward_hbm, inverse_hbm, starts_hbm, exchange_hbm,
    out_ref, forward_ref, inverse_ref, halo_ref, starts_ref, exchange_ref, sems
):
    forward_copy = pltpu.make_async_copy(forward_hbm, forward_ref, sems.at[0])
    inverse_copy = pltpu.make_async_copy(inverse_hbm, inverse_ref, sems.at[1])
    starts_copy = pltpu.make_async_copy(starts_hbm.at[pl.ds(lax.axis_index("ang"), 1)], starts_ref, sems.at[2])
    forward_copy.start()
    inverse_copy.start()
    starts_copy.start()
    exchange_copy = pltpu.make_async_copy(exchange_hbm, exchange_ref, sems.at[3])
    exchange_copy.start()
    row = lax.broadcasted_iota(jnp.int32, (SUB, LANES), 0)
    for k in range(gains_ref.shape[1]):
        for s, gain in halo_gains(gains_ref, k, row):
            halo_ref[s, k] = gain
    forward_copy.wait()
    blocks = own_ref.shape[1] // LANES
    spec = spectrum([lanes_of(own_ref, a) for a in range(blocks)], turns_ref, forward_ref)
    for k in range(blocks // 2 + 1):
        rows = slice(k * SUB, (k + 1) * SUB)
        for side in (slice(0, LANES), slice(LANES, 2 * LANES)):
            here = spec[rows, side]
            moved = [here] + [pltpu.roll(here, s, axis=0) for s in range(1, SUB)]
            total = here * gains_ref[0, k : k + 1, :]
            for d in range(1, SUB):
                pair = jnp.where(row >= d, moved[d], 0.0) + jnp.where(row < SUB - d, moved[SUB - d], 0.0)
                total += pair * gains_ref[d, k : k + 1, :]
            out_ref[rows, side] = total
    inverse_copy.wait()
    starts_copy.wait()
    exchange_copy.wait()


def tile_kernel(
    own_ref, below_ref, above_ref, starts, turns_ref, forward_ref, inverse_ref, gains_ref, out_ref,
    sheet
):
    blocks = above_ref.shape[1] // LANES
    halo = [
        jnp.concatenate((lanes_of(above_ref, a), lanes_of(below_ref, a)), axis=0).astype(jnp.float32)
        for a in range(blocks)
    ]
    spec = spectrum(halo, turns_ref, forward_ref)
    row = lax.broadcasted_iota(jnp.int32, (SUB, LANES), 0)
    lane = lax.broadcasted_iota(jnp.int32, (SUB, LANES), 1)
    parts = []
    for k in range(blocks // 2 + 1):
        rows = slice(k * SUB, (k + 1) * SUB)
        both = []
        for side in (slice(0, LANES), slice(LANES, 2 * LANES)):
            here = spec[rows, side]
            total = own_ref[rows, side] + here * gains_ref[0, k]
            for s in range(1, SUB):
                total += pltpu.roll(here, s, axis=0) * gains_ref[s, k]
            both.append(total)
        parts.append(jnp.concatenate(both, axis=1))
    filtered = columns(jnp.concatenate(parts, axis=0), turns_ref, inverse_ref, blocks)
    for a in range(blocks):
        sheet[a] = filtered[a]
    regions = starts.shape[1]
    cut = out_ref.shape[0] * LANES // (regions * SUB)
    per = LANES // cut
    keep = lane // cut == row % per
    packed = []
    for group in range(regions // per):
        gathered = None
        for q in range(per):
            start = starts[0, group * per + q]
            block = lax.shift_right_logical(start, 7)
            offset = start & (LANES - 1)
            window = jnp.where(lane >= offset, sheet[block], sheet[block + 1])
            window = pltpu.roll(window, (LANES + q * cut - offset) & (LANES - 1), axis=1)
            gathered = window if q == 0 else jnp.where(lane // cut == q, window, gathered)
        for shift in range(per):
            moved = gathered if shift == 0 else pltpu.roll(gathered, shift * cut, axis=1)
            packed.append(jnp.where(keep, moved, 0.0).astype(jnp.bfloat16))
    lines = out_ref.shape[0]
    want = lax.broadcasted_iota(jnp.int32, (lines, regions * SUB), 0)
    have = lax.broadcasted_iota(jnp.int32, (lines, regions * SUB), 1)
    have_row, have_shift, have_group = have % SUB, have // SUB % per, have // (SUB * per)
    have_region = have_group * per + (have_row % per + per - have_shift) % per
    pick = jnp.where(have_region * (SUB // per) + have_row // per == want, 1.0, 0.0).astype(jnp.bfloat16)
    out = jnp.dot(pick, jnp.concatenate(packed, axis=0), preferred_element_type=jnp.float32)
    out_ref[...] = out.astype(jnp.bfloat16)


class Routes:
    UNITS = 4
    AROUND = 16

    def __init__(self, count):
        step = count // self.AROUND
        devices = lambda steps: [s * step + c for s in steps for c in range(step)]
        link = lambda pairs: [p for src, dst in pairs for p in zip(devices([src]), devices([dst]))]
        self.count, self.half = count, count // 2
        self.near = devices((12, 13, 14, 15, 0, 1, 2, 3))
        self.far = devices(range(4, 12))
        self.relays = devices((1, 2, 3))
        self.swaps = 0
        self.enter = [
            link(((5, 2), (4, 3), (1, 6), (2, 5), (3, 4))),
            link(((10, 1), (8, 2), (6, 3))),
            link(((11, 1), (9, 2), (7, 3))),
        ]
        self.leave = [link(((12, 11), (13, 9), (2, 7), (3, 4))), link(((12, 10), (13, 8), (2, 6), (3, 5)))]

    def exchange_table(self):
        table = np.zeros((3, self.half * self.UNITS * 2, (1 + len(self.enter)) * self.count * 2), np.float32)

        def put(kind, m, unit, source, region):
            for i in range(2):
                table[kind, (m * self.UNITS + unit) * 2 + i, (source * self.count + region) * 2 + i] = 1.0

        for m, dest in enumerate(self.far):
            put(0, m, 0, 0, dest)
            put(0, m, 1, 1 + self.swaps, dest)
        for m, dest in enumerate(self.near):
            put(1, m, 0, 0, dest)
            put(2, m, 0, 0, dest)
            for turn in range(len(self.enter)):
                put(1, m, 1 + turn, 1 + turn, dest)
            for turn in range(len(self.leave)):
                for src, final in self.leave[turn]:
                    if src == dest:
                        put(2, m, 1 + turn, 0, final)
        return table.astype(jnp.bfloat16)

    def arrival_table(self):
        size = self.half * self.UNITS
        table = np.zeros((3, self.count * 2, 3 * size * 2), np.float32)

        def put(kind, angle, source, m, unit):
            for i in range(2):
                table[kind, angle * 2 + i, (source * size + m * self.UNITS + unit) * 2 + i] = 1.0

        for m, angle in enumerate(self.near):
            put(0, angle, 0, m, 0)
            for turn in range(len(self.enter)):
                for src, dst in self.enter[turn]:
                    if dst == angle:
                        put(0, src, 0, m, 1 + turn)
            for turn in range(len(self.leave)):
                if angle not in self.relays:
                    put(1 + turn, angle, 1 + turn, m, 1 + turn)
        for m, angle in enumerate(self.far):
            for turn in range(len(self.leave)):
                put(1 + turn, angle, 0, m, 0)
                for src, dst in self.enter[self.swaps]:
                    if dst == angle:
                        put(1 + turn, src, 0, m, 1)
        return table.astype(jnp.bfloat16)

    @classmethod
    def kinds(cls, device, count):
        step = device // (count // cls.AROUND)
        turned = lax.rem(step + 4, cls.AROUND)
        far = turned >= 8
        other = turned <= 4
        early = (step == 4) | ((step > 6) & (step % 2 == 1))
        return jnp.where(far, 0, jnp.where(other, 2, 1)), jnp.where(far, jnp.where(early, 1, 2), 0)

    @classmethod
    def taking_part(cls, device, count):
        step = device // (count // cls.AROUND)
        return (step > 0) & (step < cls.AROUND - 2)


def repack_kernel(lines_ref, first_ref, second_ref, third_ref, table_ref, out_ref):
    kind, _ = Routes.kinds(lax.axis_index("ang"), lax.axis_size("ang"))
    lines = jnp.concatenate((lines_ref[...], first_ref[...], second_ref[...], third_ref[...]), axis=0)
    out = jnp.dot(table_ref[kind], lines, preferred_element_type=jnp.float32)
    out_ref[...] = out.astype(out_ref.dtype)


def pixels_kernel(*refs, angles):
    _, kind = Routes.kinds(lax.axis_index("ang"), lax.axis_size("ang"))
    *held_refs, table_ref, weights_ref, out_ref, lines = refs
    held = jnp.concatenate([ref[...] for ref in held_refs], axis=0)
    table = table_ref[kind if len(held_refs) > 1 else 0, :, : held.shape[0]]
    lines[...] = jnp.dot(table, held, preferred_element_type=jnp.float32)
    cut = lines.shape[0] * LANES // SUB // angles
    per = LANES // cut
    row = lax.broadcasted_iota(jnp.int32, (SUB, LANES), 0)
    lane = lax.broadcasted_iota(jnp.int32, (SUB, LANES), 1)
    turn = (lane // cut + per - row % per) % per
    parts = []
    for group in range(angles // per):
        spread = []
        for q in range(per):
            at = (group * per + q) * (SUB // per)
            low = jnp.broadcast_to(lines[at : at + 1, :], (SUB, LANES))
            high = jnp.broadcast_to(lines[at + 1 : at + 2, :], (SUB, LANES))
            spread.append(jnp.where(row < per, low, high))
        part = None
        for shift in range(per):
            mixed = spread[shift]
            for j in range(1, per):
                mixed = jnp.where(row % per == j, spread[(j + shift) % per], mixed)
            if shift > 0:
                mixed = pltpu.roll(mixed, shift * cut, axis=1)
            part = mixed if shift == 0 else jnp.where(turn == shift, mixed, part)
        parts.append(part.astype(jnp.bfloat16))
    out_ref[...] = jnp.dot(jnp.concatenate(parts, axis=1), weights_ref[...], preferred_element_type=jnp.float32)


def in_hbm(array):
    return pltpu.with_memory_space_constraint(array, pltpu.HBM)


def make_contrast(projections, flats):
    shape = flats.shape
    edge = jax.ShapeDtypeStruct((HALO, shape[1]), halo_type)
    return pl.pallas_call(
        contrast_kernel,
        out_shape=(jax.ShapeDtypeStruct(shape, jnp.float32), edge, edge),
        in_specs=[HBM] * 2,
        out_specs=(VMEM,) * 3,
        scratch_shapes=[
            pltpu.VMEM(projections.shape, projections.dtype),
            pltpu.VMEM(flats.shape, flats.dtype),
            pltpu.SemaphoreType.DMA((2,)),
        ],
        compiler_params=PARAMS,
        name="contrast",
    )(in_hbm(projections), in_hbm(flats))


def make_own(own, turns, forward, inverse, gains, starts, exchange):
    groups = turns.shape[1]
    return pl.pallas_call(
        own_kernel,
        out_shape=(
            jax.ShapeDtypeStruct((groups * SUB, 2 * LANES), jnp.float32),
            jax.ShapeDtypeStruct(forward.shape, forward.dtype),
            jax.ShapeDtypeStruct(inverse.shape, inverse.dtype),
            jax.ShapeDtypeStruct((SUB, groups, SUB, LANES), jnp.float32),
            pltpu.SMEM((1, starts.shape[1]), jnp.int32),
            jax.ShapeDtypeStruct(exchange.shape, exchange.dtype),
        ),
        in_specs=[VMEM] * 3 + [HBM] * 4,
        out_specs=(VMEM,) * 4 + (SMEM, VMEM),
        scratch_shapes=[pltpu.SemaphoreType.DMA((4,))],
        compiler_params=PARAMS,
        name="own_rows",
    )(own, turns, gains, in_hbm(forward), in_hbm(inverse), in_hbm(starts), in_hbm(exchange))


def make_tile(own_spec, below, above, starts, turns, forward, inverse, gains, cut):
    regions = starts.shape[1]
    return pl.pallas_call(
        tile_kernel,
        out_shape=jax.ShapeDtypeStruct((regions * SUB * cut // LANES, LANES), jnp.bfloat16),
        in_specs=[VMEM] * 3 + [SMEM] + [VMEM] * 4,
        out_specs=VMEM,
        scratch_shapes=[
            pltpu.VMEM((above.shape[1] // LANES + 1, SUB, LANES), jnp.float32),
        ],
        compiler_params=PARAMS,
        name="tile",
    )(own_spec, below, above, starts, turns, forward, inverse, gains)


def make_repack(lines, first, second, third, table):
    return pl.pallas_call(
        repack_kernel,
        out_shape=jax.ShapeDtypeStruct((table.shape[1], LANES), lines.dtype),
        in_specs=[VMEM] * 5,
        out_specs=VMEM,
        compiler_params=PARAMS,
        name="repack",
    )(lines, first, second, third, table)


def make_pixels(held, table, weights):
    angles, cut, pixels = weights.shape
    return pl.pallas_call(
        partial(pixels_kernel, angles=angles),
        out_shape=jax.ShapeDtypeStruct((SUB, pixels), jnp.float32),
        in_specs=[VMEM] * (len(held) + 2),
        out_specs=VMEM,
        scratch_shapes=[pltpu.VMEM((table.shape[1], LANES), jnp.float32)],
        compiler_params=PARAMS,
        name="pixels",
    )(*held, table, weights.reshape(angles * cut, pixels))


def body(projections, flats, block_start, bp_weights):
    angles_dev, rows_dev, width = projections.shape
    cut = bp_weights.shape[1]
    assert angles_dev == 1 and rows_dev == SUB and width % (2 * LANES) == 0 and SUB * cut == 2 * LANES
    rows = lax.axis_size("row")
    up = [(i, i + 1) for i in range(rows - 1)]
    down = [(j, i) for i, j in up]
    turns, forward, inverse, gains = (jnp.asarray(t) for t in tables(width, rows_dev + 2 * HALO))
    own, first, last = make_contrast(projections, flats)
    below = lax.ppermute(first, "row", down)
    above = lax.ppermute(last, "row", up)
    routes = Routes(lax.axis_size("ang"))
    exchange, arrival = jnp.asarray(routes.exchange_table()), jnp.asarray(routes.arrival_table())
    own_spec, forward, inverse, gains, starts, exchange = make_own(
        own, turns, forward, inverse, gains, block_start, exchange
    )
    outgoing = make_tile(own_spec, below, above, starts, turns, forward, inverse, gains, cut)
    relayed = routes.taking_part(lax.axis_index("ang"), routes.count)

    def enter(lines):
        return make_repack(lines, *(lax.ppermute(lines, "ang", pairs) for pairs in routes.enter), exchange)

    def leave(lines):
        return make_pixels([lines, *(lax.ppermute(lines, "ang", pairs) for pairs in routes.leave)], arrival, bp_weights)

    packed = lax.cond(relayed, enter, lambda lines: make_repack(lines, lines, lines, lines, exchange), outgoing)
    near = lax.all_to_all(
        packed.reshape(-1, 2, LANES), "ang", split_axis=0, concat_axis=0, tiled=True,
        axis_index_groups=[routes.near, routes.far],
    ).reshape(packed.shape)
    return lax.cond(relayed, leave, lambda lines: make_pixels([lines], arrival, bp_weights), near)


def solution(mesh):
    placed = (P(("scan", "ang"), "row", None), P(("scan", "row"), None), P(), P(None, None, "ang"))
    return jax.shard_map(
        body, mesh=mesh, in_specs=placed, out_specs=P(("scan", "row"), "ang"), check_vma=False
    )
```

```python
from functools import partial

import jax
import jax.numpy as jnp
import numpy as np
from jax import lax
from jax.experimental import pallas as pl
from jax.experimental.pallas import tpu as pltpu
from jax.sharding import PartitionSpec as P

HALO = 4
LANES = 128
SUB = 8

paganin_beta = 8.0
ramp_gain = 320.0
halo_type = jnp.float32
VMEM = pl.BlockSpec(memory_space=pltpu.VMEM)
SMEM = pl.BlockSpec(memory_space=pltpu.SMEM)
HBM = pl.BlockSpec(memory_space=pltpu.HBM)
PARAMS = pltpu.CompilerParams(vmem_limit_bytes=8 * 2**20)


def tables(width, tile_rows):
    blocks = width // LANES
    half = blocks // 2
    lane = np.arange(LANES)
    ks = np.arange(half + 1)
    turn = 2.0 * np.pi / width * (ks[:, None] * lane[None, :])
    turns = np.stack((np.cos(turn), np.sin(turn))).astype(np.float32)
    angle = 2.0 * np.pi / LANES * (lane[:, None] * lane[None, :] % LANES)
    cos, sin = np.cos(angle), np.sin(angle)
    forward = np.block([[cos, -sin], [sin, cos]])

    def split(matrix):
        high = matrix.astype(jnp.bfloat16)
        low = (matrix - high.astype(np.float64)).astype(jnp.bfloat16)
        return np.stack((high, low))

    freq = (ks[:, None] + blocks * lane[None, :]).astype(np.float64)
    row = np.arange(tile_rows, dtype=np.float64)
    lam = 4.0 * np.sin(np.pi * row / tile_rows)[:, None, None] ** 2 + 4.0 * np.sin(np.pi * freq / width) ** 2
    filt = 1.0 / (1.0 + paganin_beta * lam)
    dist = np.arange(tile_rows // 2 + 1)
    gains = np.einsum("du,ukm->dkm", np.cos(2.0 * np.pi / tile_rows * dist[:, None] * row), filt) / tile_rows
    folded = np.minimum(freq, width - freq)
    ramp = ramp_gain * (folded / width) * (0.5 + 0.5 * np.cos(2.0 * np.pi * folded / width))
    twice = np.where((ks == 0) | (ks == half), 1.0, 2.0)
    gains = gains * (ramp * twice[:, None] / width)
    return turns, split(forward), split(forward.T), gains.astype(np.float32)


def plus(terms):
    return sum(terms[1:], terms[0])


def scaled(terms, weights):
    out = None
    for term, weight in zip(terms, weights):
        weight = float(weight)
        if abs(weight) < 1e-12:
            continue
        piece = term if weight == 1.0 else -term if weight == -1.0 else term * weight
        out = piece if out is None else out + piece
    return out


def cosine_sums(terms, blocks):
    half = blocks // 2
    out = [None] * (half + 1)
    for k in range(half // 2 + 1):
        wave = [np.round(np.cos(2.0 * np.pi * a * k / blocks), 15) for a in range(half + 1)]
        even = scaled(terms[0::2], wave[0::2])
        odd = scaled(terms[1::2], wave[1::2])
        out[k] = even if odd is None else even + odd
        if half - k != k:
            out[half - k] = even if odd is None else even - odd
    return out


def sine_sums(terms, blocks):
    half = blocks // 2
    out = [None] * (half + 1)
    for k in range(1, half // 2 + 1):
        wave = [np.round(np.sin(2.0 * np.pi * a * k / blocks), 15) for a in range(half)]
        even = scaled(terms[2:half:2], wave[2::2])
        odd = scaled(terms[1:half:2], wave[1::2])
        if half - k != k:
            out[k] = plus([x for x in (even, odd) if x is not None])
            out[half - k] = odd - even if even is not None else odd
        else:
            out[k] = plus([x for x in (even, odd) if x is not None])
    return out


def accurate_dot(values, matrix_ref):
    high = values.astype(jnp.bfloat16)
    low = (values - high.astype(jnp.float32)).astype(jnp.bfloat16)
    dot = partial(jnp.dot, preferred_element_type=jnp.float32)
    lines = values.shape[0]
    both = dot(jnp.concatenate((high, low), axis=0), matrix_ref[0])
    return both[:lines] + (both[lines:] + dot(high, matrix_ref[1]))


def spectrum(chunks, turns_ref, forward_ref):
    blocks = len(chunks)
    half = blocks // 2
    folds = [chunks[0]] + [chunks[a] + chunks[blocks - a] for a in range(1, half)] + [chunks[half]]
    skews = [None] + [chunks[a] - chunks[blocks - a] for a in range(1, half)] + [None]
    reals = cosine_sums(folds, blocks)
    imags = sine_sums(skews, blocks)
    parts = []
    for k in range(half + 1):
        cos, sin = turns_ref[0, k : k + 1, :], turns_ref[1, k : k + 1, :]
        if k == 0:
            re, im = reals[0], jnp.zeros_like(reals[0])
        elif imags[k] is None:
            re, im = reals[k] * cos, -(reals[k] * sin)
        else:
            re, im = reals[k] * cos - imags[k] * sin, -(imags[k] * cos) - reals[k] * sin
        parts.append(jnp.concatenate((re, im), axis=1))
    return accurate_dot(jnp.concatenate(parts, axis=0), forward_ref)


def columns(spec, turns_ref, inverse_ref, blocks):
    half = blocks // 2
    back = accurate_dot(spec, inverse_ref)
    reals, imags = [], []
    for k in range(half + 1):
        rows = slice(k * SUB, (k + 1) * SUB)
        re, im = back[rows, :LANES], back[rows, LANES:]
        cos, sin = turns_ref[0, k : k + 1, :], turns_ref[1, k : k + 1, :]
        if k == 0:
            reals.append(re)
            imags.append(None)
        else:
            reals.append(re * cos - im * sin)
            imags.append(im * cos + re * sin if k < half else None)
    even = cosine_sums(reals, blocks)
    odd = sine_sums(imags, blocks)
    out = [None] * blocks
    out[0], out[half] = even[0], even[half]
    for a in range(1, half):
        out[a] = even[a] - odd[a]
        out[blocks - a] = even[a] + odd[a]
    return out


def contrast_kernel(proj_hbm, flat_hbm, own_ref, first_ref, last_ref, proj, flat, sems):
    copies = [
        pltpu.make_async_copy(proj_hbm, proj, sems.at[0]),
        pltpu.make_async_copy(flat_hbm, flat, sems.at[1]),
    ]
    for copy in copies:
        copy.start()
    for copy in copies:
        copy.wait()
    own = 1.0 - proj[0].astype(jnp.float32) / flat[...]
    own_ref[...] = own
    first_ref[...] = own[:HALO].astype(first_ref.dtype)
    last_ref[...] = own[SUB - HALO :].astype(last_ref.dtype)


def lanes_of(ref, block):
    return ref[:, block * LANES : (block + 1) * LANES]


def halo_gains(gains_ref, k, row):
    gains = [jnp.broadcast_to(gains_ref[d, k : k + 1, :], (SUB, LANES)) for d in range(2 * HALO + 1)]
    for s in range(SUB):
        far = gains[2 * HALO - abs(s - HALO)]
        near = gains[abs(s - HALO)]
        if s < HALO:
            yield s, jnp.where(row >= s + HALO, near, far)
        else:
            yield s, jnp.where(row < s - HALO, near, far)


def own_kernel(
    own_ref, turns_ref, gains_ref, forward_hbm, inverse_hbm, starts_hbm, exchange_hbm,
    out_ref, forward_ref, inverse_ref, halo_ref, starts_ref, exchange_ref, sems
):
    forward_copy = pltpu.make_async_copy(forward_hbm, forward_ref, sems.at[0])
    inverse_copy = pltpu.make_async_copy(inverse_hbm, inverse_ref, sems.at[1])
    starts_copy = pltpu.make_async_copy(starts_hbm.at[pl.ds(lax.axis_index("ang"), 1)], starts_ref, sems.at[2])
    forward_copy.start()
    inverse_copy.start()
    starts_copy.start()
    exchange_copy = pltpu.make_async_copy(exchange_hbm, exchange_ref, sems.at[3])
    exchange_copy.start()
    row = lax.broadcasted_iota(jnp.int32, (SUB, LANES), 0)
    for k in range(gains_ref.shape[1]):
        for s, gain in halo_gains(gains_ref, k, row):
            halo_ref[s, k] = gain
    forward_copy.wait()
    blocks = own_ref.shape[1] // LANES
    spec = spectrum([lanes_of(own_ref, a) for a in range(blocks)], turns_ref, forward_ref)
    for k in range(blocks // 2 + 1):
        rows = slice(k * SUB, (k + 1) * SUB)
        for side in (slice(0, LANES), slice(LANES, 2 * LANES)):
            here = spec[rows, side]
            moved = [here] + [pltpu.roll(here, s, axis=0) for s in range(1, SUB)]
            total = here * gains_ref[0, k : k + 1, :]
            for d in range(1, SUB):
                pair = jnp.where(row >= d, moved[d], 0.0) + jnp.where(row < SUB - d, moved[SUB - d], 0.0)
                total += pair * gains_ref[d, k : k + 1, :]
            out_ref[rows, side] = total
    inverse_copy.wait()
    starts_copy.wait()
    exchange_copy.wait()


def tile_kernel(
    own_ref, below_ref, above_ref, starts, turns_ref, forward_ref, inverse_ref, gains_ref, out_ref,
    sheet
):
    blocks = above_ref.shape[1] // LANES
    halo = [
        jnp.concatenate((lanes_of(above_ref, a), lanes_of(below_ref, a)), axis=0).astype(jnp.float32)
        for a in range(blocks)
    ]
    spec = spectrum(halo, turns_ref, forward_ref)
    row = lax.broadcasted_iota(jnp.int32, (SUB, LANES), 0)
    lane = lax.broadcasted_iota(jnp.int32, (SUB, LANES), 1)
    parts = []
    for k in range(blocks // 2 + 1):
        rows = slice(k * SUB, (k + 1) * SUB)
        both = []
        for side in (slice(0, LANES), slice(LANES, 2 * LANES)):
            here = spec[rows, side]
            total = own_ref[rows, side] + here * gains_ref[0, k]
            for s in range(1, SUB):
                total += pltpu.roll(here, s, axis=0) * gains_ref[s, k]
            both.append(total)
        parts.append(jnp.concatenate(both, axis=1))
    filtered = columns(jnp.concatenate(parts, axis=0), turns_ref, inverse_ref, blocks)
    for a in range(blocks):
        sheet[a] = filtered[a]
    regions = starts.shape[1]
    cut = out_ref.shape[0] * LANES // (regions * SUB)
    per = LANES // cut
    keep = lane // cut == row % per
    packed = []
    for group in range(regions // per):
        gathered = None
        for q in range(per):
            start = starts[0, group * per + q]
            block = lax.shift_right_logical(start, 7)
            offset = start & (LANES - 1)
            window = jnp.where(lane >= offset, sheet[block], sheet[block + 1])
            window = pltpu.roll(window, (LANES + q * cut - offset) & (LANES - 1), axis=1)
            gathered = window if q == 0 else jnp.where(lane // cut == q, window, gathered)
        for shift in range(per):
            moved = gathered if shift == 0 else pltpu.roll(gathered, shift * cut, axis=1)
            packed.append(jnp.where(keep, moved, 0.0).astype(jnp.bfloat16))
    lines = out_ref.shape[0]
    want = lax.broadcasted_iota(jnp.int32, (lines, regions * SUB), 0)
    have = lax.broadcasted_iota(jnp.int32, (lines, regions * SUB), 1)
    have_row, have_shift, have_group = have % SUB, have // SUB % per, have // (SUB * per)
    have_region = have_group * per + (have_row % per + per - have_shift) % per
    pick = jnp.where(have_region * (SUB // per) + have_row // per == want, 1.0, 0.0).astype(jnp.bfloat16)
    out = jnp.dot(pick, jnp.concatenate(packed, axis=0), preferred_element_type=jnp.float32)
    out_ref[...] = out.astype(jnp.bfloat16)


class Routes:
    UNITS = 4
    AROUND = 16

    def __init__(self, count):
        step = count // self.AROUND
        devices = lambda steps: [s * step + c for s in steps for c in range(step)]
        link = lambda pairs: [p for src, dst in pairs for p in zip(devices([src]), devices([dst]))]
        self.count, self.half = count, count // 2
        self.near = devices((12, 13, 14, 15, 0, 1, 2, 3))
        self.far = devices(range(4, 12))
        self.relays = devices((1, 2, 3))
        self.swaps = 0
        self.enter = [
            link(((5, 2), (4, 3), (1, 6), (2, 5), (3, 4))),
            link(((10, 1), (8, 2), (6, 3))),
            link(((11, 1), (9, 2), (7, 3))),
        ]
        self.leave = [link(((12, 11), (13, 9), (14, 7), (3, 4))), link(((12, 10), (13, 8), (14, 6), (3, 5)))]

    def exchange_table(self):
        table = np.zeros((3, self.half * self.UNITS * 2, (1 + len(self.enter)) * self.count * 2), np.float32)

        def put(kind, m, unit, source, region):
            for i in range(2):
                table[kind, (m * self.UNITS + unit) * 2 + i, (source * self.count + region) * 2 + i] = 1.0

        for m, dest in enumerate(self.far):
            put(0, m, 0, 0, dest)
            put(0, m, 1, 1 + self.swaps, dest)
        for m, dest in enumerate(self.near):
            put(1, m, 0, 0, dest)
            put(2, m, 0, 0, dest)
            for turn in range(len(self.enter)):
                put(1, m, 1 + turn, 1 + turn, dest)
            for turn in range(len(self.leave)):
                for src, final in self.leave[turn]:
                    if src == dest:
                        put(2, m, 1 + turn, 0, final)
        return table.astype(jnp.bfloat16)

    def arrival_table(self):
        size = self.half * self.UNITS
        table = np.zeros((3, self.count * 2, 3 * size * 2), np.float32)

        def put(kind, angle, source, m, unit):
            for i in range(2):
                table[kind, angle * 2 + i, (source * size + m * self.UNITS + unit) * 2 + i] = 1.0

        for m, angle in enumerate(self.near):
            put(0, angle, 0, m, 0)
            for turn in range(len(self.enter)):
                for src, dst in self.enter[turn]:
                    if dst == angle:
                        put(0, src, 0, m, 1 + turn)
            for turn in range(len(self.leave)):
                if angle not in self.relays:
                    put(1 + turn, angle, 1 + turn, m, 1 + turn)
        for m, angle in enumerate(self.far):
            for turn in range(len(self.leave)):
                put(1 + turn, angle, 0, m, 0)
                for src, dst in self.enter[self.swaps]:
                    if dst == angle:
                        put(1 + turn, src, 0, m, 1)
        return table.astype(jnp.bfloat16)

    @classmethod
    def kinds(cls, device, count):
        step = device // (count // cls.AROUND)
        turned = lax.rem(step + 4, cls.AROUND)
        far = turned >= 8
        other = turned <= 4
        early = (step == 4) | ((step > 6) & (step % 2 == 1))
        return jnp.where(far, 0, jnp.where(other, 2, 1)), jnp.where(far, jnp.where(early, 1, 2), 0)

    @classmethod
    def taking_part(cls, device, count):
        step = device // (count // cls.AROUND)
        return (step > 0) & (step < cls.AROUND - 1)


def repack_kernel(lines_ref, first_ref, second_ref, third_ref, table_ref, out_ref):
    kind, _ = Routes.kinds(lax.axis_index("ang"), lax.axis_size("ang"))
    lines = jnp.concatenate((lines_ref[...], first_ref[...], second_ref[...], third_ref[...]), axis=0)
    out = jnp.dot(table_ref[kind], lines, preferred_element_type=jnp.float32)
    out_ref[...] = out.astype(out_ref.dtype)


def pixels_kernel(*refs, angles):
    _, kind = Routes.kinds(lax.axis_index("ang"), lax.axis_size("ang"))
    *held_refs, table_ref, weights_ref, out_hbm, lines, out_ref, sem = refs
    held = jnp.concatenate([ref[...] for ref in held_refs], axis=0)
    table = table_ref[kind if len(held_refs) > 1 else 0, :, : held.shape[0]]
    lines[...] = jnp.dot(table, held, preferred_element_type=jnp.float32)
    cut = lines.shape[0] * LANES // SUB // angles
    per = LANES // cut
    row = lax.broadcasted_iota(jnp.int32, (SUB, LANES), 0)
    lane = lax.broadcasted_iota(jnp.int32, (SUB, LANES), 1)
    turn = (lane // cut + per - row % per) % per
    parts = []
    for group in range(angles // per):
        spread = []
        for q in range(per):
            at = (group * per + q) * (SUB // per)
            low = jnp.broadcast_to(lines[at : at + 1, :], (SUB, LANES))
            high = jnp.broadcast_to(lines[at + 1 : at + 2, :], (SUB, LANES))
            spread.append(jnp.where(row < per, low, high))
        part = None
        for shift in range(per):
            mixed = spread[shift]
            for j in range(1, per):
                mixed = jnp.where(row % per == j, spread[(j + shift) % per], mixed)
            if shift > 0:
                mixed = pltpu.roll(mixed, shift * cut, axis=1)
            part = mixed if shift == 0 else jnp.where(turn == shift, mixed, part)
        parts.append(part.astype(jnp.bfloat16))
    out_ref[...] = jnp.dot(jnp.concatenate(parts, axis=1), weights_ref[...], preferred_element_type=jnp.float32)
    copy = pltpu.make_async_copy(out_ref, out_hbm, sem)
    copy.start()
    copy.wait()


def in_hbm(array):
    return pltpu.with_memory_space_constraint(array, pltpu.HBM)


def make_contrast(projections, flats):
    shape = flats.shape
    edge = jax.ShapeDtypeStruct((HALO, shape[1]), halo_type)
    return pl.pallas_call(
        contrast_kernel,
        out_shape=(jax.ShapeDtypeStruct(shape, jnp.float32), edge, edge),
        in_specs=[HBM] * 2,
        out_specs=(VMEM,) * 3,
        scratch_shapes=[
            pltpu.VMEM(projections.shape, projections.dtype),
            pltpu.VMEM(flats.shape, flats.dtype),
            pltpu.SemaphoreType.DMA((2,)),
        ],
        compiler_params=PARAMS,
        name="contrast",
    )(in_hbm(projections), in_hbm(flats))


def make_own(own, turns, forward, inverse, gains, starts, exchange):
    groups = turns.shape[1]
    return pl.pallas_call(
        own_kernel,
        out_shape=(
            jax.ShapeDtypeStruct((groups * SUB, 2 * LANES), jnp.float32),
            jax.ShapeDtypeStruct(forward.shape, forward.dtype),
            jax.ShapeDtypeStruct(inverse.shape, inverse.dtype),
            jax.ShapeDtypeStruct((SUB, groups, SUB, LANES), jnp.float32),
            pltpu.SMEM((1, starts.shape[1]), jnp.int32),
            jax.ShapeDtypeStruct(exchange.shape, exchange.dtype),
        ),
        in_specs=[VMEM] * 3 + [HBM] * 4,
        out_specs=(VMEM,) * 4 + (SMEM, VMEM),
        scratch_shapes=[pltpu.SemaphoreType.DMA((4,))],
        compiler_params=PARAMS,
        name="own_rows",
    )(own, turns, gains, in_hbm(forward), in_hbm(inverse), in_hbm(starts), in_hbm(exchange))


def make_tile(own_spec, below, above, starts, turns, forward, inverse, gains, cut):
    regions = starts.shape[1]
    return pl.pallas_call(
        tile_kernel,
        out_shape=jax.ShapeDtypeStruct((regions * SUB * cut // LANES, LANES), jnp.bfloat16),
        in_specs=[VMEM] * 3 + [SMEM] + [VMEM] * 4,
        out_specs=VMEM,
        scratch_shapes=[
            pltpu.VMEM((above.shape[1] // LANES + 1, SUB, LANES), jnp.float32),
        ],
        compiler_params=PARAMS,
        name="tile",
    )(own_spec, below, above, starts, turns, forward, inverse, gains)


def make_repack(lines, first, second, third, table):
    return pl.pallas_call(
        repack_kernel,
        out_shape=jax.ShapeDtypeStruct((table.shape[1], LANES), lines.dtype),
        in_specs=[VMEM] * 5,
        out_specs=VMEM,
        compiler_params=PARAMS,
        name="repack",
    )(lines, first, second, third, table)


def make_pixels(held, table, weights):
    angles, cut, pixels = weights.shape
    return pl.pallas_call(
        partial(pixels_kernel, angles=angles),
        out_shape=pltpu.HBM((SUB, pixels), jnp.float32),
        in_specs=[VMEM] * (len(held) + 2),
        out_specs=HBM,
        scratch_shapes=[
            pltpu.VMEM((table.shape[1], LANES), jnp.float32),
            pltpu.VMEM((SUB, pixels), jnp.float32),
            pltpu.SemaphoreType.DMA,
        ],
        compiler_params=PARAMS,
        name="pixels",
    )(*held, table, weights.reshape(angles * cut, pixels))


def body(projections, flats, block_start, bp_weights):
    angles_dev, rows_dev, width = projections.shape
    cut = bp_weights.shape[1]
    assert angles_dev == 1 and rows_dev == SUB and width % (2 * LANES) == 0 and SUB * cut == 2 * LANES
    rows = lax.axis_size("row")
    up = [(i, i + 1) for i in range(rows - 1)]
    down = [(j, i) for i, j in up]
    turns, forward, inverse, gains = (jnp.asarray(t) for t in tables(width, rows_dev + 2 * HALO))
    own, first, last = make_contrast(projections, flats)
    below = lax.ppermute(first, "row", down)
    above = lax.ppermute(last, "row", up)
    routes = Routes(lax.axis_size("ang"))
    exchange, arrival = jnp.asarray(routes.exchange_table()), jnp.asarray(routes.arrival_table())
    own_spec, forward, inverse, gains, starts, exchange = make_own(
        own, turns, forward, inverse, gains, block_start, exchange
    )
    outgoing = make_tile(own_spec, below, above, starts, turns, forward, inverse, gains, cut)
    relayed = routes.taking_part(lax.axis_index("ang"), routes.count)

    def enter(lines):
        return make_repack(lines, *(lax.ppermute(lines, "ang", pairs) for pairs in routes.enter), exchange)

    def leave(lines):
        return make_pixels([lines, *(lax.ppermute(lines, "ang", pairs) for pairs in routes.leave)], arrival, bp_weights)

    packed = lax.cond(relayed, enter, lambda lines: make_repack(lines, lines, lines, lines, exchange), outgoing)
    near = lax.all_to_all(
        packed.reshape(-1, 2, LANES), "ang", split_axis=0, concat_axis=0, tiled=True,
        axis_index_groups=[routes.near, routes.far],
    ).reshape(packed.shape)
    return lax.cond(relayed, leave, lambda lines: make_pixels([lines], arrival, bp_weights), near)


def solution(mesh):
    placed = (P(("scan", "ang"), "row", None), P(("scan", "row"), None), P(), P(None, None, "ang"))
    return jax.shard_map(
        body, mesh=mesh, in_specs=placed, out_specs=P(("scan", "row"), "ang"), check_vma=False
    )
```

```python
from functools import partial

import jax
import jax.numpy as jnp
import numpy as np
from jax import lax
from jax.experimental import pallas as pl
from jax.experimental.pallas import tpu as pltpu
from jax.sharding import PartitionSpec as P

HALO = 4
LANES = 128
SUB = 8

paganin_beta = 8.0
ramp_gain = 320.0
halo_type = jnp.float32
VMEM = pl.BlockSpec(memory_space=pltpu.VMEM)
SMEM = pl.BlockSpec(memory_space=pltpu.SMEM)
HBM = pl.BlockSpec(memory_space=pltpu.HBM)
PARAMS = pltpu.CompilerParams(vmem_limit_bytes=8 * 2**20)
TILE_PARAMS = pltpu.CompilerParams(
    vmem_limit_bytes=8 * 2**20
)


def tables(width, tile_rows):
    blocks = width // LANES
    half = blocks // 2
    lane = np.arange(LANES)
    ks = np.arange(half + 1)
    turn = 2.0 * np.pi / width * (ks[:, None] * lane[None, :])
    turns = np.stack((np.cos(turn), np.sin(turn))).astype(np.float32)
    angle = 2.0 * np.pi / LANES * (lane[:, None] * lane[None, :] % LANES)
    cos, sin = np.cos(angle), np.sin(angle)
    forward = np.block([[cos, -sin], [sin, cos]])

    def split(matrix):
        high = matrix.astype(jnp.bfloat16)
        low = (matrix - high.astype(np.float64)).astype(jnp.bfloat16)
        return np.stack((high, low))

    freq = (ks[:, None] + blocks * lane[None, :]).astype(np.float64)
    row = np.arange(tile_rows, dtype=np.float64)
    lam = 4.0 * np.sin(np.pi * row / tile_rows)[:, None, None] ** 2 + 4.0 * np.sin(np.pi * freq / width) ** 2
    filt = 1.0 / (1.0 + paganin_beta * lam)
    dist = np.arange(tile_rows // 2 + 1)
    gains = np.einsum("du,ukm->dkm", np.cos(2.0 * np.pi / tile_rows * dist[:, None] * row), filt) / tile_rows
    folded = np.minimum(freq, width - freq)
    ramp = ramp_gain * (folded / width) * (0.5 + 0.5 * np.cos(2.0 * np.pi * folded / width))
    twice = np.where((ks == 0) | (ks == half), 1.0, 2.0)
    gains = gains * (ramp * twice[:, None] / width)
    return turns, split(forward), split(forward.T), gains.astype(np.float32)


def plus(terms):
    return sum(terms[1:], terms[0])


def scaled(terms, weights):
    out = None
    for term, weight in zip(terms, weights):
        weight = float(weight)
        if abs(weight) < 1e-12:
            continue
        piece = term if weight == 1.0 else -term if weight == -1.0 else term * weight
        out = piece if out is None else out + piece
    return out


def cosine_sums(terms, blocks):
    half = blocks // 2
    out = [None] * (half + 1)
    for k in range(half // 2 + 1):
        wave = [np.round(np.cos(2.0 * np.pi * a * k / blocks), 15) for a in range(half + 1)]
        even = scaled(terms[0::2], wave[0::2])
        odd = scaled(terms[1::2], wave[1::2])
        out[k] = even if odd is None else even + odd
        if half - k != k:
            out[half - k] = even if odd is None else even - odd
    return out


def sine_sums(terms, blocks):
    half = blocks // 2
    out = [None] * (half + 1)
    for k in range(1, half // 2 + 1):
        wave = [np.round(np.sin(2.0 * np.pi * a * k / blocks), 15) for a in range(half)]
        even = scaled(terms[2:half:2], wave[2::2])
        odd = scaled(terms[1:half:2], wave[1::2])
        if half - k != k:
            out[k] = plus([x for x in (even, odd) if x is not None])
            out[half - k] = odd - even if even is not None else odd
        else:
            out[k] = plus([x for x in (even, odd) if x is not None])
    return out


def accurate_dot(values, matrix_ref):
    high = values.astype(jnp.bfloat16)
    low = (values - high.astype(jnp.float32)).astype(jnp.bfloat16)
    dot = partial(jnp.dot, preferred_element_type=jnp.float32)
    lines = values.shape[0]
    both = dot(jnp.concatenate((high, low), axis=0), matrix_ref[0])
    return both[:lines] + (both[lines:] + dot(high, matrix_ref[1]))


def spectrum(chunks, turns_ref, forward_ref):
    blocks = len(chunks)
    half = blocks // 2
    folds = [chunks[0]] + [chunks[a] + chunks[blocks - a] for a in range(1, half)] + [chunks[half]]
    skews = [None] + [chunks[a] - chunks[blocks - a] for a in range(1, half)] + [None]
    reals = cosine_sums(folds, blocks)
    imags = sine_sums(skews, blocks)
    parts = []
    for k in range(half + 1):
        cos, sin = turns_ref[0, k : k + 1, :], turns_ref[1, k : k + 1, :]
        if k == 0:
            re, im = reals[0], jnp.zeros_like(reals[0])
        elif imags[k] is None:
            re, im = reals[k] * cos, -(reals[k] * sin)
        else:
            re, im = reals[k] * cos - imags[k] * sin, -(imags[k] * cos) - reals[k] * sin
        parts.append(jnp.concatenate((re, im), axis=1))
    return accurate_dot(jnp.concatenate(parts, axis=0), forward_ref)


def columns(spec, turns_ref, inverse_ref, blocks):
    half = blocks // 2
    back = accurate_dot(spec, inverse_ref)
    reals, imags = [], []
    for k in range(half + 1):
        rows = slice(k * SUB, (k + 1) * SUB)
        re, im = back[rows, :LANES], back[rows, LANES:]
        cos, sin = turns_ref[0, k : k + 1, :], turns_ref[1, k : k + 1, :]
        if k == 0:
            reals.append(re)
            imags.append(None)
        else:
            reals.append(re * cos - im * sin)
            imags.append(im * cos + re * sin if k < half else None)
    even = cosine_sums(reals, blocks)
    odd = sine_sums(imags, blocks)
    out = [None] * blocks
    out[0], out[half] = even[0], even[half]
    for a in range(1, half):
        out[a] = even[a] - odd[a]
        out[blocks - a] = even[a] + odd[a]
    return out


def contrast_kernel(proj_hbm, flat_hbm, own_ref, first_ref, last_ref, proj, flat, sems):
    copies = [
        pltpu.make_async_copy(proj_hbm, proj, sems.at[0]),
        pltpu.make_async_copy(flat_hbm, flat, sems.at[1]),
    ]
    for copy in copies:
        copy.start()
    for copy in copies:
        copy.wait()
    own = 1.0 - proj[0].astype(jnp.float32) / flat[...]
    own_ref[...] = own
    first_ref[...] = own[:HALO].astype(first_ref.dtype)
    last_ref[...] = own[SUB - HALO :].astype(last_ref.dtype)


def lanes_of(ref, block):
    return ref[:, block * LANES : (block + 1) * LANES]


def halo_gains(gains_ref, k, row):
    gains = [jnp.broadcast_to(gains_ref[d, k : k + 1, :], (SUB, LANES)) for d in range(2 * HALO + 1)]
    for s in range(SUB):
        far = gains[2 * HALO - abs(s - HALO)]
        near = gains[abs(s - HALO)]
        if s < HALO:
            yield s, jnp.where(row >= s + HALO, near, far)
        else:
            yield s, jnp.where(row < s - HALO, near, far)


def own_kernel(
    own_ref, turns_ref, gains_ref, forward_hbm, inverse_hbm, starts_hbm, exchange_hbm,
    out_ref, forward_ref, inverse_ref, halo_ref, starts_ref, exchange_ref, sems
):
    forward_copy = pltpu.make_async_copy(forward_hbm, forward_ref, sems.at[0])
    inverse_copy = pltpu.make_async_copy(inverse_hbm, inverse_ref, sems.at[1])
    starts_copy = pltpu.make_async_copy(starts_hbm.at[pl.ds(lax.axis_index("ang"), 1)], starts_ref, sems.at[2])
    forward_copy.start()
    inverse_copy.start()
    starts_copy.start()
    exchange_copy = pltpu.make_async_copy(exchange_hbm, exchange_ref, sems.at[3])
    exchange_copy.start()
    row = lax.broadcasted_iota(jnp.int32, (SUB, LANES), 0)
    for k in range(gains_ref.shape[1]):
        for s, gain in halo_gains(gains_ref, k, row):
            halo_ref[s, k] = gain
    forward_copy.wait()
    blocks = own_ref.shape[1] // LANES
    spec = spectrum([lanes_of(own_ref, a) for a in range(blocks)], turns_ref, forward_ref)
    for k in range(blocks // 2 + 1):
        rows = slice(k * SUB, (k + 1) * SUB)
        for side in (slice(0, LANES), slice(LANES, 2 * LANES)):
            here = spec[rows, side]
            moved = [here] + [pltpu.roll(here, s, axis=0) for s in range(1, SUB)]
            total = here * gains_ref[0, k : k + 1, :]
            for d in range(1, SUB):
                pair = jnp.where(row >= d, moved[d], 0.0) + jnp.where(row < SUB - d, moved[SUB - d], 0.0)
                total += pair * gains_ref[d, k : k + 1, :]
            out_ref[rows, side] = total
    inverse_copy.wait()
    starts_copy.wait()
    exchange_copy.wait()


def tile_kernel(
    own_ref, below_ref, above_ref, starts, turns_ref, forward_ref, inverse_ref, gains_ref, out_ref,
    sheet
):
    blocks = above_ref.shape[1] // LANES
    halo = [
        jnp.concatenate((lanes_of(above_ref, a), lanes_of(below_ref, a)), axis=0).astype(jnp.float32)
        for a in range(blocks)
    ]
    spec = spectrum(halo, turns_ref, forward_ref)
    row = lax.broadcasted_iota(jnp.int32, (SUB, LANES), 0)
    lane = lax.broadcasted_iota(jnp.int32, (SUB, LANES), 1)
    parts = []
    for k in range(blocks // 2 + 1):
        rows = slice(k * SUB, (k + 1) * SUB)
        both = []
        for side in (slice(0, LANES), slice(LANES, 2 * LANES)):
            here = spec[rows, side]
            total = own_ref[rows, side] + here * gains_ref[0, k]
            for s in range(1, SUB):
                total += pltpu.roll(here, s, axis=0) * gains_ref[s, k]
            both.append(total)
        parts.append(jnp.concatenate(both, axis=1))
    filtered = columns(jnp.concatenate(parts, axis=0), turns_ref, inverse_ref, blocks)
    for a in range(blocks):
        sheet[a] = filtered[a]
    regions = starts.shape[1]
    cut = out_ref.shape[0] * LANES // (regions * SUB)
    per = LANES // cut
    keep = lane // cut == row % per
    packed = []
    for group in range(regions // per):
        gathered = None
        for q in range(per):
            start = starts[0, group * per + q]
            block = lax.shift_right_logical(start, 7)
            offset = start & (LANES - 1)
            window = jnp.where(lane >= offset, sheet[block], sheet[block + 1])
            window = pltpu.roll(window, (LANES + q * cut - offset) & (LANES - 1), axis=1)
            gathered = window if q == 0 else jnp.where(lane // cut == q, window, gathered)
        for shift in range(per):
            moved = gathered if shift == 0 else pltpu.roll(gathered, shift * cut, axis=1)
            packed.append(jnp.where(keep, moved, 0.0).astype(jnp.bfloat16))
    lines = out_ref.shape[0]
    want = lax.broadcasted_iota(jnp.int32, (lines, regions * SUB), 0)
    have = lax.broadcasted_iota(jnp.int32, (lines, regions * SUB), 1)
    have_row, have_shift, have_group = have % SUB, have // SUB % per, have // (SUB * per)
    have_region = have_group * per + (have_row % per + per - have_shift) % per
    pick = jnp.where(have_region * (SUB // per) + have_row // per == want, 1.0, 0.0).astype(jnp.bfloat16)
    out = jnp.dot(pick, jnp.concatenate(packed, axis=0), preferred_element_type=jnp.float32)
    out_ref[...] = out.astype(jnp.bfloat16)


class Routes:
    UNITS = 4
    AROUND = 16

    def __init__(self, count):
        step = count // self.AROUND
        devices = lambda steps: [s * step + c for s in steps for c in range(step)]
        link = lambda pairs: [p for src, dst in pairs for p in zip(devices([src]), devices([dst]))]
        self.count, self.half = count, count // 2
        self.near = devices((12, 13, 14, 15, 0, 1, 2, 3))
        self.far = devices(range(4, 12))
        self.relays = devices((1, 2, 3))
        self.swaps = 0
        self.enter = [
            link(((5, 2), (4, 3), (1, 6), (2, 5), (3, 4))),
            link(((10, 1), (8, 2), (6, 3))),
            link(((11, 1), (9, 2), (7, 3))),
        ]
        self.leave = [link(((12, 11), (13, 9), (14, 7), (3, 4))), link(((12, 10), (13, 8), (14, 6), (3, 5)))]

    def exchange_table(self):
        table = np.zeros((3, self.half * self.UNITS * 2, (1 + len(self.enter)) * self.count * 2), np.float32)

        def put(kind, m, unit, source, region):
            for i in range(2):
                table[kind, (m * self.UNITS + unit) * 2 + i, (source * self.count + region) * 2 + i] = 1.0

        for m, dest in enumerate(self.far):
            put(0, m, 0, 0, dest)
            put(0, m, 1, 1 + self.swaps, dest)
        for m, dest in enumerate(self.near):
            put(1, m, 0, 0, dest)
            put(2, m, 0, 0, dest)
            for turn in range(len(self.enter)):
                put(1, m, 1 + turn, 1 + turn, dest)
            for turn in range(len(self.leave)):
                for src, final in self.leave[turn]:
                    if src == dest:
                        put(2, m, 1 + turn, 0, final)
        return table.astype(jnp.bfloat16)

    def arrival_table(self):
        size = self.half * self.UNITS
        table = np.zeros((3, self.count * 2, 3 * size * 2), np.float32)

        def put(kind, angle, source, m, unit):
            for i in range(2):
                table[kind, angle * 2 + i, (source * size + m * self.UNITS + unit) * 2 + i] = 1.0

        for m, angle in enumerate(self.near):
            put(0, angle, 0, m, 0)
            for turn in range(len(self.enter)):
                for src, dst in self.enter[turn]:
                    if dst == angle:
                        put(0, src, 0, m, 1 + turn)
            for turn in range(len(self.leave)):
                if angle not in self.relays:
                    put(1 + turn, angle, 1 + turn, m, 1 + turn)
        for m, angle in enumerate(self.far):
            for turn in range(len(self.leave)):
                put(1 + turn, angle, 0, m, 0)
                for src, dst in self.enter[self.swaps]:
                    if dst == angle:
                        put(1 + turn, src, 0, m, 1)
        return table.astype(jnp.bfloat16)

    @classmethod
    def kinds(cls, device, count):
        step = device // (count // cls.AROUND)
        turned = lax.rem(step + 4, cls.AROUND)
        far = turned >= 8
        other = turned <= 4
        early = (step == 4) | ((step > 6) & (step % 2 == 1))
        return jnp.where(far, 0, jnp.where(other, 2, 1)), jnp.where(far, jnp.where(early, 1, 2), 0)

    @classmethod
    def taking_part(cls, device, count):
        step = device // (count // cls.AROUND)
        return (step > 0) & (step < cls.AROUND - 1)


def repack_kernel(lines_ref, first_ref, second_ref, third_ref, table_ref, out_ref):
    kind, _ = Routes.kinds(lax.axis_index("ang"), lax.axis_size("ang"))
    lines = jnp.concatenate((lines_ref[...], first_ref[...], second_ref[...], third_ref[...]), axis=0)
    out = jnp.dot(table_ref[kind], lines, preferred_element_type=jnp.float32)
    out_ref[...] = out.astype(out_ref.dtype)


def pixels_kernel(*refs, angles):
    _, kind = Routes.kinds(lax.axis_index("ang"), lax.axis_size("ang"))
    *held_refs, table_ref, weights_ref, out_ref, lines = refs
    held = jnp.concatenate([ref[...] for ref in held_refs], axis=0)
    table = table_ref[kind if len(held_refs) > 1 else 0, :, : held.shape[0]]
    lines[...] = jnp.dot(table, held, preferred_element_type=jnp.float32)
    cut = lines.shape[0] * LANES // SUB // angles
    per = LANES // cut
    row = lax.broadcasted_iota(jnp.int32, (SUB, LANES), 0)
    lane = lax.broadcasted_iota(jnp.int32, (SUB, LANES), 1)
    turn = (lane // cut + per - row % per) % per
    parts = []
    for group in range(angles // per):
        spread = []
        for q in range(per):
            at = (group * per + q) * (SUB // per)
            low = jnp.broadcast_to(lines[at : at + 1, :], (SUB, LANES))
            high = jnp.broadcast_to(lines[at + 1 : at + 2, :], (SUB, LANES))
            spread.append(jnp.where(row < per, low, high))
        part = None
        for shift in range(per):
            mixed = spread[shift]
            for j in range(1, per):
                mixed = jnp.where(row % per == j, spread[(j + shift) % per], mixed)
            if shift > 0:
                mixed = pltpu.roll(mixed, shift * cut, axis=1)
            part = mixed if shift == 0 else jnp.where(turn == shift, mixed, part)
        parts.append(part.astype(jnp.bfloat16))
    out_ref[...] = jnp.dot(jnp.concatenate(parts, axis=1), weights_ref[...], preferred_element_type=jnp.float32)


def in_hbm(array):
    return pltpu.with_memory_space_constraint(array, pltpu.HBM)


def make_contrast(projections, flats):
    shape = flats.shape
    edge = jax.ShapeDtypeStruct((HALO, shape[1]), halo_type)
    return pl.pallas_call(
        contrast_kernel,
        out_shape=(jax.ShapeDtypeStruct(shape, jnp.float32), edge, edge),
        in_specs=[HBM] * 2,
        out_specs=(VMEM,) * 3,
        scratch_shapes=[
            pltpu.VMEM(projections.shape, projections.dtype),
            pltpu.VMEM(flats.shape, flats.dtype),
            pltpu.SemaphoreType.DMA((2,)),
        ],
        compiler_params=PARAMS,
        name="contrast",
    )(in_hbm(projections), in_hbm(flats))


def make_own(own, turns, forward, inverse, gains, starts, exchange):
    groups = turns.shape[1]
    return pl.pallas_call(
        own_kernel,
        out_shape=(
            jax.ShapeDtypeStruct((groups * SUB, 2 * LANES), jnp.float32),
            jax.ShapeDtypeStruct(forward.shape, forward.dtype),
            jax.ShapeDtypeStruct(inverse.shape, inverse.dtype),
            jax.ShapeDtypeStruct((SUB, groups, SUB, LANES), jnp.float32),
            pltpu.SMEM((1, starts.shape[1]), jnp.int32),
            jax.ShapeDtypeStruct(exchange.shape, exchange.dtype),
        ),
        in_specs=[VMEM] * 3 + [HBM] * 4,
        out_specs=(VMEM,) * 4 + (SMEM, VMEM),
        scratch_shapes=[pltpu.SemaphoreType.DMA((4,))],
        compiler_params=PARAMS,
        name="own_rows",
    )(own, turns, gains, in_hbm(forward), in_hbm(inverse), in_hbm(starts), in_hbm(exchange))


def make_tile(own_spec, below, above, starts, turns, forward, inverse, gains, cut):
    regions = starts.shape[1]
    return pl.pallas_call(
        tile_kernel,
        out_shape=jax.ShapeDtypeStruct((regions * SUB * cut // LANES, LANES), jnp.bfloat16),
        in_specs=[VMEM] * 3 + [SMEM] + [VMEM] * 4,
        out_specs=VMEM,
        scratch_shapes=[
            pltpu.VMEM((above.shape[1] // LANES + 1, SUB, LANES), jnp.float32),
        ],
        compiler_params=TILE_PARAMS,
        name="tile",
    )(own_spec, below, above, starts, turns, forward, inverse, gains)


def make_repack(lines, first, second, third, table):
    return pl.pallas_call(
        repack_kernel,
        out_shape=jax.ShapeDtypeStruct((table.shape[1], LANES), lines.dtype),
        in_specs=[VMEM] * 5,
        out_specs=VMEM,
        compiler_params=PARAMS,
        name="repack",
    )(lines, first, second, third, table)


def make_pixels(held, table, weights):
    angles, cut, pixels = weights.shape
    return pl.pallas_call(
        partial(pixels_kernel, angles=angles),
        out_shape=jax.ShapeDtypeStruct((SUB, pixels), jnp.float32),
        in_specs=[VMEM] * (len(held) + 2),
        out_specs=VMEM,
        scratch_shapes=[pltpu.VMEM((table.shape[1], LANES), jnp.float32)],
        compiler_params=PARAMS,
        name="pixels",
    )(*held, table, weights.reshape(angles * cut, pixels))


def body(projections, flats, block_start, bp_weights):
    angles_dev, rows_dev, width = projections.shape
    cut = bp_weights.shape[1]
    assert angles_dev == 1 and rows_dev == SUB and width % (2 * LANES) == 0 and SUB * cut == 2 * LANES
    rows = lax.axis_size("row")
    up = [(i, i + 1) for i in range(rows - 1)]
    down = [(j, i) for i, j in up]
    turns, forward, inverse, gains = (jnp.asarray(t) for t in tables(width, rows_dev + 2 * HALO))
    own, first, last = make_contrast(projections, flats)
    below = lax.ppermute(first, "row", down)
    above = lax.ppermute(last, "row", up)
    routes = Routes(lax.axis_size("ang"))
    exchange, arrival = jnp.asarray(routes.exchange_table()), jnp.asarray(routes.arrival_table())
    own_spec, forward, inverse, gains, starts, exchange = make_own(
        own, turns, forward, inverse, gains, block_start, exchange
    )
    outgoing = make_tile(own_spec, below, above, starts, turns, forward, inverse, gains, cut)
    relayed = routes.taking_part(lax.axis_index("ang"), routes.count)

    def enter(lines):
        return make_repack(lines, *(lax.ppermute(lines, "ang", pairs) for pairs in routes.enter), exchange)

    def leave(lines):
        return make_pixels([lines, *(lax.ppermute(lines, "ang", pairs) for pairs in routes.leave)], arrival, bp_weights)

    packed = lax.cond(relayed, enter, lambda lines: make_repack(lines, lines, lines, lines, exchange), outgoing)
    near = lax.all_to_all(
        packed.reshape(-1, 2, LANES), "ang", split_axis=0, concat_axis=0, tiled=True,
        axis_index_groups=[routes.near, routes.far],
    ).reshape(packed.shape)
    return lax.cond(relayed, leave, lambda lines: make_pixels([lines], arrival, bp_weights), near)


def solution(mesh):
    placed = (P(("scan", "ang"), "row", None), P(("scan", "row"), None), P(), P(None, None, "ang"))
    return jax.shard_map(
        body, mesh=mesh, in_specs=placed, out_specs=P(("scan", "row"), "ang"), check_vma=False
    )
```
